32 devices in a mesh: gx: 8 (over z, core), gy: 4 (over y, x).
Axes of the slice: x: 2, y: 2, z: 4, core: 2. Of those that a mesh axis runs over, the one named last changes fastest.
Arguments:
- potential: float32 [32, 64, 256], P('gx', 'gy'), may hold values from -0.2 to 1.2
- recovery: float32 [32, 64, 256], P('gx', 'gy'), may hold values from 0 to 1.5
- fiber_angles: float32 [2, 32, 64, 256], P(None, 'gx', 'gy'), may hold values from -3.140625 to 3.140625
- deform: float32 [9, 8192], P(None, ('gx', 'gy')), may hold values from -0.15 to 1.25, as said below
- elem_slot: int32 [8, 16, 64], P('gx', 'gy'), may hold values from 0 to 8191, as said below
Outputs:
- potential_next: float32 [32, 64, 256], P('gx', 'gy')
- recovery_next: float32 [32, 64, 256], P('gx', 'gy')
The draws below stay inside these ranges and needn't reach their ends.
Inputs may be any that keep to these rules, and one draw needn't show every extreme that they name: `elem_slot`: entries are distinct. Slot s lies on device s / 256 (rounded down) of gx+gy. The elements of one device's block along gx and gy lie in the slots of the devices with the same index along gx, exactly 64 of them in each. `deform`: components 0, 4 and 8 (the diagonal of F) lie in 0.8 to 1.25, the other six in -0.15 to 0.15.
All inputs are finite; a program needn't handle non-finite values.
Results may differ from the reference program's by a relative error of at most 0.0003.
Values sent between devices are 32-bit elements; how exact they have to be, the bound alone decides.
A program may use at most 64 MiB of HBM per device.

```python
import math
import jax
import jax.numpy as jnp
from jax import lax

RATIO = 4
KX = 1
KY = 4
NCZ = 64
NZ = 256
NX = 32
NY = 64
CB = 256
SHARE = 64
NE = 8192
N_GX = 8
N_GY = 4
DEVICES = 32


def draw_deform(key, part):
    diag_key = jax.random.fold_in(key, 21)
    off_key = jax.random.fold_in(key, 22)
    diagonal = jnp.exp(jax.random.uniform(diag_key, (3, NE), jnp.float32, math.log(0.8), math.log(1.25)))
    offside = jnp.clip(0.06 * jax.random.normal(off_key, (6, NE), jnp.float32), -0.15, 0.15)
    diagonal = jnp.clip(diagonal, 0.8, 1.25)
    rows = [diagonal[0], offside[0], offside[1], offside[2], diagonal[1], offside[3], offside[4], offside[5], diagonal[2]]
    return jnp.stack(rows).astype(jnp.float32)


def draw_elem_slot(key, part):
    block_keys = jax.random.split(jax.random.fold_in(key, 31), DEVICES)
    holder_keys = jax.random.split(jax.random.fold_in(key, 32), DEVICES)
    ranks = jax.vmap(lambda one_key: jax.random.permutation(one_key, CB))(block_keys).astype(jnp.int32)
    holding = jax.vmap(lambda one_key: jax.random.permutation(one_key, CB))(holder_keys).astype(jnp.int32)
    device_index = jnp.arange(DEVICES, dtype=jnp.int32)
    row_start = device_index // N_GY * N_GY
    column = device_index % N_GY
    holder = row_start[:, None] + ranks // SHARE
    position = column[:, None] * SHARE + ranks % SHARE
    local_slot = holding[holder, position]
    slots = holder * CB + local_slot
    grid = slots.reshape(N_GX, N_GY, KX, KY, NCZ).transpose(0, 2, 1, 3, 4).reshape(N_GX * KX, N_GY * KY, NCZ)
    return grid.astype(jnp.int32)


def block_scale(key, dims, shards, smallest, largest):
    def one(dim, parts):
        draws = jax.random.uniform(jax.random.fold_in(jax.random.fold_in(key, 6), dim), (parts,), jnp.float32, smallest / len(shards), largest / len(shards))
        return jnp.repeat(jnp.exp(draws), dims[dim] // parts).reshape((-1,) + (1,) * (len(dims) - dim - 1))

    level = one(*shards[0])
    for cut in shards[1:]:
        level = level * one(*cut)
    return level


def setup_inputs(seed: int = 0) -> dict:
    seeds = jax.random.split(jax.random.key(seed), 6)
    potential = jnp.clip(-0.2 + 1.4000001 * jax.random.uniform(seeds[0], (NX, NY, NZ), jnp.float32) ** block_scale(seeds[0], (NX, NY, NZ), ((0, 8), (1, 4)), -0.2, 0.2), -0.2, 1.2)
    recovery = jnp.clip(1.5 * jax.random.uniform(seeds[1], (NX, NY, NZ), jnp.float32) ** block_scale(seeds[1], (NX, NY, NZ), ((0, 8), (1, 4)), -0.2, 0.2), 0.0, 1.5)
    fiber_angles = jnp.clip(jax.random.uniform(seeds[2], (2, NX, NY, NZ), jnp.float32, -3.140625, 3.140625), -3.140625, 3.140625)
    deform = draw_deform(jax.random.fold_in(seeds[5], 71), 0)
    elem_slot = draw_elem_slot(jax.random.fold_in(seeds[5], 71), 0)
    return dict(potential=potential, recovery=recovery, fiber_angles=fiber_angles, deform=deform, elem_slot=elem_slot)


sigma_fiber = 1.0
sigma_cross = 0.3
time_step = 0.1
excite_gain = 8.0
excite_level = 0.15
stretch_gain = 10.0
stretch_reversal = 0.6
recover_rate = 0.5

def refine(padded, dim):
    inner_size = padded.shape[dim] - 2
    lower = lax.slice_in_dim(padded, 0, inner_size, axis=dim)
    middle = lax.slice_in_dim(padded, 1, inner_size + 1, axis=dim)
    upper = lax.slice_in_dim(padded, 2, inner_size + 2, axis=dim)
    pieces = []
    for position in range(RATIO):
        offset = (position + 0.5) / RATIO - 0.5
        weight = abs(offset)
        neighbor = lower if offset < 0 else upper
        pieces.append((1.0 - weight) * middle + weight * neighbor)
    stacked = jnp.stack(pieces, axis=dim + 1)
    new_shape = list(padded.shape)
    new_shape[dim] = inner_size * RATIO
    return stacked.reshape(new_shape)

def directions(angles):
    azimuth = angles[0]
    elevation = angles[1]
    return jnp.stack([jnp.cos(azimuth) * jnp.cos(elevation), jnp.sin(azimuth) * jnp.cos(elevation), jnp.sin(elevation)])

def tensors(field, fiber):
    entries = [field[number] for number in range(9)]

    def element(row_index, col_index):
        return entries[3 * (row_index % 3) + col_index % 3]
    cofactor = [[element(row_index + 1, col_index + 1) * element(row_index + 2, col_index + 2) - element(row_index + 1, col_index + 2) * element(row_index + 2, col_index + 1) for col_index in range(3)] for row_index in range(3)]
    determinant = element(0, 0) * cofactor[0][0] + element(0, 1) * cofactor[0][1] + element(0, 2) * cofactor[0][2]
    inverse = [[cofactor[col_index][row_index] / determinant for col_index in range(3)] for row_index in range(3)]
    stretched = [element(row_index, 0) * fiber[0] + element(row_index, 1) * fiber[1] + element(row_index, 2) * fiber[2] for row_index in range(3)]
    stretch = jnp.sqrt(stretched[0] * stretched[0] + stretched[1] * stretched[1] + stretched[2] * stretched[2])
    pulled = [inverse[row_index][0] * fiber[0] + inverse[row_index][1] * fiber[1] + inverse[row_index][2] * fiber[2] for row_index in range(3)]
    conduct = []
    for first_index, second_index in ((0, 0), (1, 1), (2, 2), (0, 1), (0, 2), (1, 2)):
        metric = inverse[first_index][0] * inverse[second_index][0] + inverse[first_index][1] * inverse[second_index][1] + inverse[first_index][2] * inverse[second_index][2]
        conduct.append(sigma_cross * metric + (sigma_fiber - sigma_cross) * pulled[first_index] * pulled[second_index])
    return (jnp.stack(conduct), stretch)

def close_faces(flux, dim, at_first, at_last):
    extent = flux.shape[dim]
    face_index = lax.broadcasted_iota(jnp.int32, flux.shape, dim)
    closed = (face_index == 0) & at_first | (face_index == extent - 1) & at_last
    return jnp.where(closed, jnp.zeros_like(flux), flux)

def divergence(potential_pad, tensor_pad, first_x, last_x, first_y, last_y):
    grad_x = (potential_pad[2:, :, :] - potential_pad[:-2, :, :]) * 0.5
    grad_y = (potential_pad[:, 2:, :] - potential_pad[:, :-2, :]) * 0.5
    grad_z = (potential_pad[:, :, 2:] - potential_pad[:, :, :-2]) * 0.5

    def face_mean(component, dim):
        inner = tensor_pad[component]
        if dim == 0:
            inner = inner[:, 1:-1, 1:-1]
        elif dim == 1:
            inner = inner[1:-1, :, 1:-1]
        else:
            inner = inner[1:-1, 1:-1, :]
        extent = inner.shape[dim]
        return (lax.slice_in_dim(inner, 1, extent, axis=dim) + lax.slice_in_dim(inner, 0, extent - 1, axis=dim)) * 0.5
    step_x = potential_pad[1:, 1:-1, 1:-1] - potential_pad[:-1, 1:-1, 1:-1]
    mean_y = (grad_y[1:, :, 1:-1] + grad_y[:-1, :, 1:-1]) * 0.5
    mean_z = (grad_z[1:, 1:-1, :] + grad_z[:-1, 1:-1, :]) * 0.5
    flux_x = face_mean(0, 0) * step_x + face_mean(3, 0) * mean_y + face_mean(4, 0) * mean_z
    flux_x = close_faces(flux_x, 0, first_x, last_x)
    step_y = potential_pad[1:-1, 1:, 1:-1] - potential_pad[1:-1, :-1, 1:-1]
    mean_x = (grad_x[:, 1:, 1:-1] + grad_x[:, :-1, 1:-1]) * 0.5
    mean_z = (grad_z[1:-1, 1:, :] + grad_z[1:-1, :-1, :]) * 0.5
    flux_y = face_mean(3, 1) * mean_x + face_mean(1, 1) * step_y + face_mean(5, 1) * mean_z
    flux_y = close_faces(flux_y, 1, first_y, last_y)
    step_z = potential_pad[1:-1, 1:-1, 1:] - potential_pad[1:-1, 1:-1, :-1]
    mean_x = (grad_x[:, 1:-1, 1:] + grad_x[:, 1:-1, :-1]) * 0.5
    mean_y = (grad_y[1:-1, :, 1:] + grad_y[1:-1, :, :-1]) * 0.5
    flux_z = face_mean(4, 2) * mean_x + face_mean(5, 2) * mean_y + face_mean(2, 2) * step_z
    flux_z = close_faces(flux_z, 2, True, True)
    return flux_x[1:] - flux_x[:-1] + (flux_y[:, 1:] - flux_y[:, :-1]) + (flux_z[:, :, 1:] - flux_z[:, :, :-1])

def update(voltage, recovery, divergent, stretch):
    current = excite_gain * voltage * (voltage - excite_level) * (voltage - 1.0) + voltage * recovery
    current = current + stretch_gain * jnp.maximum(stretch - 1.0, 0.0) * (voltage - stretch_reversal)
    voltage_next = voltage + time_step * (divergent - current)
    recovery_next = recovery + time_step * recover_rate * (-recovery - excite_gain * voltage * (voltage - excite_level - 1.0))
    return (voltage_next, recovery_next)

def reference(potential, recovery, fiber_angles, deform, elem_slot):
    coarse = deform[:, elem_slot]
    coarse = jnp.pad(coarse, ((0, 0), (1, 1), (1, 1), (1, 1)), mode='edge')
    along_x = refine(coarse, 1)
    along_x = jnp.pad(along_x, ((0, 0), (1, 1), (0, 0), (0, 0)), mode='edge')
    angles_pad = jnp.pad(fiber_angles, ((0, 0), (1, 1), (0, 0), (0, 0)), mode='edge')
    potential_all = jnp.pad(potential, 1, mode='edge')
    width = NX // N_GX

    def slab(index):
        start = (index * width).astype(jnp.int32)
        segment = lax.dynamic_slice_in_dim(along_x, start, width + 2, axis=1)
        fine_field = refine(refine(segment, 2), 3)
        angles = lax.dynamic_slice_in_dim(angles_pad, start, width + 2, axis=1)
        conduct, stretch = tensors(fine_field, directions(angles))
        tensor_pad = jnp.pad(conduct, ((0, 0), (0, 0), (1, 1), (1, 1)), mode='edge')
        potential_pad = lax.dynamic_slice_in_dim(potential_all, start, width + 2, axis=0)
        divergent = divergence(potential_pad, tensor_pad, index == 0, index == N_GX - 1, True, True)
        voltage = lax.dynamic_slice_in_dim(potential, start, width, axis=0)
        resting = lax.dynamic_slice_in_dim(recovery, start, width, axis=0)
        return update(voltage, resting, divergent, stretch[1:-1])
    voltage_next, recovery_next = lax.map(slab, jnp.arange(N_GX, dtype=jnp.int32))
    return (voltage_next.reshape(NX, NY, NZ), recovery_next.reshape(NX, NY, NZ))
```

```python
import functools

import jax
import jax.numpy as jnp
from jax import lax
from jax.experimental import pallas as pl
from jax.experimental.pallas import tpu as pltpu
from jax.sharding import PartitionSpec as P

MESH = pl.DeviceIdType.MESH
RATIO = 4
LANES = 128
VMEM_LIMIT = 16 * 1024 * 1024
TOP = 8


def split_two(values):
    high = values.astype(jnp.bfloat16)
    low = (values - high.astype(jnp.float32)).astype(jnp.bfloat16)
    return high, low


def dot_two(values, weights):
    high, low = split_two(values)
    return jnp.dot(high, weights, preferred_element_type=jnp.float32) + jnp.dot(
        low, weights, preferred_element_type=jnp.float32
    )


def sine_cosine(angle):
    turn = jnp.floor(angle * 0.6366197723675814 + 0.5)
    rest = angle - turn * 1.5703125
    rest = rest - turn * 4.8375129699707031e-4
    rest = rest - turn * 7.549789948768648e-8
    square = rest * rest
    sine = rest + rest * square * (
        -1.6666654611e-1 + square * (8.3321608736e-3 + square * -1.9515295891e-4)
    )
    cosine = (
        1.0
        - 0.5 * square
        + square
        * square
        * (4.166664568298827e-2 + square * (-1.388731625493765e-3 + square * 2.443315711809948e-5))
    )
    size = jnp.abs(turn)
    odd = size == 1.0
    sine_part = jnp.where(odd, cosine * turn, sine)
    cosine_part = jnp.where(odd, sine * -turn, cosine)
    flip = jnp.where(size == 2.0, -1.0, 1.0)
    return sine_part * flip, cosine_part * flip


def fiber_of(azimuth, elevation):
    sin_u, cos_u = sine_cosine(azimuth)
    sin_e, cos_e = sine_cosine(elevation)
    return cos_u * cos_e, sin_u * cos_e, sin_e


def tensor_of(entries, fiber):
    def element(i, j):
        return entries[3 * (i % 3) + j % 3]

    adjugate = [
        [
            element(j + 1, i + 1) * element(j + 2, i + 2)
            - element(j + 1, i + 2) * element(j + 2, i + 1)
            for j in range(3)
        ]
        for i in range(3)
    ]
    determinant = (
        element(0, 0) * adjugate[0][0]
        + element(0, 1) * adjugate[1][0]
        + element(0, 2) * adjugate[2][0]
    )
    inverse = 1.0 / determinant
    square = inverse * inverse
    cross = 0.3 * square
    along = 0.7 * square
    pulled = [
        adjugate[i][0] * fiber[0] + adjugate[i][1] * fiber[1] + adjugate[i][2] * fiber[2]
        for i in range(3)
    ]
    scaled = [along * pulled[i] for i in range(3)]
    conduct = []
    for i, j in ((0, 0), (1, 1), (2, 2), (0, 1), (0, 2), (1, 2)):
        metric = (
            adjugate[i][0] * adjugate[j][0]
            + adjugate[i][1] * adjugate[j][1]
            + adjugate[i][2] * adjugate[j][2]
        )
        conduct.append(cross * metric + scaled[i] * pulled[j])
    return conduct


def stretch_of(entries, fiber):
    parts = [
        entries[3 * i] * fiber[0] + entries[3 * i + 1] * fiber[1] + entries[3 * i + 2] * fiber[2]
        for i in range(3)
    ]
    return jnp.sqrt(parts[0] * parts[0] + parts[1] * parts[1] + parts[2] * parts[2])


def exchange(
    across,
    down,
    sizes,
    potential,
    recovery,
    angles,
    deform,
    slots,
    cells,
    rest_in,
    held,
    near_slots,
    fibers,
    spread_y,
    spread_z,
    send_sem,
    deform_sem,
    slot_sem,
    side_sem,
    edge_sem,
    corner_sem,
    local_sem,
):
    bx, by, nz, ex, ey, ez, parts, count = sizes
    blocks = count // LANES
    gx, gy = lax.axis_index("gx"), lax.axis_index("gy")
    first_y, last_y = gy == 0, gy == down - 1
    leave = 2 * lax.rem(gx, 2) - 1
    sides = []
    for dx in (leave, -leave):
        sides.append((dx, jnp.logical_and(gx + dx >= 0, gx + dx < across)))

    def row_targets(include_self):
        for mask in sorted(range(down), key=lambda m: (-m.bit_count(), m)):
            if mask == 0 and not include_self:
                continue
            if down & (down - 1):
                yield lax.rem(gy + mask, down)
            else:
                target = gy
                for bit in range(down.bit_length() - 1):
                    if mask >> bit & 1:
                        step = 1 << bit
                        target = target + step - 2 * step * lax.rem(gy // step, 2)
                yield target

    barrier = pltpu.get_barrier_semaphore()

    def greet(dx):
        for target in row_targets(not isinstance(dx, int)):
            pl.semaphore_signal(barrier, inc=1, device_id=(gx + dx, target), device_id_type=MESH)

    for dx, there in sides:
        pl.when(there)(functools.partial(greet, dx))
    greet(0)

    packed = held.at[1, gy]
    for b in range(blocks):
        columns = pl.ds(b * LANES, LANES)
        pltpu.make_async_copy(
            deform.at[pl.ds(0, 8), columns], packed.at[pl.ds(8 * b, 8)], local_sem.at[0]
        ).start()
        pltpu.make_async_copy(
            deform.at[pl.ds(8, 1), columns], packed.at[pl.ds(8 * blocks + b, 1)], local_sem.at[0]
        ).start()
    inside = pl.ds(TOP, by)
    get_slots = pltpu.make_async_copy(slots, near_slots.at[1, 1], local_sem.at[1])
    get_slots.start()
    own_cells = cells.at[:, pl.ds(1, bx), inside]
    pltpu.make_async_copy(potential, cells.at[0, pl.ds(1, bx), inside], local_sem.at[2]).start()
    pltpu.make_async_copy(angles, cells.at[pl.ds(1, 2), pl.ds(1, bx), inside], local_sem.at[2]).start()
    get_rest = pltpu.make_async_copy(recovery, rest_in, local_sem.at[3])
    get_rest.start()

    def drain(ref, sem):
        pltpu.make_async_copy(ref, ref, sem).wait()

    rows = pl.ds(0, 9 * blocks)
    drain(held.at[1, gy, rows], local_sem.at[0])
    rows_here = 1 + sum(there.astype(jnp.int32) for _, there in sides)
    pl.semaphore_wait(barrier, rows_here * down - 1)

    def put(source, target, sem, dx, where):
        return pltpu.make_async_remote_copy(
            src_ref=source,
            dst_ref=target,
            send_sem=send_sem.at[0],
            recv_sem=sem,
            device_id=(gx + dx, where),
            device_id_type=MESH,
        )

    def send_deform(dx):
        q = 1 - dx
        for target in row_targets(not isinstance(dx, int)):
            put(held.at[1, gy, rows], held.at[q, gy, rows], deform_sem.at[q], dx, target).start()

    for dx, there in sides:
        pl.when(there)(functools.partial(send_deform, dx))
    send_deform(0)

    def at_y(dy, act):
        pl.when(jnp.logical_not(first_y if dy < 0 else last_y))(act)

    get_slots.wait()

    def send_slots(dx, dy):
        q = 1 - dx
        put(near_slots.at[1, 1], near_slots.at[q, 1 - dy], slot_sem.at[q], dx, gy + dy).start()

    def slots_side(dx, straight):
        if straight:
            send_slots(dx, 0)
        for dy in (-1, 1):
            at_y(dy, functools.partial(send_slots, dx, dy))

    for dx, there in sides:
        pl.when(there)(functools.partial(slots_side, dx, True))
    slots_side(0, False)

    drain(own_cells, local_sem.at[2])

    def edges(dy):
        source = pl.ds(TOP if dy < 0 else TOP + by - 1, 1)
        target = pl.ds(TOP + by if dy < 0 else TOP - 1, 1)
        return source, target

    def send_side(dx):
        q = 1 - dx
        x_source = pl.ds(jnp.where(dx < 0, 1, bx), 1)
        x_target = pl.ds(jnp.where(dx < 0, bx + 1, 0), 1)
        put(cells.at[:, x_source, inside], cells.at[:, x_target, inside], side_sem.at[q // 2], dx, gy).start()
        for dy in (-1, 1):
            y_source, y_target = edges(dy)

            def corner(dy=dy, y_source=y_source, y_target=y_target):
                put(
                    cells.at[pl.ds(0, 1), x_source, y_source],
                    cells.at[pl.ds(0, 1), x_target, y_target],
                    corner_sem.at[q // 2],
                    dx,
                    gy + dy,
                ).start()

            at_y(dy, corner)

    def send_edge(dy):
        y_source, y_target = edges(dy)
        x_here = pl.ds(1, bx)
        put(cells.at[:, x_here, y_source], cells.at[:, x_here, y_target], edge_sem.at[0], 0, gy + dy).start()

    for dx, there in sides:
        pl.when(there)(functools.partial(send_side, dx))
    for dy in (-1, 1):
        at_y(dy, functools.partial(send_edge, dy))
    get_rest.wait()

    width = (ey + 2) * ez
    tall = by + 8
    row = lax.broadcasted_iota(jnp.int32, (tall, width), 0)
    lane = lax.broadcasted_iota(jnp.int32, (tall, width), 1)
    cell = jnp.where(row < by, row, jnp.where(row < by + bx, -1, by))
    spot = (cell.astype(jnp.float32) + 0.5) * (1.0 / RATIO) - 0.5
    spread_y[...] = jnp.maximum(
        1.0 - jnp.abs(spot - ((lane // ez) - 1).astype(jnp.float32)), 0.0
    )
    row = lax.broadcasted_iota(jnp.int32, (width, nz), 0)
    lane = lax.broadcasted_iota(jnp.int32, (width, nz), 1)
    spot = jnp.clip((lane.astype(jnp.float32) + 0.5) * (1.0 / RATIO) - 0.5, 0.0, ez - 1.0)
    weight = jnp.maximum(1.0 - jnp.abs(spot - lax.rem(row, ez).astype(jnp.float32)), 0.0)
    spread_z[...] = weight.astype(jnp.bfloat16)

    for s in range(bx):
        own = [cells[number, s + 1, TOP : TOP + by] for number in (1, 2)]
        for number, part in enumerate(fiber_of(*own)):
            fibers[number, s] = part

    middle_y = jnp.logical_not(jnp.logical_or(first_y, last_y))
    some_y = jnp.logical_xor(first_y, last_y)

    def over_y(act):
        pl.when(middle_y)(functools.partial(act, 2))
        pl.when(some_y)(functools.partial(act, 1))

    def wait_deform(sem, dx):
        q = 1 - dx
        part = pl.ds(0, down - 1 if isinstance(dx, int) else down)
        drain(held.at[q, part, rows], sem if sem is not None else deform_sem.at[q])

    def wait_slots(sem, dx, straight):
        q = 1 - dx
        sem = slot_sem.at[q] if sem is None else sem
        if down == 1:
            if straight:
                drain(near_slots.at[1, pl.ds(0, 1)], sem)
        else:
            over_y(lambda n: drain(near_slots.at[1, pl.ds(0, n + straight)], sem))

    def wait_side(sem, dx):
        q = 1 - dx
        drain(cells.at[:, pl.ds(0, 1), inside], side_sem.at[q // 2] if sem is None else sem)
        sem = corner_sem.at[q // 2] if sem is None else sem
        over_y(lambda n: drain(cells.at[pl.ds(0, 1), pl.ds(0, 1), pl.ds(0, n)], sem))

    def wait_all(sem):
        for dx, there in sides:
            pl.when(there)(functools.partial(wait_deform, sem, -dx if sem is None else dx))
        wait_deform(sem, 0)
        for dx, there in sides:
            pl.when(there)(functools.partial(wait_slots, sem, -dx if sem is None else dx, 1))
        wait_slots(sem, 0, 0)
        for dx, there in sides:
            pl.when(there)(functools.partial(wait_side, sem, -dx if sem is None else dx))
        edge = edge_sem.at[0] if sem is None else sem
        over_y(lambda n: drain(cells.at[:, pl.ds(1, bx), pl.ds(0, n)], edge))

    wait_all(None)
    wait_all(send_sem.at[0])


def compute(
    across,
    down,
    sizes,
    cells,
    rest_in,
    held,
    near_slots,
    fibers,
    spread_y,
    spread_z,
    next_potential,
    next_recovery,
    volts,
    conducts,
    out_potential,
    out_recovery,
    out_sem,
):
    bx, by, nz, ex, ey, ez, parts, count = sizes
    blocks = count // LANES
    gx, gy = lax.axis_index("gx"), lax.axis_index("gy")
    first_x, last_x = gx == 0, gx == across - 1
    first_y, last_y = gy == 0, gy == down - 1
    width = (ey + 2) * ez
    tall = by + 8

    for i in range(bx):
        voltage = cells[0, i + 1, TOP : TOP + by]
        resting = rest_in[i]
        out_recovery[i] = resting + 0.05 * (-resting - 8.0 * voltage * (voltage - 1.15))
    leaving = [pltpu.make_async_copy(out_recovery, next_recovery, out_sem.at[bx])]
    leaving[0].start()

    gathered = []
    digits = lax.broadcasted_iota(jnp.int32, (LANES, width), 0)
    pages = down * blocks
    for q in range(3):
        low = jnp.where(first_y, near_slots[q, 1, 0, 0:1], near_slots[q, 0, 0, ey - 1 : ey])
        high = jnp.where(last_y, near_slots[q, 1, 0, ey - 1 : ey], near_slots[q, 2, 0, 0:1])
        pieces = [low] + [near_slots[q, 1, 0, c : c + 1] for c in range(ey)] + [high]
        index = jnp.concatenate(pieces, axis=1) - (gx + q - 1) * (down * count)
        chosen = (digits == (index & (LANES - 1))).astype(jnp.float32).astype(jnp.bfloat16)
        table = [held[q, h, 0 : 8 * blocks] for h in range(down)]
        table += [held[q, h, 8 * blocks : 9 * blocks] for h in range(down)]
        found = dot_two(jnp.concatenate(table, axis=0), chosen)
        page = index >> (LANES.bit_length() - 1)
        total = jnp.zeros((8, width), jnp.float32)
        for h in range(pages):
            total = jnp.where(page == h, found[8 * h : 8 * h + 8], total)
        last = found[8 * pages : 9 * pages]
        kept = lax.broadcasted_iota(jnp.int32, (pages, width), 0) == page
        last = jnp.sum(jnp.where(kept, last, 0.0), axis=0, keepdims=True)
        gathered.append([total, last])
    for part in range(2):
        gathered[0][part] = jnp.where(first_x, gathered[1][part], gathered[0][part])
        gathered[2][part] = jnp.where(last_x, gathered[1][part], gathered[2][part])

    refined = []
    weight_y = spread_y[...]
    weight_z = spread_z[...]
    for q in range(3):
        total, last = gathered[q]
        spread = [weight_y * total[k : k + 1] for k in range(8)] + [weight_y * last]
        refined.append(dot_two(jnp.concatenate(spread, axis=0), weight_z))

    volts[...] = cells[0, :, 0:by + 16]

    @pl.when(first_y)
    def _():
        volts[:, TOP - 1 : TOP] = volts[:, TOP : TOP + 1]

    @pl.when(last_y)
    def _():
        volts[:, TOP + by : TOP + by + 1] = volts[:, TOP + by - 1 : TOP + by]

    @pl.when(first_x)
    def _():
        volts[0] = volts[1]

    @pl.when(last_x)
    def _():
        volts[bx + 1] = volts[bx]

    def rim_of(number):
        rows = [cells[number, s + 1, row : row + 1] for row in (TOP - 1, TOP + by) for s in range(bx)]
        return jnp.concatenate(rows, axis=0)

    rim = [rim_of(1), rim_of(2)]
    rim_fiber = fiber_of(rim[0], rim[1])

    def hat(s):
        spot = (s + 0.5) / RATIO - 0.5
        return [max(0.0, 1.0 - abs(spot - (q - 1))) for q in range(3)]

    for s in range(bx + 2):
        weights = hat(s - 1)
        for half in range(by // 8):
            rows = slice(8 * half, 8 * half + 8)
            entries = []
            for k in range(parts):
                at = tall * k + 8 * half
                terms = [w * refined[q][at : at + 8] for q, w in enumerate(weights) if w]
                entries.append(functools.reduce(jnp.add, terms))
            if 1 <= s <= bx:
                fiber = [fibers[number, s - 1, rows] for number in range(3)]
            else:
                fiber = fiber_of(*(cells[number, s, TOP + 8 * half : TOP + 8 * half + 8] for number in (1, 2)))
            for number, value in enumerate(tensor_of(entries, fiber)):
                conducts[number, s, TOP + 8 * half : TOP + 8 * half + 8] = value
            if 1 <= s <= bx:
                out_potential[s - 1, rows] = stretch_of(entries, fiber)
    rim_row = lax.rem(lax.broadcasted_iota(jnp.int32, (2 * bx, nz), 0), bx).astype(jnp.float32)
    spot = (rim_row + 0.5) * (1.0 / RATIO) - 0.5
    rim_weights = [jnp.maximum(1.0 - jnp.abs(spot - (q - 1.0)), 0.0) for q in range(3)]
    entries = []
    for k in range(parts):
        at = tall * k + by
        entries.append(
            functools.reduce(
                jnp.add, [rim_weights[q] * refined[q][at : at + 2 * bx] for q in range(3)]
            )
        )
    for number, value in enumerate(tensor_of(entries, rim_fiber)):
        for s in range(bx):
            conducts[number, s + 1, TOP - 1 : TOP] = value[s : s + 1]
            conducts[number, s + 1, TOP + by : TOP + by + 1] = value[bx + s : bx + s + 1]

    z_lane = lax.broadcasted_iota(jnp.int32, (by, nz), 1)
    y_row = lax.broadcasted_iota(jnp.int32, (by, nz), 0)

    def next_z(values):
        return jnp.where(z_lane == nz - 1, values, pltpu.roll(values, nz - 1, 1))

    def last_z(values):
        return jnp.where(z_lane == 0, values, pltpu.roll(values, 1, 1))

    def grad_z(values):
        return next_z(values) - last_z(values)

    def at(s, shift):
        return volts[s, TOP + shift : TOP + shift + by]

    def tensor(number, s, shift=0):
        return conducts[number, s, TOP + shift : TOP + shift + by]

    XX, YY, ZZ, XY, XZ, YZ = range(6)
    middle = [at(s, 0) for s in range(bx + 2)]
    grads_y = [at(s, 1) - at(s, -1) for s in range(bx + 2)]
    grads_z = [grad_z(middle[s]) for s in range(bx + 2)]

    def face_x(f):
        def mean(number):
            return tensor(number, f) + tensor(number, f + 1)

        return (
            0.5 * mean(XX) * (middle[f + 1] - middle[f])
            + 0.125 * mean(XY) * (grads_y[f] + grads_y[f + 1])
            + 0.125 * mean(XZ) * (grads_z[f] + grads_z[f + 1])
        )

    faces = [face_x(f) for f in range(bx + 1)]
    faces[0] = jnp.where(first_x, 0.0, faces[0])
    faces[bx] = jnp.where(last_x, 0.0, faces[bx])

    for i in range(bx):
        s = i + 1
        grad_x = middle[s + 1] - middle[s - 1]

        def face_y(shift):
            def mean(number):
                return tensor(number, s) + tensor(number, s, shift)

            step = (at(s, shift) - middle[s]) * (1.0 if shift > 0 else -1.0)
            other_x = at(s + 1, shift) - at(s - 1, shift)
            return (
                0.125 * mean(XY) * (grad_x + other_x)
                + 0.5 * mean(YY) * step
                + 0.125 * mean(YZ) * (grads_z[s] + grad_z(at(s, shift)))
            )

        upper = jnp.where(jnp.logical_and(y_row == by - 1, last_y), 0.0, face_y(1))
        lower = jnp.where(jnp.logical_and(y_row == 0, first_y), 0.0, face_y(-1))

        def pair(values):
            return values + next_z(values)

        face_z = (
            0.125 * pair(tensor(XZ, s)) * pair(grad_x)
            + 0.125 * pair(tensor(YZ, s)) * pair(grads_y[s])
            + 0.5 * pair(tensor(ZZ, s)) * (next_z(middle[s]) - middle[s])
        )
        face_z = jnp.where(z_lane == nz - 1, 0.0, face_z)
        divergent = (
            (faces[i + 1] - faces[i]) + (upper - lower) + (face_z - pltpu.roll(face_z, 1, 1))
        )
        voltage = middle[s]
        resting = rest_in[i]
        current = 8.0 * voltage * (voltage - 0.15) * (voltage - 1.0) + voltage * resting
        current = current + 10.0 * jnp.maximum(out_potential[i] - 1.0, 0.0) * (voltage - 0.6)
        out_potential[i] = voltage + 0.1 * (divergent - current)
        copy = pltpu.make_async_copy(out_potential.at[i], next_potential.at[i], out_sem.at[i])
        copy.start()
        leaving.append(copy)
    for copy in leaving:
        copy.wait()


def solution(mesh):
    across, down = mesh.shape["gx"], mesh.shape["gy"]

    def local(potential, recovery, angles, deform, slots):
        bx, by, nz = potential.shape
        ex, ey, ez = slots.shape
        parts, count = deform.shape
        assert ex == 1 and bx == RATIO and by % 8 == 0 and count % LANES == 0 and parts == 9
        sizes = (bx, by, nz, ex, ey, ez, parts, count)
        blocks = count // LANES
        width = (ey + 2) * ez
        f32 = jnp.float32
        shape = jax.ShapeDtypeStruct(potential.shape, f32)
        anywhere = pl.BlockSpec(memory_space=pl.ANY)
        in_vmem = pl.BlockSpec(memory_space=pltpu.VMEM)
        passed = (
            pltpu.VMEM((3, bx + 2, by + 16, nz), f32),
            pltpu.VMEM(recovery.shape, f32),
            pltpu.VMEM((3, down, 8 * blocks + 8, LANES), f32),
            pltpu.VMEM((3, 3, ex, ey, ez), jnp.int32),
            pltpu.VMEM((3, bx, by, nz), f32),
            pltpu.VMEM((by + 8, width), f32),
            pltpu.VMEM((width, nz), jnp.bfloat16),
        )
        arrived = pl.pallas_call(
            functools.partial(exchange, across, down, sizes),
            out_shape=passed,
            in_specs=[pl.BlockSpec(memory_space=pltpu.MemorySpace.HBM)] * 5,
            out_specs=(in_vmem,) * len(passed),
            scratch_shapes=[
                pltpu.SemaphoreType.DMA((1,)),
                pltpu.SemaphoreType.DMA((3,)),
                pltpu.SemaphoreType.DMA((3,)),
                pltpu.SemaphoreType.DMA((2,)),
                pltpu.SemaphoreType.DMA((1,)),
                pltpu.SemaphoreType.DMA((2,)),
                pltpu.SemaphoreType.DMA((4,)),
            ],
            compiler_params=pltpu.CompilerParams(
                collective_id=0, has_side_effects=True, vmem_limit_bytes=VMEM_LIMIT
            ),
        )(*(pltpu.with_memory_space_constraint(x, pltpu.MemorySpace.HBM) for x in (potential, recovery, angles, deform, slots)))
        return pl.pallas_call(
            functools.partial(compute, across, down, sizes),
            out_shape=(shape, shape),
            in_specs=[in_vmem] * len(passed),
            out_specs=(anywhere,) * 2,
            scratch_shapes=[
                pltpu.VMEM((bx + 2, by + 16, nz), f32),
                pltpu.VMEM((6, bx + 2, by + 16, nz), f32),
                pltpu.VMEM((bx, by, nz), f32),
                pltpu.VMEM((bx, by, nz), f32),
                pltpu.SemaphoreType.DMA((bx + 1,)),
            ],
            compiler_params=pltpu.CompilerParams(vmem_limit_bytes=VMEM_LIMIT),
        )(*arrived)

    return jax.shard_map(
        local,
        mesh=mesh,
        in_specs=(
            P("gx", "gy", None),
            P("gx", "gy", None),
            P(None, "gx", "gy", None),
            P(None, ("gx", "gy")),
            P("gx", "gy", None),
        ),
        out_specs=(P("gx", "gy", None), P("gx", "gy", None)),
        check_vma=False,
    )
```

```python
import functools

import jax
import jax.numpy as jnp
from jax import lax
from jax.experimental import pallas as pl
from jax.experimental.pallas import tpu as pltpu
from jax.sharding import PartitionSpec as P

MESH = pl.DeviceIdType.MESH
RATIO = 4
LANES = 128
VMEM_LIMIT = 16 * 1024 * 1024
TOP = 8
WINDOW = 4
FIBER_SCALE = (7.0 / 3.0) ** 0.5
STRETCH_SCALE = (3.0 / 7.0) ** 0.5
XX, YY, ZZ, XY, XZ, YZ = range(6)
PAIRS = ((0, 0), (1, 1), (2, 2), (0, 1), (0, 2), (1, 2))


def split_two(values):
    high = values.astype(jnp.bfloat16)
    low = (values - high.astype(jnp.float32)).astype(jnp.bfloat16)
    return high, low


def dot_two(values, weights):
    high, low = split_two(values)
    return jnp.dot(high, weights, preferred_element_type=jnp.float32) + jnp.dot(
        low, weights, preferred_element_type=jnp.float32
    )


def sine_cosine(angle):
    turn = jnp.floor(angle * 0.6366197723675814 + 0.5)
    rest = angle - turn * 1.5703125
    rest = rest - turn * 4.8375129699707031e-4
    rest = rest - turn * 7.549789948768648e-8
    square = rest * rest
    sine = rest + rest * square * (
        -1.6666654611e-1 + square * (8.3321608736e-3 + square * -1.9515295891e-4)
    )
    cosine = (
        1.0
        - 0.5 * square
        + square
        * square
        * (4.166664568298827e-2 + square * (-1.388731625493765e-3 + square * 2.443315711809948e-5))
    )
    size = jnp.abs(turn)
    odd = size == 1.0
    sine_part = jnp.where(odd, cosine * turn, sine)
    cosine_part = jnp.where(odd, sine * -turn, cosine)
    flip = jnp.where(size == 2.0, -1.0, 1.0)
    return sine_part * flip, cosine_part * flip


def fiber_of(azimuth, elevation):
    sin_u, cos_u = sine_cosine(azimuth)
    sin_e, cos_e = sine_cosine(elevation)
    flat = FIBER_SCALE * cos_e
    return cos_u * flat, sin_u * flat, FIBER_SCALE * sin_e


def tensor_of(entries, fiber, sign, wanted):
    def element(i, j):
        return entries[3 * (i % 3) + j % 3]

    adjugate = [
        [
            element(j + 1, i + 1) * element(j + 2, i + 2)
            - element(j + 1, i + 2) * element(j + 2, i + 1)
            for j in range(3)
        ]
        for i in range(3)
    ]
    determinant = (
        element(0, 0) * adjugate[0][0]
        + element(0, 1) * adjugate[1][0]
        + element(0, 2) * adjugate[2][0]
    )
    inverse = 1.0 / determinant
    square = inverse * inverse
    diagonal = (0.3 * 0.5) * square
    mixed = (0.3 * 0.125) * square
    mirrored = (0.3 * 0.125 * sign) * square
    rows = sorted({i for number in wanted for i in PAIRS[number]})
    pulled = {
        i: adjugate[i][0] * fiber[0] + adjugate[i][1] * fiber[1] + adjugate[i][2] * fiber[2]
        for i in rows
    }
    scale = {XX: diagonal, YY: diagonal, ZZ: diagonal, XY: mirrored, XZ: mirrored, YZ: mixed}
    conduct = {}
    for number in wanted:
        i, j = PAIRS[number]
        metric = (
            adjugate[i][0] * adjugate[j][0]
            + adjugate[i][1] * adjugate[j][1]
            + adjugate[i][2] * adjugate[j][2]
        )
        conduct[number] = scale[number] * (metric + pulled[i] * pulled[j])
    return conduct


def excess_of(entries, fiber):
    parts = [
        entries[3 * i] * fiber[0] + entries[3 * i + 1] * fiber[1] + entries[3 * i + 2] * fiber[2]
        for i in range(3)
    ]
    square = parts[0] * parts[0] + parts[1] * parts[1] + parts[2] * parts[2]
    return jnp.maximum(STRETCH_SCALE * (square * lax.rsqrt(square)) - 1.0, 0.0)


class Place:
    def __init__(self, across, down, sizes):
        self.across, self.down, self.sizes = across, down, sizes
        self.gx, self.gy = lax.axis_index("gx"), lax.axis_index("gy")
        self.first_x, self.last_x = self.gx == 0, self.gx == across - 1
        self.first_y, self.last_y = self.gy == 0, self.gy == down - 1
        odd = lax.rem(self.gx, 2)
        self.odd, self.even = odd == 1, odd == 0
        self.leave = 2 * odd - 1
        self.leaves = jnp.logical_not(jnp.logical_or(self.first_x, self.last_x))
        self.late = jnp.where(self.leaves, self.leave, -self.leave)
        self.sign = jnp.where(self.late > 0, 1.0, -1.0)

    def slab(self, j):
        last = self.sizes[0] + 1
        return jnp.where(self.late > 0, j, last - j)


def gather_index(place, near_slots, q, offset):
    ey = place.sizes[4]
    low = jnp.where(place.first_y, near_slots[q, 1, 0, 0:1], near_slots[q, 0, 0, ey - 1 : ey])
    high = jnp.where(place.last_y, near_slots[q, 1, 0, ey - 1 : ey], near_slots[q, 2, 0, 0:1])
    pieces = [low] + [near_slots[q, 1, 0, c : c + 1] for c in range(ey)] + [high]
    count = place.sizes[7]
    return jnp.concatenate(pieces, axis=1) - (place.gx + offset) * (place.down * count)


def gather_row(place, held, q, index):
    blocks = place.sizes[7] // LANES
    pages = place.down * blocks
    width = index.shape[1]
    digits = lax.broadcasted_iota(jnp.int32, (LANES, width), 0)
    chosen = (digits == (index & (LANES - 1))).astype(jnp.float32).astype(jnp.bfloat16)
    table = [held[q, h, 0 : 8 * blocks] for h in range(place.down)]
    table += [held[q, h, 8 * blocks : 9 * blocks] for h in range(place.down)]
    found = dot_two(jnp.concatenate(table, axis=0), chosen)
    page = index >> (LANES.bit_length() - 1)
    total = jnp.zeros((8, width), jnp.float32)
    for h in range(pages):
        total = jnp.where(page == h, found[8 * h : 8 * h + 8], total)
    last = found[8 * pages : 9 * pages]
    kept = lax.broadcasted_iota(jnp.int32, (pages, width), 0) == page
    return total, jnp.sum(jnp.where(kept, last, 0.0), axis=0, keepdims=True)


def refine_row(place, row, weight_y, weight_z):
    by, ez = place.sizes[1], place.sizes[5]
    total, last = row
    span = WINDOW * ez
    spread = []
    for k in range(9):
        values = total[k : k + 1] if k < 8 else last
        for half in range(by // 8):
            at = 2 * half * ez
            spread.append(weight_y[8 * half : 8 * half + 8] * values[:, at : at + span])
        at = (by // 4 - 2) * ez
        rim = lax.broadcasted_iota(jnp.int32, (8, span), 0) < 4
        spread.append(weight_y[by : by + 8] * jnp.where(rim, values[:, 0:span], values[:, at : at + span]))
    return dot_two(jnp.concatenate(spread, axis=0), weight_z)


def rolls(nz, by):
    lane = lax.broadcasted_iota(jnp.int32, (by, nz), 1)

    def ahead(values):
        return pltpu.roll(values, nz - 1, 1)

    def behind(values):
        return pltpu.roll(values, 1, 1)

    return lane, ahead, behind


def grad_z(values):
    nz = values.shape[1]
    lane, ahead, behind = rolls(nz, values.shape[0])
    upper = jnp.where(lane == nz - 1, values, ahead(values))
    lower = jnp.where(lane == 0, values, behind(values))
    return upper - lower


def make_flux(place, volts, slopes, conducts, first):
    by, nz = place.sizes[1], place.sizes[2]
    lane, ahead, behind = rolls(nz, by)
    y_row = lax.broadcasted_iota(jnp.int32, (by, nz), 0)

    def volt(j, shift=0):
        return volts[j, TOP + shift : TOP + shift + by]

    def slope_z(j, shift=0):
        return slopes[j, TOP + shift : TOP + shift + by]

    def tensor(number, j, shift=0):
        return conducts[number, j - first, TOP + shift : TOP + shift + by]

    def slope_y(j):
        return volt(j, 1) - volt(j, -1)

    def slope_x(j, shift=0):
        return volt(j + 1, shift) - volt(j - 1, shift)

    def face_x(j, mine, next_one):
        return (
            (mine[0] + next_one[0]) * (volt(j + 1) - volt(j))
            + (mine[1] + next_one[1]) * (slope_y(j) + slope_y(j + 1))
            + (mine[2] + next_one[2]) * (slope_z(j) + slope_z(j + 1))
        )

    def face_y(j, shift):
        def mean(number):
            return tensor(number, j) + tensor(number, j, shift)

        step = volt(j, shift) - volt(j) if shift > 0 else volt(j) - volt(j, shift)
        return (
            mean(XY) * (slope_x(j) + slope_x(j, shift))
            + mean(YY) * step
            + mean(YZ) * (slope_z(j) + slope_z(j, shift))
        )

    def across_yz(j):
        upper = jnp.where(jnp.logical_and(y_row == by - 1, place.last_y), 0.0, face_y(j, 1))
        lower = jnp.where(jnp.logical_and(y_row == 0, place.first_y), 0.0, face_y(j, -1))

        def pair(values):
            return values + ahead(values)

        face_z = (
            pair(tensor(XZ, j)) * pair(slope_x(j))
            + pair(tensor(YZ, j)) * pair(slope_y(j))
            + pair(tensor(ZZ, j)) * (ahead(volt(j)) - volt(j))
        )
        face_z = jnp.where(lane == nz - 1, 0.0, face_z)
        return (upper - lower) + (face_z - behind(face_z))

    def x_parts(j):
        return [tensor(number, j) for number in (XX, XY, XZ)]

    return face_x, across_yz, x_parts


def put_tensors(place, conducts, slot, mid, side, weight, fiber_at, halo, note):
    by = place.sizes[1]
    tall = by + 8
    for half in range(by // 8):
        rows = slice(8 * half, 8 * half + 8)
        entries = []
        for k in range(9):
            at = tall * k + 8 * half
            base = mid(at)
            entries.append(base + weight * (side(at) - base))
        fiber = fiber_at(rows)
        wanted = (XX, XY, XZ) if halo else tuple(range(6))
        for number, value in tensor_of(entries, fiber, place.sign, wanted).items():
            conducts[number, slot, TOP + 8 * half : TOP + 8 * half + 8] = value
        if not halo:
            note(rows, excess_of(entries, fiber))


def put_rims(place, conducts, slabs, mid, side, rim_fiber):
    bx, by, nz = place.sizes[:3]
    tall = by + 8
    row = lax.rem(lax.broadcasted_iota(jnp.int32, (8, nz), 0), bx)
    weight = jnp.zeros((8, nz), jnp.float32)
    for j in slabs.values():
        weight = jnp.where(row == j - 1, abs((j - 0.5) / RATIO - 0.5), weight)
    entries = []
    for k in range(9):
        base = mid(tall * k + by)
        entries.append(base + weight * (side(tall * k + by) - base))
    for number, value in tensor_of(entries, rim_fiber, place.sign, (YY, XY, YZ)).items():
        for slot, j in slabs.items():
            conducts[number, slot, TOP - 1 : TOP] = value[j - 1 : j]
            conducts[number, slot, TOP + by : TOP + by + 1] = value[bx + j - 1 : bx + j]


def put_volts(place, cells, volts, slopes, j):
    by = place.sizes[1]
    spot = place.slab(j)
    own = cells[0, spot, TOP : TOP + by]
    volts[j, TOP : TOP + by] = own
    low, high = cells[0, spot, TOP - 1 : TOP], cells[0, spot, TOP + by : TOP + by + 1]
    volts[j, TOP - 1 : TOP] = jnp.where(place.first_y, own[0:1], low)
    volts[j, TOP + by : TOP + by + 1] = jnp.where(place.last_y, own[by - 1 : by], high)


def exchange(
    across,
    down,
    sizes,
    potential,
    recovery,
    angles,
    deform,
    slots,
    cells,
    held,
    near_slots,
    fibers,
    rim_fibers,
    spread_y,
    spread_z,
    refined,
    volts,
    slopes,
    edge_tensor,
    partial,
    base,
    next_recovery,
    rest_in,
    conducts,
    early_refined,
    send_sem,
    deform_sem,
    slot_sem,
    side_sem,
    edge_sem,
    corner_sem,
    local_sem,
    plane_sem,
    above_sem,
):
    bx, by, nz, ex, ey, ez, parts, count = sizes
    blocks = count // LANES
    place = Place(across, down, sizes)
    gx, gy = place.gx, place.gy
    first_y, last_y, odd, even, leave = place.first_y, place.last_y, place.odd, place.even, place.leave
    sides = ((leave, place.leaves), (-leave, None))

    def when(check, act):
        if check is None:
            act()
        else:
            pl.when(check)(act)

    def row_targets(include_self=True):
        for mask in sorted(range(down), key=lambda m: (-m.bit_count(), m)):
            if mask == 0 and not include_self:
                continue
            if down & (down - 1):
                yield lax.rem(gy + mask, down)
            else:
                target = gy
                for bit in range(down.bit_length() - 1):
                    if mask >> bit & 1:
                        step = 1 << bit
                        target = target + step - 2 * step * lax.rem(gy // step, 2)
                yield target

    barrier = pltpu.get_barrier_semaphore()

    def tell(sem, row, target):
        pl.semaphore_signal(sem, inc=1, device_id=(row, target), device_id_type=MESH)

    @pl.when(odd)
    def _():
        for target in row_targets(False):
            tell(barrier, gx, target)

        @pl.when(place.leaves)
        def _():
            for target in row_targets():
                tell(barrier, gx + 1, target)

        tell(barrier, gx - 1, gy)

    @pl.when(even)
    def _():
        for target in row_targets():
            tell(barrier, gx + 1, target)

    packed = held.at[1, gy]
    for b in range(blocks):
        columns = pl.ds(b * LANES, LANES)
        pltpu.make_async_copy(
            deform.at[pl.ds(0, 8), columns], packed.at[pl.ds(8 * b, 8)], local_sem.at[0]
        ).start()
        pltpu.make_async_copy(
            deform.at[pl.ds(8, 1), columns], packed.at[pl.ds(8 * blocks + b, 1)], local_sem.at[0]
        ).start()
    inside = pl.ds(TOP, by)
    get_slots = pltpu.make_async_copy(slots, near_slots.at[1, 1], local_sem.at[1])
    get_slots.start()
    own_cells = cells.at[:, pl.ds(1, bx), inside]
    pltpu.make_async_copy(potential, cells.at[0, pl.ds(1, bx), inside], local_sem.at[2]).start()
    pltpu.make_async_copy(angles, cells.at[pl.ds(1, 2), pl.ds(1, bx), inside], local_sem.at[2]).start()
    get_rest = pltpu.make_async_copy(recovery, rest_in, local_sem.at[3])
    get_rest.start()

    def drain(ref, sem):
        pltpu.make_async_copy(ref, ref, sem).wait()

    pl.semaphore_wait(barrier, jnp.where(odd, 2 * down - 1, jnp.where(gx > 0, down + 1, 1)))

    @pl.when(odd)
    def _():
        tell(plane_sem, gx - 1, gy)

    @pl.when(jnp.logical_and(even, place.leaves))
    def _():
        for target in row_targets():
            tell(above_sem, gx - 1, target)

    rows = pl.ds(0, 9 * blocks)
    drain(held.at[1, gy, rows], local_sem.at[0])

    def put(source, target, sem, dx, where):
        pltpu.make_async_remote_copy(
            src_ref=source,
            dst_ref=target,
            send_sem=send_sem.at[0],
            recv_sem=sem,
            device_id=(gx + dx, where),
            device_id_type=MESH,
        ).start()

    def at_y(dy, act):
        pl.when(jnp.logical_not(first_y if dy < 0 else last_y))(act)

    def send_deform(dx):
        q = 1 - dx
        for target in row_targets(not isinstance(dx, int)):
            put(held.at[1, gy, rows], held.at[q, gy, rows], deform_sem.at[q], dx, target)

    def send_slots(dx):
        q = 1 - dx

        def one(dy):
            put(near_slots.at[1, 1], near_slots.at[q, 1 - dy], slot_sem.at[q], dx, gy + dy)

        if not isinstance(dx, int):
            one(0)
        for dy in (-1, 1):
            at_y(dy, functools.partial(one, dy))

    def edges(dy):
        source = pl.ds(TOP if dy < 0 else TOP + by - 1, 1)
        target = pl.ds(TOP + by if dy < 0 else TOP - 1, 1)
        return source, target

    def send_side(dx):
        q = 1 - dx
        x_source = pl.ds(jnp.where(dx < 0, 1, bx), 1)
        x_target = pl.ds(jnp.where(dx < 0, bx + 1, 0), 1)
        put(cells.at[:, x_source, inside], cells.at[:, x_target, inside], side_sem.at[q // 2], dx, gy)

        def corner(dy):
            y_source, y_target = edges(dy)
            source = cells.at[pl.ds(0, 1), x_source, y_source]
            put(source, cells.at[pl.ds(0, 1), x_target, y_target], corner_sem.at[q // 2], dx, gy + dy)

        for dy in (-1, 1):
            at_y(dy, functools.partial(corner, dy))

    def send_edge(dy):
        y_source, y_target = edges(dy)
        x_here = pl.ds(1, bx)
        put(cells.at[:, x_here, y_source], cells.at[:, x_here, y_target], edge_sem.at[0], 0, gy + dy)

    def send_plane():
        send_deform(-leave)
        send_deform(0)
        send_slots(-leave)
        send_slots(0)

    def send_plane_cells():
        send_side(-leave)
        for dy in (-1, 1):
            at_y(dy, functools.partial(send_edge, dy))

    def send_leave():
        send_deform(leave)
        send_slots(leave)

    def local_work():
        width = WINDOW * ez
        row = lax.broadcasted_iota(jnp.int32, (by + 8, width), 0)
        lane = lax.broadcasted_iota(jnp.int32, (by + 8, width), 1)
        low = row < by + bx
        cell = jnp.where(row < by, row, jnp.where(low, -1, by))
        start = jnp.where(row < by, 2 * (row // 8), jnp.where(low, 0, ey - 2))
        spot = (cell.astype(jnp.float32) + 0.5) * (1.0 / RATIO) - 0.5
        coarse = (lane // ez + start - 1).astype(jnp.float32)
        spread_y[...] = jnp.maximum(1.0 - jnp.abs(spot - coarse), 0.0)
        row = lax.broadcasted_iota(jnp.int32, (width, nz), 0)
        lane = lax.broadcasted_iota(jnp.int32, (width, nz), 1)
        spot = jnp.clip((lane.astype(jnp.float32) + 0.5) * (1.0 / RATIO) - 0.5, 0.0, ez - 1.0)
        weight = jnp.maximum(1.0 - jnp.abs(spot - lax.rem(row, ez).astype(jnp.float32)), 0.0)
        spread_z[...] = weight.astype(jnp.bfloat16)
        for s in range(bx):
            own = [cells[number, s + 1, TOP : TOP + by] for number in (1, 2)]
            for number, part in enumerate(fiber_of(*own)):
                fibers[number, s] = part
            voltage = cells[0, s + 1, TOP : TOP + by]
            resting = rest_in[s]
            next_recovery[s] = resting + 0.05 * (-resting - 8.0 * voltage * (voltage - 1.15))
            current = 8.0 * voltage * (voltage - 0.15) * (voltage - 1.0) + voltage * resting
            base[s] = voltage - 0.1 * current

    def stage_odd():
        send_deform(-leave)
        send_deform(0)
        get_slots.wait()
        send_slots(-leave)
        send_slots(0)
        drain(own_cells, local_sem.at[2])
        send_plane_cells()
        get_rest.wait()
        local_work()

        @pl.when(place.leaves)
        def _():
            pl.semaphore_wait(above_sem, down)
            send_leave()
            send_side(leave)

    def stage_even():
        pl.when(place.leaves)(functools.partial(send_deform, leave))
        get_slots.wait()
        pl.when(place.leaves)(functools.partial(send_slots, leave))
        pl.semaphore_wait(plane_sem, 1)
        send_plane()
        drain(own_cells, local_sem.at[2])
        pl.when(place.leaves)(functools.partial(send_side, leave))
        send_plane_cells()
        get_rest.wait()
        local_work()

    pl.when(odd)(stage_odd)
    pl.when(even)(stage_even)

    middle_y = jnp.logical_not(jnp.logical_or(first_y, last_y))
    some_y = jnp.logical_xor(first_y, last_y)

    def over_y(act):
        pl.when(middle_y)(functools.partial(act, 2))
        pl.when(some_y)(functools.partial(act, 1))

    def wait_deform(sem, q, others=0):
        drain(held.at[q, pl.ds(0, down - others), rows], deform_sem.at[q] if sem is None else sem)

    def wait_slots(sem, q, straight=1):
        sem = slot_sem.at[q] if sem is None else sem
        if down == 1:
            if straight:
                drain(near_slots.at[1, pl.ds(0, 1)], sem)
        else:
            over_y(lambda n: drain(near_slots.at[1, pl.ds(0, n + straight)], sem))

    def wait_side(sem, q):
        drain(cells.at[:, pl.ds(0, 1), inside], side_sem.at[q // 2] if sem is None else sem)
        sem = corner_sem.at[q // 2] if sem is None else sem
        over_y(lambda n: drain(cells.at[pl.ds(0, 1), pl.ds(0, 1), pl.ds(0, n)], sem))

    def wait_edge(sem):
        over_y(lambda n: drain(cells.at[:, pl.ds(1, bx), pl.ds(0, n)], sem))

    late = 1 + place.late
    early = 1 - place.late

    def wait_early():
        wait_slots(None, early)
        wait_deform(None, early)
        wait_side(None, early)

    wait_slots(None, 1, 0)
    wait_edge(edge_sem.at[0])
    wait_deform(None, 1, 1)
    pl.when(place.leaves)(wait_early)

    weight_y, weight_z = spread_y[...], spread_z[...]
    middle_row = gather_row(place, held, 1, gather_index(place, near_slots, 1, 0))
    early_row = gather_row(place, held, early, gather_index(place, near_slots, early, -place.late))
    early_row = [jnp.where(place.leaves, a, b) for a, b in zip(early_row, middle_row)]
    refined[...] = refine_row(place, middle_row, weight_y, weight_z)
    early_refined[...] = refine_row(place, early_row, weight_y, weight_z)

    for j in range(bx + 1):
        put_volts(place, cells, volts, slopes, j)

    @pl.when(jnp.logical_not(place.leaves))
    def _():
        volts[0] = volts[1]

    for j in range(bx + 1):
        slopes[j] = grad_z(volts[j])

    def rim_of(number):
        pieces = [cells[number, place.slab(j), row : row + 1] for row in (TOP - 1, TOP + by) for j in range(1, bx + 1)]
        return jnp.concatenate(pieces, axis=0)

    rim_fiber = fiber_of(rim_of(1), rim_of(2))
    for number, value in enumerate(rim_fiber):
        rim_fibers[number] = value

    def mid(at):
        return refined[at : at + 8]

    def side(at):
        return early_refined[at : at + 8]

    half = RATIO // 2
    for j in range(half + 1):
        spot = place.slab(j)

        def fiber_at(rows, j=j, spot=spot):
            if j:
                return [fibers[number, spot - 1, rows] for number in range(3)]
            start = TOP + rows.start
            return fiber_of(*(cells[number, spot, start : start + 8] for number in (1, 2)))

        def note(rows, excess, j=j, spot=spot):
            voltage = volts[j, TOP + rows.start : TOP + rows.stop]
            partial[j - 1, rows] = base[spot - 1, rows] - excess * (voltage - 0.6)

        weight = abs((j - 0.5) / RATIO - 0.5)
        put_tensors(place, conducts, j, mid, side, weight, fiber_at, j == 0, note)
    put_rims(place, conducts, {j: j for j in range(1, half + 1)}, mid, side, rim_fiber)
    face_x, across_yz, x_parts = make_flux(place, volts, slopes, conducts, 0)
    faces = [face_x(j, x_parts(j), x_parts(j + 1)) for j in range(half)]
    faces[0] = jnp.where(place.leaves, faces[0], 0.0)
    partial[0] = partial[0] + 0.1 * (across_yz(1) + (faces[1] - faces[0]))
    partial[1] = partial[1] + 0.1 * (across_yz(2) - faces[1])
    for number, value in enumerate(x_parts(half)):
        edge_tensor[number] = value

    wait_slots(None, late)
    wait_deform(None, late)
    wait_side(None, late)
    out = send_sem.at[0]
    for dx, there in sides:
        when(there, functools.partial(wait_deform, out, 1 - dx))
    wait_deform(out, 1, 1)
    for dx, there in sides:
        when(there, functools.partial(wait_slots, out, 1 - dx))
    wait_slots(out, 1, 0)
    for dx, there in sides:
        when(there, functools.partial(wait_side, out, 1 - dx))
    wait_edge(out)


def compute(
    across,
    down,
    sizes,
    cells,
    held,
    near_slots,
    fibers,
    rim_fibers,
    spread_y,
    spread_z,
    refined,
    volts_in,
    slopes_in,
    edge_tensor,
    partial,
    base,
    recovered,
    next_potential,
    next_recovery,
    volts,
    slopes,
    conducts,
    late_refined,
    result,
    out_sem,
):
    bx, by, nz, ex, ey, ez, parts, count = sizes
    place = Place(across, down, sizes)
    half = RATIO // 2
    late = 1 + place.late

    leaving = [pltpu.make_async_copy(recovered, next_recovery, out_sem.at[0])]
    leaving[0].start()

    def finish(j, source):
        copy = pltpu.make_async_copy(source, next_potential.at[place.slab(j) - 1], out_sem.at[j])
        copy.start()
        leaving.append(copy)

    finish(1, partial.at[0])

    row = gather_row(place, held, late, gather_index(place, near_slots, late, place.late))
    late_refined[...] = refine_row(place, row, spread_y[...], spread_z[...])

    for j in range(half - 1, bx + 1):
        volts[j] = volts_in[j]
        slopes[j] = slopes_in[j]
    put_volts(place, cells, volts, slopes, bx + 1)
    slopes[bx + 1] = grad_z(volts[bx + 1])

    def mid(at):
        return refined[at : at + 8]

    def side(at):
        return late_refined[at : at + 8]

    for j in range(half + 1, bx + 2):
        spot = place.slab(j)

        def fiber_at(rows, j=j, spot=spot):
            if j <= bx:
                return [fibers[number, spot - 1, rows] for number in range(3)]
            start = TOP + rows.start
            return fiber_of(*(cells[number, spot, start : start + 8] for number in (1, 2)))

        def note(rows, excess, j=j, spot=spot):
            voltage = volts[j, TOP + rows.start : TOP + rows.stop]
            result[j - half, rows] = base[spot - 1, rows] - excess * (voltage - 0.6)

        weight = abs((j - 0.5) / RATIO - 0.5)
        put_tensors(place, conducts, j - half - 1, mid, side, weight, fiber_at, j == bx + 1, note)
    rim_fiber = [rim_fibers[number] for number in range(3)]
    put_rims(place, conducts, {j - half - 1: j for j in range(half + 1, bx + 1)}, mid, side, rim_fiber)
    face_x, across_yz, x_parts = make_flux(place, volts, slopes, conducts, half + 1)
    edge = [edge_tensor[number] for number in range(3)]
    faces = {}
    for j in range(half, bx + 1):
        faces[j] = face_x(j, edge if j == half else x_parts(j), x_parts(j + 1))
    result[0] = partial[1] + 0.1 * faces[half]
    finish(half, result.at[0])
    for j in range(half + 1, bx + 1):
        result[j - half] = result[j - half] + 0.1 * (across_yz(j) + (faces[j] - faces[j - 1]))
        finish(j, result.at[j - half])
    for copy in leaving:
        copy.wait()


def solution(mesh):
    across, down = mesh.shape["gx"], mesh.shape["gy"]

    def local(potential, recovery, angles, deform, slots):
        bx, by, nz = potential.shape
        ex, ey, ez = slots.shape
        parts, count = deform.shape
        assert ex == 1 and bx == RATIO and by == RATIO * ey and by % 8 == 0
        assert count % LANES == 0 and parts == 9 and across % 2 == 0 and (2 * ez) % LANES == 0
        sizes = (bx, by, nz, ex, ey, ez, parts, count)
        blocks = count // LANES
        f32 = jnp.float32
        half = RATIO // 2
        shape = jax.ShapeDtypeStruct(potential.shape, f32)
        anywhere = pl.BlockSpec(memory_space=pl.ANY)
        in_vmem = pl.BlockSpec(memory_space=pltpu.VMEM)
        passed = (
            pltpu.VMEM((3, bx + 2, by + 16, nz), f32),
            pltpu.VMEM((3, down, 8 * blocks + 8, LANES), f32),
            pltpu.VMEM((3, 3, ex, ey, ez), jnp.int32),
            pltpu.VMEM((3, bx, by, nz), f32),
            pltpu.VMEM((3, 2 * bx, nz), f32),
            pltpu.VMEM((by + 8, WINDOW * ez), f32),
            pltpu.VMEM((WINDOW * ez, nz), jnp.bfloat16),
            pltpu.VMEM((9 * (by + 8), nz), f32),
            pltpu.VMEM((bx + 1, by + 16, nz), f32),
            pltpu.VMEM((bx + 1, by + 16, nz), f32),
            pltpu.VMEM((3, by, nz), f32),
            pltpu.VMEM((half, by, nz), f32),
            pltpu.VMEM((bx, by, nz), f32),
            pltpu.VMEM((bx, by, nz), f32),
        )
        arrived = pl.pallas_call(
            functools.partial(exchange, across, down, sizes),
            out_shape=passed,
            in_specs=[pl.BlockSpec(memory_space=pltpu.MemorySpace.HBM)] * 5,
            out_specs=(in_vmem,) * len(passed),
            scratch_shapes=[
                pltpu.VMEM(recovery.shape, f32),
                pltpu.VMEM((6, half + 1, by + 16, nz), f32),
                pltpu.VMEM((9 * (by + 8), nz), f32),
                pltpu.SemaphoreType.DMA((1,)),
                pltpu.SemaphoreType.DMA((3,)),
                pltpu.SemaphoreType.DMA((3,)),
                pltpu.SemaphoreType.DMA((2,)),
                pltpu.SemaphoreType.DMA((1,)),
                pltpu.SemaphoreType.DMA((2,)),
                pltpu.SemaphoreType.DMA((4,)),
                pltpu.SemaphoreType.REGULAR,
                pltpu.SemaphoreType.REGULAR,
            ],
            compiler_params=pltpu.CompilerParams(
                collective_id=0, has_side_effects=True, vmem_limit_bytes=VMEM_LIMIT
            ),
        )(*(pltpu.with_memory_space_constraint(x, pltpu.MemorySpace.HBM) for x in (potential, recovery, angles, deform, slots)))
        return pl.pallas_call(
            functools.partial(compute, across, down, sizes),
            out_shape=(shape, shape),
            in_specs=[in_vmem] * len(passed),
            out_specs=(anywhere,) * 2,
            scratch_shapes=[
                pltpu.VMEM((bx + 2, by + 16, nz), f32),
                pltpu.VMEM((bx + 2, by + 16, nz), f32),
                pltpu.VMEM((6, half + 1, by + 16, nz), f32),
                pltpu.VMEM((9 * (by + 8), nz), f32),
                pltpu.VMEM((half + 1, by, nz), f32),
                pltpu.SemaphoreType.DMA((bx + 1,)),
            ],
            compiler_params=pltpu.CompilerParams(vmem_limit_bytes=VMEM_LIMIT),
        )(*arrived)

    return jax.shard_map(
        local,
        mesh=mesh,
        in_specs=(
            P("gx", "gy", None),
            P("gx", "gy", None),
            P(None, "gx", "gy", None),
            P(None, ("gx", "gy")),
            P("gx", "gy", None),
        ),
        out_specs=(P("gx", "gy", None), P("gx", "gy", None)),
        check_vma=False,
    )
```

```python
import functools

import jax
import jax.numpy as jnp
from jax import lax
from jax.experimental import pallas as pl
from jax.experimental.pallas import tpu as pltpu
from jax.sharding import PartitionSpec as P

MESH = pl.DeviceIdType.MESH
RATIO = 4
LANES = 128
VMEM_LIMIT = 16 * 1024 * 1024
TOP = 8
WINDOW = 4
FIBER_SCALE = (7.0 / 3.0) ** 0.5
STRETCH_SCALE = (3.0 / 7.0) ** 0.5
XX, YY, ZZ, XY, XZ, YZ = range(6)
PAIRS = ((0, 0), (1, 1), (2, 2), (0, 1), (0, 2), (1, 2))


def split_two(values):
    high = values.astype(jnp.bfloat16)
    low = (values - high.astype(jnp.float32)).astype(jnp.bfloat16)
    return high, low


def dot_two(values, weights):
    high, low = split_two(values)
    return jnp.dot(high, weights, preferred_element_type=jnp.float32) + jnp.dot(
        low, weights, preferred_element_type=jnp.float32
    )


def sine_cosine(angle):
    turn = jnp.floor(angle * 0.6366197723675814 + 0.5)
    rest = angle - turn * 1.5703125
    rest = rest - turn * 4.8375129699707031e-4
    rest = rest - turn * 7.549789948768648e-8
    square = rest * rest
    sine = rest + rest * square * (
        -1.6666654611e-1 + square * (8.3321608736e-3 + square * -1.9515295891e-4)
    )
    cosine = (
        1.0
        - 0.5 * square
        + square
        * square
        * (4.166664568298827e-2 + square * (-1.388731625493765e-3 + square * 2.443315711809948e-5))
    )
    size = jnp.abs(turn)
    odd = size == 1.0
    sine_part = jnp.where(odd, cosine * turn, sine)
    cosine_part = jnp.where(odd, sine * -turn, cosine)
    flip = jnp.where(size == 2.0, -1.0, 1.0)
    return sine_part * flip, cosine_part * flip


def fiber_of(azimuth, elevation):
    sin_u, cos_u = sine_cosine(azimuth)
    sin_e, cos_e = sine_cosine(elevation)
    flat = FIBER_SCALE * cos_e
    return cos_u * flat, sin_u * flat, FIBER_SCALE * sin_e


def tensor_of(entries, fiber, sign, wanted):
    def element(i, j):
        return entries[3 * (i % 3) + j % 3]

    adjugate = [
        [
            element(j + 1, i + 1) * element(j + 2, i + 2)
            - element(j + 1, i + 2) * element(j + 2, i + 1)
            for j in range(3)
        ]
        for i in range(3)
    ]
    determinant = (
        element(0, 0) * adjugate[0][0]
        + element(0, 1) * adjugate[1][0]
        + element(0, 2) * adjugate[2][0]
    )
    inverse = 1.0 / determinant
    square = inverse * inverse
    diagonal = (0.3 * 0.5) * square
    mixed = (0.3 * 0.125) * square
    mirrored = (0.3 * 0.125 * sign) * square
    rows = sorted({i for number in wanted for i in PAIRS[number]})
    pulled = {
        i: adjugate[i][0] * fiber[0] + adjugate[i][1] * fiber[1] + adjugate[i][2] * fiber[2]
        for i in rows
    }
    scale = {XX: diagonal, YY: diagonal, ZZ: diagonal, XY: mirrored, XZ: mirrored, YZ: mixed}
    conduct = {}
    for number in wanted:
        i, j = PAIRS[number]
        metric = (
            adjugate[i][0] * adjugate[j][0]
            + adjugate[i][1] * adjugate[j][1]
            + adjugate[i][2] * adjugate[j][2]
        )
        conduct[number] = scale[number] * (metric + pulled[i] * pulled[j])
    return conduct


def excess_of(entries, fiber):
    parts = [
        entries[3 * i] * fiber[0] + entries[3 * i + 1] * fiber[1] + entries[3 * i + 2] * fiber[2]
        for i in range(3)
    ]
    square = parts[0] * parts[0] + parts[1] * parts[1] + parts[2] * parts[2]
    return jnp.maximum(STRETCH_SCALE * (square * lax.rsqrt(square)) - 1.0, 0.0)


class Place:
    def __init__(self, across, down, sizes):
        self.across, self.down, self.sizes = across, down, sizes
        self.gx, self.gy = lax.axis_index("gx"), lax.axis_index("gy")
        self.first_x, self.last_x = self.gx == 0, self.gx == across - 1
        self.first_y, self.last_y = self.gy == 0, self.gy == down - 1
        odd = lax.rem(self.gx, 2)
        self.leave = 2 * odd - 1
        self.leaves = jnp.logical_not(jnp.logical_or(self.first_x, self.last_x))
        self.late = jnp.where(self.leaves, self.leave, -self.leave)
        self.sign = jnp.where(self.late > 0, 1.0, -1.0)

    def slab(self, j):
        last = self.sizes[0] + 1
        return jnp.where(self.late > 0, j, last - j)


def gather_index(place, near_slots, q, offset):
    ey = place.sizes[4]
    low = jnp.where(place.first_y, near_slots[q, 1, 0, 0:1], near_slots[q, 0, 0, ey - 1 : ey])
    high = jnp.where(place.last_y, near_slots[q, 1, 0, ey - 1 : ey], near_slots[q, 2, 0, 0:1])
    pieces = [low] + [near_slots[q, 1, 0, c : c + 1] for c in range(ey)] + [high]
    count = place.sizes[7]
    return jnp.concatenate(pieces, axis=1) - (place.gx + offset) * (place.down * count)


def choose(index):
    digits = lax.broadcasted_iota(jnp.int32, (LANES, index.shape[1]), 0)
    return (digits == (index & (LANES - 1))).astype(jnp.float32).astype(jnp.bfloat16)


def page_of(index):
    return index >> (LANES.bit_length() - 1)


def keep_page(rows, page):
    kept = lax.broadcasted_iota(jnp.int32, rows.shape, 0) == page
    return jnp.sum(jnp.where(kept, rows, 0.0), axis=0, keepdims=True)


def gather_row(place, held, q, index, chosen):
    blocks = place.sizes[7] // LANES
    pages = place.down * blocks
    table = [held[q, h, 0 : 8 * blocks] for h in range(place.down)]
    table += [held[q, h, 8 * blocks : 9 * blocks] for h in range(place.down)]
    found = dot_two(jnp.concatenate(table, axis=0), chosen)
    page = page_of(index)
    total = found[0:8]
    for h in range(1, pages):
        total = jnp.where(page == h, found[8 * h : 8 * h + 8], total)
    return total, keep_page(found[8 * pages : 9 * pages], page)


def pick_row(place, held, q, index):
    blocks = place.sizes[7] // LANES
    totals, lasts = [], []
    for t in range(index.shape[1] // LANES):
        lanes = index[:, t * LANES : (t + 1) * LANES]
        page = page_of(lanes)
        spot = jnp.broadcast_to(lanes & (LANES - 1), (8, LANES))

        def take(rows):
            return jnp.take_along_axis(rows, spot, axis=1, mode="promise_in_bounds")

        total = None
        tails = []
        for h in range(place.down):
            tails.append(held[q, h, 8 * blocks : 9 * blocks])
            for b in range(blocks):
                found = take(held[q, h, 8 * b : 8 * b + 8])
                total = found if total is None else jnp.where(page == h * blocks + b, found, total)
        totals.append(total)
        tails = jnp.concatenate(tails, axis=0)
        last = None
        for g in range(0, place.down * blocks, 8):
            part = keep_page(take(tails[g : g + 8]), page - g)
            last = part if last is None else last + part
        lasts.append(last)
    return jnp.concatenate(totals, axis=1), jnp.concatenate(lasts, axis=1)


def refine_row(place, row, weight_y, weight_z, whole):
    by, ez = place.sizes[1], place.sizes[5]
    total, last = row
    span = WINDOW * ez
    spread = []
    for k in range(9):
        values = total[k : k + 1] if k < 8 else last
        for half in range(by // 8):
            at = 2 * half * ez
            spread.append(weight_y[8 * half : 8 * half + 8] * values[:, at : at + span])
        at = (by // 4 - 2) * ez
        rim = lax.broadcasted_iota(jnp.int32, (8, span), 0) < 4
        spread.append(weight_y[by : by + 8] * jnp.where(rim, values[:, 0:span], values[:, at : at + span]))
    spread = jnp.concatenate(spread, axis=0)
    if whole:
        return dot_two(spread, weight_z)
    return jnp.dot(spread.astype(jnp.bfloat16), weight_z, preferred_element_type=jnp.float32)


def rolls(nz, by):
    lane = lax.broadcasted_iota(jnp.int32, (by, nz), 1)

    def ahead(values):
        return pltpu.roll(values, nz - 1, 1)

    def behind(values):
        return pltpu.roll(values, 1, 1)

    return lane, ahead, behind


def grad_z(values):
    nz = values.shape[1]
    lane, ahead, behind = rolls(nz, values.shape[0])
    upper = jnp.where(lane == nz - 1, values, ahead(values))
    lower = jnp.where(lane == 0, values, behind(values))
    return upper - lower


def make_flux(place, volts, slopes, early, late, first):
    by, nz = place.sizes[1], place.sizes[2]
    lane, ahead, behind = rolls(nz, by)
    y_row = lax.broadcasted_iota(jnp.int32, (by, nz), 0)

    def volt(j, shift=0):
        return volts[j, TOP + shift : TOP + shift + by]

    def slope_z(j, shift=0):
        return slopes[j, TOP + shift : TOP + shift + by]

    def tensor(number, j, shift=0):
        rows = slice(TOP + shift, TOP + shift + by)
        return early[number, j, rows] if j < first else late[number, j - first, rows]

    def slope_y(j):
        return volt(j, 1) - volt(j, -1)

    def slope_x(j, shift=0):
        return volt(j + 1, shift) - volt(j - 1, shift)

    def face_x(j, mine, next_one):
        return (
            (mine[0] + next_one[0]) * (volt(j + 1) - volt(j))
            + (mine[1] + next_one[1]) * (slope_y(j) + slope_y(j + 1))
            + (mine[2] + next_one[2]) * (slope_z(j) + slope_z(j + 1))
        )

    def face_y(j, shift):
        def mean(number):
            return tensor(number, j) + tensor(number, j, shift)

        step = volt(j, shift) - volt(j) if shift > 0 else volt(j) - volt(j, shift)
        return (
            mean(XY) * (slope_x(j) + slope_x(j, shift))
            + mean(YY) * step
            + mean(YZ) * (slope_z(j) + slope_z(j, shift))
        )

    def across_yz(j):
        upper = jnp.where(jnp.logical_and(y_row == by - 1, place.last_y), 0.0, face_y(j, 1))
        lower = jnp.where(jnp.logical_and(y_row == 0, place.first_y), 0.0, face_y(j, -1))

        def pair(values):
            return values + ahead(values)

        face_z = (
            pair(tensor(XZ, j)) * pair(slope_x(j))
            + pair(tensor(YZ, j)) * pair(slope_y(j))
            + pair(tensor(ZZ, j)) * (ahead(volt(j)) - volt(j))
        )
        face_z = jnp.where(lane == nz - 1, 0.0, face_z)
        return (upper - lower) + (face_z - behind(face_z))

    def x_parts(j):
        return [tensor(number, j) for number in (XX, XY, XZ)]

    return face_x, across_yz, x_parts


def put_tensors(place, conducts, slot, mid, side, weight, fiber_at, halo, note):
    by = place.sizes[1]
    tall = by + 8
    for half in range(by // 8):
        rows = slice(8 * half, 8 * half + 8)
        entries = []
        for k in range(9):
            at = tall * k + 8 * half
            entries.append(mid(at) + weight * side(at))
        fiber = fiber_at(rows)
        wanted = (XX, XY, XZ) if halo else tuple(range(6))
        for number, value in tensor_of(entries, fiber, place.sign, wanted).items():
            conducts[number, slot, TOP + 8 * half : TOP + 8 * half + 8] = value
        if not halo:
            note(rows, excess_of(entries, fiber))


def put_rims(place, conducts, slabs, mid, side, rim_fiber):
    bx, by, nz = place.sizes[:3]
    tall = by + 8
    row = lax.rem(lax.broadcasted_iota(jnp.int32, (8, nz), 0), bx)
    weight = jnp.zeros((8, nz), jnp.float32)
    for j in slabs.values():
        weight = jnp.where(row == j - 1, abs((j - 0.5) / RATIO - 0.5), weight)
    entries = []
    for k in range(9):
        entries.append(mid(tall * k + by) + weight * side(tall * k + by))
    for number, value in tensor_of(entries, rim_fiber, place.sign, (YY, XY, YZ)).items():
        for slot, j in slabs.items():
            conducts[number, slot, TOP - 1 : TOP] = value[j - 1 : j]
            conducts[number, slot, TOP + by : TOP + by + 1] = value[bx + j - 1 : bx + j]


def put_volts(place, cells, volts, slopes, j):
    by = place.sizes[1]
    spot = place.slab(j)
    own = cells[0, spot, TOP : TOP + by]
    volts[j, TOP : TOP + by] = own
    low, high = cells[0, spot, TOP - 1 : TOP], cells[0, spot, TOP + by : TOP + by + 1]
    volts[j, TOP - 1 : TOP] = jnp.where(place.first_y, own[0:1], low)
    volts[j, TOP + by : TOP + by + 1] = jnp.where(place.last_y, own[by - 1 : by], high)


def exchange(
    across,
    down,
    sizes,
    potential,
    recovery,
    angles,
    deform,
    slots,
    cells,
    held,
    near_slots,
    fibers,
    rim_fibers,
    spread_y,
    spread_z,
    refined,
    middle,
    volts,
    slopes,
    partial,
    base,
    next_recovery,
    conducts,
    rest_in,
    early_refined,
    halo_fibers,
    gauge,
    slot_gauge,
    send_sem,
    deform_sem,
    slot_sem,
    near_sem,
    local_sem,
    plane_ready,
    leave_ready,
    equal_ready,
):
    bx, by, nz, ex, ey, ez, parts, count = sizes
    blocks = count // LANES
    place = Place(across, down, sizes)
    gx, gy = place.gx, place.gy
    first_y, last_y, leave = place.first_y, place.last_y, place.leave
    sides = ((leave, place.leaves), (-leave, None))

    def when(check, act):
        if check is None:
            act()
        else:
            pl.when(check)(act)

    bits = max(down - 1, 1).bit_length()
    far = 4 * across * down

    def rank_of(row, column):
        chip = row // 2
        if isinstance(column, int):
            hops = column.bit_count()
        else:
            hops = sum(lax.rem(column // (1 << bit), 2) for bit in range(bits))
        return (chip + hops) * far + chip

    rank = rank_of(gx, gy)
    columns_by_hops = sorted(range(down), key=lambda column: (column.bit_count(), column))

    def peers(act, groups):
        for group in groups:
            rows = ((leave,),) if group else ((-leave, 0),)

            def visit(rows=rows[0]):
                for column in columns_by_hops:
                    for dx in rows:
                        act(dx, column, rank_of(gx + dx, column) - rank)

            when(place.leaves if group else None, visit)

    def other(dx, column):
        return column != gy if isinstance(dx, int) else True

    def guarded(test, act):
        def visit(dx, column, above):
            pl.when(jnp.logical_and(test(above), other(dx, column)))(functools.partial(act, dx, column))

        return visit

    upper_core = lax.rem(gx, 2) == 1

    def meets(row, above, column):
        even_row = lax.rem(row, 2) == 0
        return jnp.logical_or(above < 0, jnp.logical_and(above == 0, jnp.logical_or(jnp.logical_not(even_row), column == gy)))

    def lower(act):
        def visit(dx, column, above):
            here = jnp.logical_and(meets(gx, above, column), other(dx, column))
            pl.when(here)(functools.partial(act, dx, column))

        return visit

    def level(act):
        def visit(dx, column, above):
            there = jnp.logical_and(meets(gx + dx, -above, column), other(dx, column))
            pl.when(there)(functools.partial(act, dx, column))

        return visit

    def equal(act):
        def visit(dx, column, above):
            pl.when(jnp.logical_and(above == 0, column != gy))(functools.partial(act, dx, column))

        return visit

    def beneath(act):
        return guarded(lambda above: above < 0, act)

    def higher(act):
        return guarded(lambda above: above > 0, act)

    packed = held.at[1, gy]
    for b in range(blocks):
        columns = pl.ds(b * LANES, LANES)
        pltpu.make_async_copy(
            deform.at[pl.ds(0, 8), columns], packed.at[pl.ds(8 * b, 8)], local_sem.at[0]
        ).start()
        pltpu.make_async_copy(
            deform.at[pl.ds(8, 1), columns], packed.at[pl.ds(8 * blocks + b, 1)], local_sem.at[0]
        ).start()
    inside = pl.ds(TOP, by)
    pltpu.make_async_copy(slots, near_slots.at[1, 1], local_sem.at[2]).start()
    pltpu.make_async_copy(potential, cells.at[0, pl.ds(1, bx), inside], local_sem.at[1]).start()
    pltpu.make_async_copy(angles, cells.at[pl.ds(1, 2), pl.ds(1, bx), inside], local_sem.at[1]).start()
    pltpu.make_async_copy(recovery, rest_in, local_sem.at[1]).start()

    barrier = pltpu.get_barrier_semaphore()

    def tell(sem, dx, column):
        pl.semaphore_signal(sem, inc=1, device_id=(gx + dx, column), device_id_type=MESH)

    peers(level(functools.partial(tell, barrier)), (0, 1))
    below = 0
    equals = 0
    plane_above, leave_above = [], []
    for column in range(down):
        higher_here = 0
        for dx in (-leave, 0):
            above = rank_of(gx + dx, column) - rank
            below = below + jnp.where(jnp.logical_and(meets(gx, above, column), other(dx, column)), 1, 0)
            higher_here = higher_here + jnp.where(above > 0, 1, 0)
            equals = equals + jnp.where(jnp.logical_and(above == 0, column != gy), 1, 0)
        plane_above.append(higher_here)
        above = rank_of(gx + leave, column) - rank
        below = below + jnp.where(jnp.logical_and(place.leaves, meets(gx, above, column)), 1, 0)
        leave_above.append(jnp.where(jnp.logical_and(place.leaves, above > 0), 1, 0))

    pl.semaphore_wait(barrier, below)
    pl.when(upper_core)(lambda: tell(equal_ready, -1, gy))
    peers(beneath(functools.partial(tell, leave_ready.at[gy])), (1,))
    peers(beneath(functools.partial(tell, plane_ready.at[gy])), (0,))

    def drain(ref, sem):
        pltpu.make_async_copy(ref, ref, sem).wait()

    rows = pl.ds(0, 9 * blocks)
    line = 4 * nz

    def drain_bytes(amount, sem):
        assert amount % line == 0
        drain(gauge.at[pl.ds(0, amount // line)], sem)

    def drain_slots(amount, sem):
        drain(slot_gauge.at[pl.ds(0, amount)], sem)

    drain(held.at[1, gy, rows], local_sem.at[0])
    drain_slots(1, local_sem.at[2])

    def put(source, target, sem, dx, where):
        pltpu.make_async_remote_copy(
            src_ref=source,
            dst_ref=target,
            send_sem=send_sem.at[0],
            recv_sem=sem,
            device_id=(gx + dx, where),
            device_id_type=MESH,
        ).start()

    def near_of(dx):
        return 0 if isinstance(dx, int) else jnp.where(dx == leave, 1, 0)

    def send_deform(dx, column):
        q = 1 - dx
        put(held.at[1, gy, rows], held.at[q, gy, rows], deform_sem.at[near_of(dx)], dx, column)

    def send_slots(dx, dy):
        put(near_slots.at[1, 1], near_slots.at[1 - dx, 1 - dy], slot_sem.at[near_of(dx)], dx, gy + dy)

    def send_cells(dx, dy):
        y_source = inside if dy == 0 else pl.ds(TOP if dy < 0 else TOP + by - 1, 1)
        y_target = inside if dy == 0 else pl.ds(TOP + by if dy < 0 else TOP - 1, 1)
        if isinstance(dx, int):
            x_source = x_target = pl.ds(1, bx)
        else:
            x_source = pl.ds(jnp.where(dx < 0, 1, bx), 1)
            x_target = pl.ds(jnp.where(dx < 0, bx + 1, 0), 1)
        corner = dy != 0 and not isinstance(dx, int)
        fields = pl.ds(0, 1 if corner else 3)
        source, target = cells.at[fields, x_source, y_source], cells.at[fields, x_target, y_target]
        put(source, target, near_sem.at[near_of(dx)], dx, gy + dy)

    def neighbours(act, group, sign, column=None):
        for dx in (leave,) if group else (-leave, 0):
            for dy in (-1, 0, 1):
                if isinstance(dx, int) and dy == 0:
                    continue
                above = rank_of(gx + dx, gy + dy) - rank
                if sign > 0:
                    check = above > 0
                elif sign < 0:
                    check = meets(gx, above, gy + dy)
                else:
                    check = jnp.logical_and(above == 0, dy != 0)
                if column is not None:
                    check = jnp.logical_and(check, gy + dy == column)
                if dy:
                    check = jnp.logical_and(check, jnp.logical_not(first_y if dy < 0 else last_y))
                if group:
                    check = jnp.logical_and(check, place.leaves)
                pl.when(check)(functools.partial(act, dx, dy))

    def local_work():
        width = WINDOW * ez
        row = lax.broadcasted_iota(jnp.int32, (by + 8, width), 0)
        lane = lax.broadcasted_iota(jnp.int32, (by + 8, width), 1)
        low = row < by + bx
        cell = jnp.where(row < by, row, jnp.where(low, -1, by))
        start = jnp.where(row < by, 2 * (row // 8), jnp.where(low, 0, ey - 2))
        spot = (cell.astype(jnp.float32) + 0.5) * (1.0 / RATIO) - 0.5
        coarse = (lane // ez + start - 1).astype(jnp.float32)
        spread_y[...] = jnp.maximum(1.0 - jnp.abs(spot - coarse), 0.0)
        row = lax.broadcasted_iota(jnp.int32, (width, nz), 0)
        lane = lax.broadcasted_iota(jnp.int32, (width, nz), 1)
        spot = jnp.clip((lane.astype(jnp.float32) + 0.5) * (1.0 / RATIO) - 0.5, 0.0, ez - 1.0)
        weight = jnp.maximum(1.0 - jnp.abs(spot - lax.rem(row, ez).astype(jnp.float32)), 0.0)
        spread_z[...] = weight.astype(jnp.bfloat16)
        for s in range(bx):
            own = [cells[number, s + 1, TOP : TOP + by] for number in (1, 2)]
            for number, part in enumerate(fiber_of(*own)):
                fibers[number, s] = part
            voltage = cells[0, s + 1, TOP : TOP + by]
            resting = rest_in[s]
            next_recovery[s] = resting + 0.05 * (-resting - 8.0 * voltage * (voltage - 1.15))
            current = 8.0 * voltage * (voltage - 0.15) * (voltage - 1.0) + voltage * resting
            base[s] = voltage - 0.1 * current

    peers(lower(send_deform), (1, 0))
    for group in (0, 1):
        neighbours(send_slots, group, -1)
    drain_bytes(4 * bx * by * line, local_sem.at[1])
    for group in (1, 0):
        neighbours(send_cells, group, -1)
    local_work()

    def send_near(dx, dy):
        send_slots(dx, dy)
        send_cells(dx, dy)

    @pl.when(jnp.logical_not(upper_core))
    def _():
        pl.semaphore_wait(equal_ready, 1)

        @pl.when(equals > 0)
        def _():
            peers(equal(send_deform), (0,))
            neighbours(send_near, 0, 0)

    for group, ready, counts in ((0, plane_ready, plane_above), (1, leave_ready, leave_above)):
        for column in columns_by_hops:

            @pl.when(counts[column] > 0)
            def _(group=group, ready=ready, counts=counts, column=column):
                pl.semaphore_wait(ready.at[column], counts[column])
                for dx in (leave,) if group else (-leave, 0):
                    higher(send_deform)(dx, column, rank_of(gx + dx, column) - rank)
                neighbours(send_near, group, 1, column)

    middle_y = jnp.logical_not(jnp.logical_or(first_y, last_y))
    some_y = jnp.logical_xor(first_y, last_y)
    no_y = jnp.logical_and(first_y, last_y)

    def over_y(act):
        pl.when(middle_y)(functools.partial(act, 2))
        pl.when(some_y)(functools.partial(act, 1))
        pl.when(no_y)(functools.partial(act, 0))

    table = 4 * parts * count

    def wait_plane_near(slot, near):
        over_y(lambda n: drain_slots(2 * n + 1, slot))
        over_y(lambda n: drain_bytes((3 * by + n * (3 * bx + 1)) * line, near))

    def wait_leave_near(slot, near):
        over_y(lambda n: drain_slots(n + 1, slot))
        over_y(lambda n: drain_bytes((3 * by + n) * line, near))

    late = 1 + place.late
    early = 1 - place.late

    wait_plane_near(slot_sem.at[0], near_sem.at[0])
    index_middle = gather_index(place, near_slots, 1, 0)
    index_early = gather_index(place, near_slots, early, -place.late)
    chosen_middle, chosen_early = choose(index_middle), choose(index_early)
    for j in range(bx + 1):
        put_volts(place, cells, volts, slopes, j)

    @pl.when(jnp.logical_not(place.leaves))
    def _():
        volts[0] = volts[1]

    for j in range(bx + 1):
        slopes[j] = grad_z(volts[j])

    def rim_of(number):
        pieces = [cells[number, place.slab(j), row : row + 1] for row in (TOP - 1, TOP + by) for j in range(1, bx + 1)]
        return jnp.concatenate(pieces, axis=0)

    for number, value in enumerate(fiber_of(rim_of(1), rim_of(2))):
        rim_fibers[number] = value
    halo = place.slab(0)
    for number, value in enumerate(fiber_of(*(cells[n, halo, TOP : TOP + by] for n in (1, 2)))):
        halo_fibers[number] = value

    drain_bytes((2 * down - 1) * table, deform_sem.at[0])
    weight_y, weight_z = spread_y[...], spread_z[...]
    middle_row = gather_row(place, held, 1, index_middle, chosen_middle)
    early_row = gather_row(place, held, early, index_early, chosen_early)
    refined[...] = refine_row(place, middle_row, weight_y, weight_z, True)
    early_row = [jnp.where(place.leaves, a - b, 0.0) for a, b in zip(early_row, middle_row)]
    early_refined[...] = refine_row(place, early_row, weight_y, weight_z, False)
    middle[0:8] = middle_row[0]
    middle[8:9] = middle_row[1]

    def mid(at):
        return refined[at : at + 8]

    def side(at):
        return early_refined[at : at + 8]

    half = RATIO // 2
    for j in range(half + 1):
        spot = place.slab(j)

        def fiber_at(rows, j=j, spot=spot):
            if j:
                return [fibers[number, spot - 1, rows] for number in range(3)]
            return [halo_fibers[number, rows] for number in range(3)]

        def note(rows, excess, j=j, spot=spot):
            voltage = volts[j, TOP + rows.start : TOP + rows.stop]
            partial[j - 1, rows] = base[spot - 1, rows] - excess * (voltage - 0.6)

        weight = abs((j - 0.5) / RATIO - 0.5)
        put_tensors(place, conducts, j, mid, side, weight, fiber_at, j == 0, note)
    rim_fiber = [rim_fibers[number] for number in range(3)]
    put_rims(place, conducts, {j: j for j in range(1, half + 1)}, mid, side, rim_fiber)

    out = send_sem.at[0]
    wait_plane_near(out, out)
    drain_bytes((2 * down - 1) * table, out)

    @pl.when(place.leaves)
    def _():
        wait_leave_near(out, out)
        drain_bytes(down * table, out)

    @pl.when(place.leaves)
    def _():
        wait_leave_near(slot_sem.at[1], near_sem.at[1])
        drain_bytes(down * table, deform_sem.at[1])


def compute(
    across,
    down,
    sizes,
    cells,
    held,
    near_slots,
    fibers,
    rim_fibers,
    spread_y,
    spread_z,
    refined,
    middle,
    volts_in,
    slopes_in,
    partial,
    base,
    recovered,
    early_conducts,
    next_potential,
    next_recovery,
    volts,
    slopes,
    conducts,
    late_refined,
    result,
    out_sem,
):
    bx, by, nz, ex, ey, ez, parts, count = sizes
    place = Place(across, down, sizes)
    half = RATIO // 2
    late = 1 + place.late

    leaving = [pltpu.make_async_copy(recovered, next_recovery, out_sem.at[0])]
    leaving[0].start()

    def finish(j):
        copy = pltpu.make_async_copy(result.at[j - 1], next_potential.at[place.slab(j) - 1], out_sem.at[j])
        copy.start()
        leaving.append(copy)

    row = pick_row(place, held, late, gather_index(place, near_slots, late, place.late))
    row = [a - b for a, b in zip(row, (middle[0:8], middle[8:9]))]
    late_refined[...] = refine_row(place, row, spread_y[...], spread_z[...], False)

    for j in range(bx + 1):
        volts[j] = volts_in[j]
        slopes[j] = slopes_in[j]
    put_volts(place, cells, volts, slopes, bx + 1)
    slopes[bx + 1] = grad_z(volts[bx + 1])

    def mid(at):
        return refined[at : at + 8]

    def side(at):
        return late_refined[at : at + 8]

    for j in range(half + 1, bx + 2):
        spot = place.slab(j)

        def fiber_at(rows, j=j, spot=spot):
            if j <= bx:
                return [fibers[number, spot - 1, rows] for number in range(3)]
            start = TOP + rows.start
            return fiber_of(*(cells[number, spot, start : start + 8] for number in (1, 2)))

        def note(rows, excess, j=j, spot=spot):
            voltage = volts[j, TOP + rows.start : TOP + rows.stop]
            result[j - 1, rows] = base[spot - 1, rows] - excess * (voltage - 0.6)

        weight = abs((j - 0.5) / RATIO - 0.5)
        put_tensors(place, conducts, j - half - 1, mid, side, weight, fiber_at, j == bx + 1, note)
    rim_fiber = [rim_fibers[number] for number in range(3)]
    put_rims(place, conducts, {j - half - 1: j for j in range(half + 1, bx + 1)}, mid, side, rim_fiber)
    face_x, across_yz, x_parts = make_flux(place, volts, slopes, early_conducts, conducts, half + 1)
    faces = [face_x(j, x_parts(j), x_parts(j + 1)) for j in range(bx + 1)]
    faces[0] = jnp.where(place.leaves, faces[0], 0.0)
    for j in range(1, bx + 1):
        local = partial[j - 1] if j <= half else result[j - 1]
        result[j - 1] = local + 0.1 * (across_yz(j) + (faces[j] - faces[j - 1]))
        finish(j)
    for copy in leaving:
        copy.wait()


def solution(mesh):
    across, down = mesh.shape["gx"], mesh.shape["gy"]

    def local(potential, recovery, angles, deform, slots):
        bx, by, nz = potential.shape
        ex, ey, ez = slots.shape
        parts, count = deform.shape
        assert ex == 1 and bx == RATIO and by == RATIO * ey and by % 8 == 0
        assert count % LANES == 0 and parts == 9 and across % 2 == 0 and (2 * ez) % LANES == 0
        sizes = (bx, by, nz, ex, ey, ez, parts, count)
        blocks = count // LANES
        f32 = jnp.float32
        half = RATIO // 2
        shape = jax.ShapeDtypeStruct(potential.shape, f32)
        anywhere = pl.BlockSpec(memory_space=pl.ANY)
        in_vmem = pl.BlockSpec(memory_space=pltpu.VMEM)
        passed = (
            pltpu.VMEM((3, bx + 2, by + 16, nz), f32),
            pltpu.VMEM((3, down, 8 * blocks + 8, LANES), f32),
            pltpu.VMEM((3, 3, ex, ey, ez), jnp.int32),
            pltpu.VMEM((3, bx, by, nz), f32),
            pltpu.VMEM((3, 2 * bx, nz), f32),
            pltpu.VMEM((by + 8, WINDOW * ez), f32),
            pltpu.VMEM((WINDOW * ez, nz), jnp.bfloat16),
            pltpu.VMEM((9 * (by + 8), nz), f32),
            pltpu.VMEM((16, (ey + 2) * ez), f32),
            pltpu.VMEM((bx + 1, by + 16, nz), f32),
            pltpu.VMEM((bx + 1, by + 16, nz), f32),
            pltpu.VMEM((half, by, nz), f32),
            pltpu.VMEM((bx, by, nz), f32),
            pltpu.VMEM((bx, by, nz), f32),
            pltpu.VMEM((6, half + 1, by + 16, nz), f32),
        )
        arrived = pl.pallas_call(
            functools.partial(exchange, across, down, sizes),
            out_shape=passed,
            in_specs=[pl.BlockSpec(memory_space=pltpu.MemorySpace.HBM)] * 5,
            out_specs=(in_vmem,) * len(passed),
            scratch_shapes=[
                pltpu.VMEM(recovery.shape, f32),
                pltpu.VMEM((9 * (by + 8), nz), f32),
                pltpu.VMEM((3, by, nz), f32),
                pltpu.VMEM((max(4 * bx * by, 2 * down * parts * count // nz), 1, nz), f32),
                pltpu.VMEM((5, ex, ey, ez), jnp.int32),
                pltpu.SemaphoreType.DMA((1,)),
                pltpu.SemaphoreType.DMA((2,)),
                pltpu.SemaphoreType.DMA((2,)),
                pltpu.SemaphoreType.DMA((2,)),
                pltpu.SemaphoreType.DMA((3,)),
                pltpu.SemaphoreType.REGULAR((down,)),
                pltpu.SemaphoreType.REGULAR((down,)),
                pltpu.SemaphoreType.REGULAR,
            ],
            compiler_params=pltpu.CompilerParams(
                collective_id=0, has_side_effects=True, vmem_limit_bytes=VMEM_LIMIT
            ),
        )(*(pltpu.with_memory_space_constraint(x, pltpu.MemorySpace.HBM) for x in (potential, recovery, angles, deform, slots)))
        return pl.pallas_call(
            functools.partial(compute, across, down, sizes),
            out_shape=(shape, shape),
            in_specs=[in_vmem] * len(passed),
            out_specs=(anywhere,) * 2,
            scratch_shapes=[
                pltpu.VMEM((bx + 2, by + 16, nz), f32),
                pltpu.VMEM((bx + 2, by + 16, nz), f32),
                pltpu.VMEM((6, half + 1, by + 16, nz), f32),
                pltpu.VMEM((9 * (by + 8), nz), f32),
                pltpu.VMEM((bx, by, nz), f32),
                pltpu.SemaphoreType.DMA((bx + 1,)),
            ],
            compiler_params=pltpu.CompilerParams(vmem_limit_bytes=VMEM_LIMIT),
        )(*arrived)

    return jax.shard_map(
        local,
        mesh=mesh,
        in_specs=(
            P("gx", "gy", None),
            P("gx", "gy", None),
            P(None, "gx", "gy", None),
            P(None, ("gx", "gy")),
            P("gx", "gy", None),
        ),
        out_specs=(P("gx", "gy", None), P("gx", "gy", None)),
        check_vma=False,
    )
```

```python
import functools

import jax
import jax.numpy as jnp
from jax import lax
from jax.experimental import pallas as pl
from jax.experimental.pallas import tpu as pltpu
from jax.sharding import PartitionSpec as P

MESH = pl.DeviceIdType.MESH
RATIO = 4
LANES = 128
VMEM_LIMIT = 16 * 1024 * 1024
TOP = 8
WINDOW = 4
FIBER_SCALE = (7.0 / 3.0) ** 0.5
STRETCH_SCALE = (3.0 / 7.0) ** 0.5
XX, YY, ZZ, XY, XZ, YZ = range(6)
PAIRS = ((0, 0), (1, 1), (2, 2), (0, 1), (0, 2), (1, 2))


def split_two(values):
    high = values.astype(jnp.bfloat16)
    low = (values - high.astype(jnp.float32)).astype(jnp.bfloat16)
    return high, low


def dot_two(values, weights):
    high, low = split_two(values)
    return jnp.dot(high, weights, preferred_element_type=jnp.float32) + jnp.dot(
        low, weights, preferred_element_type=jnp.float32
    )


def polynomial(terms, value):
    total = terms[-1]
    for term in terms[-2::-1]:
        total = total * value + term
    return total


HALF_SINE = (0.707106764632592, -0.02946274890445726, 3.682656229209654e-4, -2.187710743548062e-6, 7.155278665108425e-9)
HALF_COSINE = (1.414213496564441, -0.17677636064176425, 3.6825754039592376e-3, -3.0612650004537585e-5, 1.2790856262670407e-7)


def sine_cosine(angle):
    square = angle * angle
    sine = angle * polynomial(HALF_SINE, square)
    cosine = polynomial(HALF_COSINE, square)
    return sine * cosine, 1.0 - sine * sine


def fiber_of(azimuth, elevation):
    sin_u, cos_u = sine_cosine(azimuth)
    sin_e, cos_e = sine_cosine(elevation)
    flat = FIBER_SCALE * cos_e
    return cos_u * flat, sin_u * flat, FIBER_SCALE * sin_e


def tensor_of(entries, fiber, sign, wanted):
    def element(i, j):
        return entries[3 * (i % 3) + j % 3]

    adjugate = [
        [
            element(j + 1, i + 1) * element(j + 2, i + 2)
            - element(j + 1, i + 2) * element(j + 2, i + 1)
            for j in range(3)
        ]
        for i in range(3)
    ]
    determinant = (
        element(0, 0) * adjugate[0][0]
        + element(0, 1) * adjugate[1][0]
        + element(0, 2) * adjugate[2][0]
    )
    inverse = 1.0 / determinant
    square = inverse * inverse
    diagonal = (0.3 * 0.5) * square
    mixed = (0.3 * 0.125) * square
    mirrored = (0.3 * 0.125 * sign) * square
    rows = sorted({i for number in wanted for i in PAIRS[number]})
    pulled = {
        i: adjugate[i][0] * fiber[0] + adjugate[i][1] * fiber[1] + adjugate[i][2] * fiber[2]
        for i in rows
    }
    scale = {XX: diagonal, YY: diagonal, ZZ: diagonal, XY: mirrored, XZ: mirrored, YZ: mixed}
    conduct = {}
    for number in wanted:
        i, j = PAIRS[number]
        metric = (
            adjugate[i][0] * adjugate[j][0]
            + adjugate[i][1] * adjugate[j][1]
            + adjugate[i][2] * adjugate[j][2]
        )
        conduct[number] = scale[number] * (metric + pulled[i] * pulled[j])
    return conduct


def excess_of(entries, fiber):
    parts = [
        entries[3 * i] * fiber[0] + entries[3 * i + 1] * fiber[1] + entries[3 * i + 2] * fiber[2]
        for i in range(3)
    ]
    square = parts[0] * parts[0] + parts[1] * parts[1] + parts[2] * parts[2]
    return jnp.maximum(STRETCH_SCALE * (square * lax.rsqrt(square)) - 1.0, 0.0)


class Place:
    def __init__(self, across, down, sizes):
        self.across, self.down, self.sizes = across, down, sizes
        self.gx, self.gy = lax.axis_index("gx"), lax.axis_index("gy")
        self.first_x, self.last_x = self.gx == 0, self.gx == across - 1
        self.first_y, self.last_y = self.gy == 0, self.gy == down - 1
        odd = lax.rem(self.gx, 2)
        self.odd = odd
        self.leave = 2 * odd - 1
        self.leaves = jnp.logical_not(jnp.logical_or(self.first_x, self.last_x))
        self.late = jnp.where(self.leaves, self.leave, -self.leave)
        self.sign = jnp.where(self.late > 0, 1.0, -1.0)

    def slab(self, j):
        last = self.sizes[0] + 1
        return jnp.where(self.late > 0, j, last - j)


def load_rows(ref, at, start, size):
    planes = [ref[(*at, part, slice(start, start + size))] for part in range(ref.shape[-3])]
    return jnp.concatenate(planes, axis=1)


def store_rows(ref, at, start, value):
    for part in range(ref.shape[-3]):
        rows = slice(start, start + value.shape[0])
        ref[(*at, part, rows)] = value[:, part * LANES : (part + 1) * LANES]


def gather_index(place, near_slots, q, offset):
    ey = place.sizes[4]
    low = jnp.where(place.first_y, near_slots[q, 1, 0, 0:1], near_slots[q, 0, 0, ey - 1 : ey])
    high = jnp.where(place.last_y, near_slots[q, 1, 0, ey - 1 : ey], near_slots[q, 2, 0, 0:1])
    pieces = [low] + [near_slots[q, 1, 0, c : c + 1] for c in range(ey)] + [high]
    count = place.sizes[7]
    return jnp.concatenate(pieces, axis=1) - (place.gx + offset) * (place.down * count)


def page_of(index):
    return index >> (LANES.bit_length() - 1)


def keep_page(rows, page):
    kept = lax.broadcasted_iota(jnp.int32, rows.shape, 0) == page
    return jnp.sum(jnp.where(kept, rows, 0.0), axis=0, keepdims=True)


def pick_row(place, held, q, index):
    blocks = place.sizes[7] // LANES
    totals, lasts = [], []
    for t in range(index.shape[1] // LANES):
        lanes = index[:, t * LANES : (t + 1) * LANES]
        page = page_of(lanes)
        spot = jnp.broadcast_to(lanes & (LANES - 1), (8, LANES))

        def take(rows):
            return jnp.take_along_axis(rows, spot, axis=1, mode="promise_in_bounds")

        total = None
        tails = []
        for h in range(place.down):
            tails.append(held[q, h, 8 * blocks : 9 * blocks])
            for b in range(blocks):
                found = take(held[q, h, 8 * b : 8 * b + 8])
                total = found if total is None else jnp.where(page == h * blocks + b, found, total)
        totals.append(total)
        tails = jnp.concatenate(tails, axis=0)
        last = None
        for g in range(0, place.down * blocks, 8):
            part = keep_page(take(tails[g : g + 8]), page - g)
            last = part if last is None else last + part
        lasts.append(last)
    return jnp.concatenate(totals, axis=1), jnp.concatenate(lasts, axis=1)


def refine_row(place, row, weight_y, weight_z, whole):
    by, ez = place.sizes[1], place.sizes[5]
    total, last = row
    span = WINDOW * ez
    spread = []
    for k in range(9):
        values = total[k : k + 1] if k < 8 else last
        for half in range(by // 8):
            at = 2 * half * ez
            spread.append(weight_y[8 * half : 8 * half + 8] * values[:, at : at + span])
        at = (by // 4 - 2) * ez
        rim = lax.broadcasted_iota(jnp.int32, (8, span), 0) < 4
        spread.append(weight_y[by : by + 8] * jnp.where(rim, values[:, 0:span], values[:, at : at + span]))
    spread = jnp.concatenate(spread, axis=0)
    if whole:
        return dot_two(spread, weight_z)
    return jnp.dot(spread.astype(jnp.bfloat16), weight_z, preferred_element_type=jnp.float32)


def rolls(nz, by):
    lane = lax.broadcasted_iota(jnp.int32, (by, nz), 1)

    def ahead(values):
        return pltpu.roll(values, nz - 1, 1)

    def behind(values):
        return pltpu.roll(values, 1, 1)

    return lane, ahead, behind


def grad_z(values):
    nz = values.shape[1]
    lane, ahead, behind = rolls(nz, values.shape[0])
    upper = jnp.where(lane == nz - 1, values, ahead(values))
    lower = jnp.where(lane == 0, values, behind(values))
    return upper - lower


class Slopes:
    def __init__(self, place, volts, slopes, parts_x, parts_y, parts_z):
        self.place, self.volts, self.slopes = place, volts, slopes
        self.parts_x, self.parts_y, self.parts_z = parts_x, parts_y, parts_z

    def volt(self, j, shift=0):
        return load_rows(self.volts, (j,), TOP + shift, self.place.sizes[1])

    def slope_z(self, j, shift=0):
        return load_rows(self.slopes, (j,), TOP + shift, self.place.sizes[1])

    def slope_y(self, j):
        return self.volt(j, 1) - self.volt(j, -1)

    def slope_x(self, j, shift=0):
        return self.volt(j + 1, shift) - self.volt(j - 1, shift)

    def pair(self, values):
        return values + pltpu.roll(values, values.shape[1] - 1, 1)

    def along_x(self, j):
        self.parts_x[j, 0] = self.volt(j + 1) - self.volt(j)
        self.parts_x[j, 1] = self.slope_y(j) + self.slope_y(j + 1)
        self.parts_x[j, 2] = self.slope_z(j) + self.slope_z(j + 1)

    def with_x(self, j):
        for side, shift in enumerate((1, -1)):
            self.parts_y[j - 1, side, 0] = self.slope_x(j) + self.slope_x(j, shift)
        self.parts_z[j - 1, 0] = self.pair(self.slope_x(j))

    def within(self, j):
        here = self.volt(j)
        for side, shift in enumerate((1, -1)):
            self.parts_y[j - 1, side, 1] = shift * (self.volt(j, shift) - here)
            self.parts_y[j - 1, side, 2] = self.slope_z(j) + self.slope_z(j, shift)
        self.parts_z[j - 1, 1] = self.pair(self.slope_y(j))
        self.parts_z[j - 1, 2] = pltpu.roll(here, here.shape[1] - 1, 1) - here


def make_flux(place, parts_x, parts_y, parts_z, early, late, first):
    by, nz = place.sizes[1:3]
    lane, ahead, behind = rolls(nz, by)
    y_row = lax.broadcasted_iota(jnp.int32, (by, nz), 0)

    def tensor(number, j, shift=0):
        at = (number, j) if j < first else (number, j - first)
        return load_rows(early if j < first else late, at, TOP + shift, by)

    def face_x(j):
        terms = [
            (tensor(number, j) + tensor(number, j + 1)) * parts_x[j, part]
            for part, number in enumerate((XX, XY, XZ))
        ]
        return terms[0] + terms[1] + terms[2]

    def face_y(j, side, shift):
        terms = [
            (tensor(number, j) + tensor(number, j, shift)) * parts_y[j - 1, side, part]
            for part, number in enumerate((XY, YY, YZ))
        ]
        return terms[0] + terms[1] + terms[2]

    def across_yz(j):
        upper = jnp.where(jnp.logical_and(y_row == by - 1, place.last_y), 0.0, face_y(j, 0, 1))
        lower = jnp.where(jnp.logical_and(y_row == 0, place.first_y), 0.0, face_y(j, 1, -1))
        terms = []
        for part, number in enumerate((XZ, YZ, ZZ)):
            mine = tensor(number, j)
            terms.append((mine + ahead(mine)) * parts_z[j - 1, part])
        face_z = jnp.where(lane == nz - 1, 0.0, terms[0] + terms[1] + terms[2])
        return (upper - lower) + (face_z - behind(face_z))

    return face_x, across_yz


def put_tensors(place, conducts, slot, mid, side, weight, fiber_at, halo, note):
    by = place.sizes[1]
    tall = by + 8
    for half in range(by // 8):
        rows = slice(8 * half, 8 * half + 8)
        entries = []
        for k in range(9):
            at = tall * k + 8 * half
            entries.append(mid(at) + weight * side(at))
        fiber = fiber_at(rows)
        wanted = (XX, XY, XZ) if halo else tuple(range(6))
        for number, value in tensor_of(entries, fiber, place.sign, wanted).items():
            store_rows(conducts, (number, slot), TOP + 8 * half, value)
        if not halo:
            note(rows, excess_of(entries, fiber))


def put_rims(place, conducts, slabs, mid, side, rim_fiber, share):
    bx, by, nz = place.sizes[:3]
    tall = by + 8
    row = lax.rem(lax.broadcasted_iota(jnp.int32, (8, nz), 0), bx)
    weight = jnp.zeros((8, nz), jnp.float32)
    for j in slabs.values():
        weight = jnp.where(row == j - 1, share * abs((j - 0.5) / RATIO - 0.5), weight)
    entries = []
    for k in range(9):
        entries.append(mid(tall * k + by) + weight * side(tall * k + by))
    for number, value in tensor_of(entries, rim_fiber, place.sign, (YY, XY, YZ)).items():
        for slot, j in slabs.items():
            store_rows(conducts, (number, slot), TOP - 1, value[j - 1 : j])
            store_rows(conducts, (number, slot), TOP + by, value[bx + j - 1 : bx + j])


def put_volts(place, cells, volts, slopes, spot, slot):
    by = place.sizes[1]
    own = cells[0, spot, TOP : TOP + by]
    low, high = cells[0, spot, TOP - 1 : TOP], cells[0, spot, TOP + by : TOP + by + 1]
    low = jnp.where(place.first_y, own[0:1], low)
    high = jnp.where(place.last_y, own[by - 1 : by], high)
    for start, value in ((TOP, own), (TOP - 1, low), (TOP + by, high)):
        store_rows(volts, (slot,), start, value)
        store_rows(slopes, (slot,), start, grad_z(value))


def exchange(
    across,
    down,
    sizes,
    potential,
    recovery,
    angles,
    deform,
    slots,
    fibers,
    rim_fibers,
    refined,
    diffs,
    volts,
    slopes,
    parts_x,
    parts_y,
    parts_z,
    partial,
    base,
    next_recovery,
    conducts,
    cells,
    held,
    near_slots,
    rest_in,
    spread_y,
    spread_z,
    middle,
    gauge,
    slot_gauge,
    send_sem,
    deform_sem,
    slot_sem,
    near_sem,
    local_sem,
    plane_ready,
    leave_ready,
    equal_ready,
):
    bx, by, nz, ex, ey, ez, parts, count = sizes
    blocks = count // LANES
    place = Place(across, down, sizes)
    half = RATIO // 2
    gx, gy = place.gx, place.gy
    first_y, last_y, leave = place.first_y, place.last_y, place.leave
    for b in range(blocks):
        columns = pl.ds(b * LANES, LANES)
        pltpu.make_async_copy(
            deform.at[pl.ds(0, 8), columns], held.at[1, gy, pl.ds(8 * b, 8)], local_sem.at[0]
        ).start()
        pltpu.make_async_copy(
            deform.at[pl.ds(8, 1), columns], held.at[1, gy, pl.ds(8 * blocks + b, 1)], local_sem.at[0]
        ).start()
    inside = pl.ds(TOP, by)
    pltpu.make_async_copy(slots, near_slots.at[1, 1], local_sem.at[2]).start()
    pltpu.make_async_copy(potential, cells.at[0, pl.ds(1, bx), inside], local_sem.at[1]).start()
    pltpu.make_async_copy(angles, cells.at[pl.ds(1, 2), pl.ds(1, bx), inside], local_sem.at[1]).start()
    pltpu.make_async_copy(recovery, rest_in, local_sem.at[1]).start()

    sides = ((leave, place.leaves), (-leave, None))

    def when(check, act):
        if check is None:
            act()
        else:
            pl.when(check)(act)

    bits = max(down - 1, 1).bit_length()
    odd = place.odd

    def hops_of(column):
        if isinstance(column, int):
            return column.bit_count()
        hops = 0
        for _ in range(bits):
            halved = column // 2
            hops = hops + column - 2 * halved
            column = halved
        return hops

    own_hops = hops_of(gy)

    def above_of(dx, hops):
        chips = leave if dx is leave else 0
        return 4 * (chips + hops - own_hops) + chips

    columns_by_hops = sorted(range(down), key=lambda column: (column.bit_count(), column))

    def peers(act, groups):
        for group in groups:
            rows = ((leave,),) if group else ((-leave, 0),)

            def visit(rows=rows[0]):
                for column in columns_by_hops:
                    for dx in rows:
                        act(dx, column, above_of(dx, hops_of(column)))

            when(place.leaves if group else None, visit)

    def other(dx, column):
        return column != gy if isinstance(dx, int) else True

    def guarded(test, act):
        def visit(dx, column, above):
            pl.when(jnp.logical_and(test(above), other(dx, column)))(functools.partial(act, dx, column))

        return visit

    upper_core = odd == 1

    def meets(dx, above, column):
        even_row = odd == 0 if isinstance(dx, int) else odd == 1
        return jnp.logical_or(above < 0, jnp.logical_and(above == 0, jnp.logical_or(jnp.logical_not(even_row), column == gy)))

    def lower(act):
        def visit(dx, column, above):
            here = jnp.logical_and(meets(0, above, column), other(dx, column))
            pl.when(here)(functools.partial(act, dx, column))

        return visit

    def level(act):
        def visit(dx, column, above):
            there = jnp.logical_and(meets(dx, -above, column), other(dx, column))
            pl.when(there)(functools.partial(act, dx, column))

        return visit

    def equal(act):
        def visit(dx, column, above):
            pl.when(jnp.logical_and(above == 0, column != gy))(functools.partial(act, dx, column))

        return visit

    def beneath(act):
        return guarded(lambda above: above < 0, act)

    def higher(act):
        return guarded(lambda above: above > 0, act)

    near_hops = {dy: hops_of(gy + dy) for dy in (-1, 0, 1)}
    barrier = pltpu.get_barrier_semaphore()

    def tell(sem, dx, column):
        pl.semaphore_signal(sem, inc=1, device_id=(gx + dx, column), device_id_type=MESH)

    peers(level(functools.partial(tell, barrier)), (0, 1))
    below = 0
    equals = 0
    plane_above, leave_above = [], []
    for column in range(down):
        higher_here = 0
        for dx in (-leave, 0):
            above = above_of(dx, hops_of(column))
            below = below + jnp.where(jnp.logical_and(meets(0, above, column), other(dx, column)), 1, 0)
            higher_here = higher_here + jnp.where(above > 0, 1, 0)
            equals = equals + jnp.where(jnp.logical_and(above == 0, column != gy), 1, 0)
        plane_above.append(higher_here)
        above = above_of(leave, hops_of(column))
        below = below + jnp.where(jnp.logical_and(place.leaves, meets(0, above, column)), 1, 0)
        leave_above.append(jnp.where(jnp.logical_and(place.leaves, above > 0), 1, 0))

    pl.semaphore_wait(barrier, below)
    pl.when(upper_core)(lambda: tell(equal_ready, -1, gy))
    peers(beneath(functools.partial(tell, leave_ready.at[gy])), (1,))
    peers(beneath(functools.partial(tell, plane_ready.at[gy])), (0,))

    def drain(ref, sem):
        pltpu.make_async_copy(ref, ref, sem).wait()

    rows = pl.ds(0, 9 * blocks)
    line = 4 * nz

    def drain_bytes(amount, sem):
        assert amount % line == 0
        drain(gauge.at[pl.ds(0, amount // line)], sem)

    def drain_slots(amount, sem):
        drain(slot_gauge.at[pl.ds(0, amount)], sem)

    drain(held.at[1, gy, rows], local_sem.at[0])
    drain_slots(1, local_sem.at[2])

    def put(source, target, sem, dx, where):
        pltpu.make_async_remote_copy(
            src_ref=source,
            dst_ref=target,
            send_sem=send_sem.at[0],
            recv_sem=sem,
            device_id=(gx + dx, where),
            device_id_type=MESH,
        ).start()

    def near_of(dx):
        return 0 if isinstance(dx, int) else jnp.where(dx == leave, 1, 0)

    def deform_of(dx):
        return 0 if isinstance(dx, int) else jnp.where(dx == leave, 2, 1)

    def send_deform(dx, column):
        q = 1 - dx
        put(held.at[1, gy, rows], held.at[q, gy, rows], deform_sem.at[deform_of(dx)], dx, column)

    def send_slots(dx, dy):
        put(near_slots.at[1, 1], near_slots.at[1 - dx, 1 - dy], slot_sem.at[near_of(dx)], dx, gy + dy)

    def send_cells(dx, dy):
        y_source = inside if dy == 0 else pl.ds(TOP if dy < 0 else TOP + by - 1, 1)
        y_target = inside if dy == 0 else pl.ds(TOP + by if dy < 0 else TOP - 1, 1)
        if isinstance(dx, int):
            x_source = x_target = pl.ds(1, bx)
        else:
            x_source = pl.ds(jnp.where(dx < 0, 1, bx), 1)
            x_target = pl.ds(jnp.where(dx < 0, bx + 1, 0), 1)
        corner = dy != 0 and not isinstance(dx, int)
        fields = pl.ds(0, 1 if corner else 3)
        source, target = cells.at[fields, x_source, y_source], cells.at[fields, x_target, y_target]
        put(source, target, near_sem.at[near_of(dx)], dx, gy + dy)

    def neighbours(act, group, sign, column=None):
        for dx in (leave,) if group else (-leave, 0):
            for dy in (-1, 0, 1):
                if isinstance(dx, int) and dy == 0:
                    continue
                above = above_of(dx, near_hops[dy])
                if sign > 0:
                    check = above > 0
                elif sign < 0:
                    check = meets(0, above, gy + dy)
                else:
                    check = jnp.logical_and(above == 0, dy != 0)
                if column is not None:
                    check = jnp.logical_and(check, gy + dy == column)
                if dy:
                    check = jnp.logical_and(check, jnp.logical_not(first_y if dy < 0 else last_y))
                if group:
                    check = jnp.logical_and(check, place.leaves)
                pl.when(check)(functools.partial(act, dx, dy))

    def local_work():
        width = WINDOW * ez
        row = lax.broadcasted_iota(jnp.int32, (by + 8, width), 0)
        lane = lax.broadcasted_iota(jnp.int32, (by + 8, width), 1)
        low = row < by + bx
        cell = jnp.where(row < by, row, jnp.where(low, -1, by))
        start = jnp.where(row < by, 2 * (row // 8), jnp.where(low, 0, ey - 2))
        spot = (cell.astype(jnp.float32) + 0.5) * (1.0 / RATIO) - 0.5
        coarse = (lane // ez + start - 1).astype(jnp.float32)
        spread_y[...] = jnp.maximum(1.0 - jnp.abs(spot - coarse), 0.0)
        row = lax.broadcasted_iota(jnp.int32, (width, nz), 0)
        lane = lax.broadcasted_iota(jnp.int32, (width, nz), 1)
        spot = jnp.clip((lane.astype(jnp.float32) + 0.5) * (1.0 / RATIO) - 0.5, 0.0, ez - 1.0)
        weight = jnp.maximum(1.0 - jnp.abs(spot - lax.rem(row, ez).astype(jnp.float32)), 0.0)
        spread_z[...] = weight.astype(jnp.bfloat16)
        for s in range(bx):
            own = [cells[number, s + 1, TOP : TOP + by] for number in (1, 2)]
            for number, part in enumerate(fiber_of(*own)):
                fibers[number, s] = part
            voltage = cells[0, s + 1, TOP : TOP + by]
            resting = rest_in[s]
            next_recovery[s] = resting + 0.05 * (-resting - 8.0 * voltage * (voltage - 1.15))
            current = 8.0 * voltage * (voltage - 0.15) * (voltage - 1.0) + voltage * resting
            base[s] = voltage - 0.1 * current

    peers(lower(send_deform), (1, 0))
    for group in (0, 1):
        neighbours(send_slots, group, -1)
    drain_bytes(4 * bx * by * line, local_sem.at[1])
    for group in (1, 0):
        neighbours(send_cells, group, -1)
    local_work()

    def send_near(dx, dy):
        send_slots(dx, dy)
        send_cells(dx, dy)

    @pl.when(jnp.logical_not(upper_core))
    def _():
        pl.semaphore_wait(equal_ready, 1)

        @pl.when(equals > 0)
        def _():
            peers(equal(send_deform), (0,))
            neighbours(send_near, 0, 0)

    for group, ready, counts in ((0, plane_ready, plane_above), (1, leave_ready, leave_above)):
        for column in columns_by_hops:

            @pl.when(counts[column] > 0)
            def _(group=group, ready=ready, counts=counts, column=column):
                pl.semaphore_wait(ready.at[column], counts[column])
                for dx in (leave,) if group else (-leave, 0):
                    higher(send_deform)(dx, column, above_of(dx, hops_of(column)))
                neighbours(send_near, group, 1, column)

    middle_y = jnp.logical_not(jnp.logical_or(first_y, last_y))
    some_y = jnp.logical_xor(first_y, last_y)
    no_y = jnp.logical_and(first_y, last_y)

    def over_y(act):
        pl.when(middle_y)(functools.partial(act, 2))
        pl.when(some_y)(functools.partial(act, 1))
        pl.when(no_y)(functools.partial(act, 0))

    table = 4 * parts * count

    def wait_leave_near(slot, near):
        over_y(lambda n: drain_slots(n + 1, slot))
        over_y(lambda n: drain_bytes((3 * by + n) * line, near))

    def wait_plane_slots(sem):
        over_y(lambda n: drain_slots(2 * n + 1, sem))

    def wait_plane_cells(sem):
        over_y(lambda n: drain_bytes((3 * by + n * (3 * bx + 1)) * line, sem))

    wait_plane_slots(slot_sem.at[0])
    wait_plane_cells(near_sem.at[0])
    drain_bytes((down - 1) * table, deform_sem.at[0])
    drain_bytes(down * table, deform_sem.at[1])
    index_middle = gather_index(place, near_slots, 1, 0)
    index_side = gather_index(place, near_slots, 1 - leave, -leave)
    weight_y, weight_z = spread_y[...], spread_z[...]
    middle_row = pick_row(place, held, 1, index_middle)
    refined[...] = refine_row(place, middle_row, weight_y, weight_z, True)
    middle[0:8] = middle_row[0]
    middle[8:9] = middle_row[1]
    side_row = pick_row(place, held, 1 - leave, index_side)
    side_row = [a - b for a, b in zip(side_row, middle_row)]
    diffs[0] = refine_row(place, side_row, weight_y, weight_z, False)

    for j in range(bx + 1):
        spot = place.slab(j) if j else jnp.where(place.leaves, place.slab(0), place.slab(1))
        put_volts(place, cells, volts, slopes, spot, j)
    slope = Slopes(place, volts, slopes, parts_x, parts_y, parts_z)

    def rim_of(number):
        pieces = [cells[number, place.slab(j), row : row + 1] for row in (TOP - 1, TOP + by) for j in range(1, bx + 1)]
        return jnp.concatenate(pieces, axis=0)

    rim_fiber = fiber_of(rim_of(1), rim_of(2))
    for number, value in enumerate(rim_fiber):
        rim_fibers[number] = value

    def mid(at):
        return refined[at : at + 8]

    def side(at):
        return diffs[0, at : at + 8]

    share = jnp.where(place.leaves, 1.0, 0.0)
    for j in range(half + 1):
        spot = place.slab(j)

        def fiber_at(rows, j=j, spot=spot):
            if j:
                return [fibers[number, spot - 1, rows] for number in range(3)]
            start = TOP + rows.start
            return fiber_of(*(cells[number, spot, start : start + 8] for number in (1, 2)))

        def note(rows, excess, j=j, spot=spot):
            voltage = load_rows(volts, (j,), TOP + rows.start, 8)
            partial[j - 1, rows] = base[spot - 1, rows] - excess * (voltage - 0.6)

        weight = share * abs((j - 0.5) / RATIO - 0.5)
        put_tensors(place, conducts, j, mid, side, weight, fiber_at, j == 0, note)
    put_rims(place, conducts, {j: j for j in range(1, half + 1)}, mid, side, rim_fiber, share)
    for j in range(bx):
        slope.along_x(j)
        slope.within(j + 1)
    for j in range(1, bx):
        slope.with_x(j)

    out = send_sem.at[0]
    wait_plane_slots(out)
    wait_plane_cells(out)
    drain_bytes((2 * down - 1) * table, out)

    @pl.when(place.leaves)
    def _():
        wait_leave_near(out, out)
        drain_bytes(down * table, out)

    @pl.when(place.leaves)
    def _():
        wait_leave_near(slot_sem.at[1], near_sem.at[1])
        index = gather_index(place, near_slots, 1 + leave, leave)
        drain_bytes(down * table, deform_sem.at[2])
        row = pick_row(place, held, 1 + leave, index)
        row = [a - b for a, b in zip(row, (middle[0:8], middle[8:9]))]
        diffs[1] = refine_row(place, row, spread_y[...], spread_z[...], False)


def compute(
    across,
    down,
    sizes,
    fibers,
    rim_fibers,
    refined,
    diffs,
    volts,
    slopes,
    parts_x,
    parts_y,
    parts_z,
    partial,
    base,
    recovered,
    early_conducts,
    cells,
    next_potential,
    next_recovery,
    conducts,
    result,
    out_sem,
):
    bx, by, nz = sizes[:3]
    place = Place(across, down, sizes)
    half = RATIO // 2

    pltpu.make_async_copy(recovered, next_recovery, out_sem.at[0]).start()

    which = jnp.where(place.leaves, 1, 0)
    put_volts(place, cells, volts, slopes, place.slab(bx + 1), bx + 1)
    slope = Slopes(place, volts, slopes, parts_x, parts_y, parts_z)
    slope.along_x(bx)
    slope.with_x(bx)

    def finish(j):
        target = next_potential.at[place.slab(j) - 1]
        pltpu.make_async_copy(result.at[j - 1], target, out_sem.at[0]).start()

    def mid(at):
        return refined[at : at + 8]

    def side(at):
        return diffs[which, at : at + 8]

    for j in range(half + 1, bx + 2):
        spot = place.slab(j)

        def fiber_at(rows, j=j, spot=spot):
            if j <= bx:
                return [fibers[number, spot - 1, rows] for number in range(3)]
            start = TOP + rows.start
            return fiber_of(*(cells[number, spot, start : start + 8] for number in (1, 2)))

        def note(rows, excess, j=j, spot=spot):
            voltage = load_rows(volts, (j,), TOP + rows.start, 8)
            result[j - 1, rows] = base[spot - 1, rows] - excess * (voltage - 0.6)

        weight = abs((j - 0.5) / RATIO - 0.5)
        put_tensors(place, conducts, j - half - 1, mid, side, weight, fiber_at, j == bx + 1, note)
    rim_fiber = [rim_fibers[number] for number in range(3)]
    put_rims(place, conducts, {j - half - 1: j for j in range(half + 1, bx + 1)}, mid, side, rim_fiber, 1.0)
    face_x, across_yz = make_flux(place, parts_x, parts_y, parts_z, early_conducts, conducts, half + 1)
    faces = [face_x(j) for j in range(bx + 1)]
    faces[0] = jnp.where(place.leaves, faces[0], 0.0)
    for j in range(1, bx + 1):
        local = partial[j - 1] if j <= half else result[j - 1]
        result[j - 1] = local + 0.1 * (across_yz(j) + (faces[j] - faces[j - 1]))
        finish(j)
    both = fibers.at[pl.ds(0, 2)]
    pltpu.make_async_copy(both, both, out_sem.at[0]).wait()


def solution(mesh):
    across, down = mesh.shape["gx"], mesh.shape["gy"]

    def local(potential, recovery, angles, deform, slots):
        bx, by, nz = potential.shape
        ex, ey, ez = slots.shape
        parts, count = deform.shape
        assert ex == 1 and bx == RATIO and by == RATIO * ey and by % 8 == 0
        assert count % LANES == 0 and parts == 9 and across % 2 == 0 and (2 * ez) % LANES == 0
        sizes = (bx, by, nz, ex, ey, ez, parts, count)
        blocks = count // LANES
        f32 = jnp.float32
        half = RATIO // 2
        shape = jax.ShapeDtypeStruct(potential.shape, f32)
        anywhere = pl.BlockSpec(memory_space=pl.ANY)
        in_vmem = pl.BlockSpec(memory_space=pltpu.VMEM)
        planes = nz // LANES
        fine = 9 * (by + 8)
        planes = nz // LANES
        fine = 9 * (by + 8)
        rows = pltpu.VMEM((bx + 2, planes, by + 16, LANES), f32)
        passed = (
            pltpu.VMEM((3, bx, by, nz), f32),
            pltpu.VMEM((3, 2 * bx, nz), f32),
            pltpu.VMEM((fine, nz), f32),
            pltpu.VMEM((2, fine, nz), f32),
            rows,
            rows,
            pltpu.VMEM((bx + 1, 3, by, nz), f32),
            pltpu.VMEM((bx, 2, 3, by, nz), f32),
            pltpu.VMEM((bx, 3, by, nz), f32),
            pltpu.VMEM((half, by, nz), f32),
            pltpu.VMEM((bx, by, nz), f32),
            pltpu.VMEM((bx, by, nz), f32),
            pltpu.VMEM((6, half + 1, planes, by + 16, LANES), f32),
            pltpu.VMEM((3, bx + 2, by + 16, nz), f32),
        )
        arrived = pl.pallas_call(
            functools.partial(exchange, across, down, sizes),
            out_shape=passed,
            in_specs=[pl.BlockSpec(memory_space=pltpu.MemorySpace.HBM)] * 5,
            out_specs=(in_vmem,) * len(passed),
            scratch_shapes=[
                pltpu.VMEM((3, down, 8 * blocks + 8, LANES), f32),
                pltpu.VMEM((3, 3, ex, ey, ez), jnp.int32),
                pltpu.VMEM(recovery.shape, f32),
                pltpu.VMEM((by + 8, WINDOW * ez), f32),
                pltpu.VMEM((WINDOW * ez, nz), jnp.bfloat16),
                pltpu.VMEM((16, (ey + 2) * ez), f32),
                pltpu.VMEM((max(4 * bx * by, 2 * down * parts * count // nz), 1, nz), f32),
                pltpu.VMEM((5, ex, ey, ez), jnp.int32),
                pltpu.SemaphoreType.DMA((1,)),
                pltpu.SemaphoreType.DMA((3,)),
                pltpu.SemaphoreType.DMA((2,)),
                pltpu.SemaphoreType.DMA((2,)),
                pltpu.SemaphoreType.DMA((3,)),
                pltpu.SemaphoreType.REGULAR((down,)),
                pltpu.SemaphoreType.REGULAR((down,)),
                pltpu.SemaphoreType.REGULAR,
            ],
            compiler_params=pltpu.CompilerParams(
                collective_id=0, has_side_effects=True, vmem_limit_bytes=VMEM_LIMIT
            ),
        )(*(pltpu.with_memory_space_constraint(x, pltpu.MemorySpace.HBM) for x in (potential, recovery, angles, deform, slots)))
        return pl.pallas_call(
            functools.partial(compute, across, down, sizes),
            out_shape=(shape, shape),
            in_specs=[in_vmem] * len(passed),
            out_specs=(anywhere,) * 2,
            scratch_shapes=[
                pltpu.VMEM((6, half + 1, planes, by + 16, LANES), f32),
                pltpu.VMEM((bx, by, nz), f32),
                pltpu.SemaphoreType.DMA((1,)),
            ],
            compiler_params=pltpu.CompilerParams(vmem_limit_bytes=VMEM_LIMIT),
        )(*arrived)

    return jax.shard_map(
        local,
        mesh=mesh,
        in_specs=(
            P("gx", "gy", None),
            P("gx", "gy", None),
            P(None, "gx", "gy", None),
            P(None, ("gx", "gy")),
            P("gx", "gy", None),
        ),
        out_specs=(P("gx", "gy", None), P("gx", "gy", None)),
        check_vma=False,
    )
```

```python
import functools

import jax
import jax.numpy as jnp
from jax import lax
from jax.experimental import pallas as pl
from jax.experimental.pallas import tpu as pltpu
from jax.sharding import PartitionSpec as P

MESH = pl.DeviceIdType.MESH
RATIO = 4
LANES = 128
VMEM_LIMIT = 16 * 1024 * 1024
TOP = 8
WINDOW = 4
FIBER_SCALE = (7.0 / 3.0) ** 0.5
STRETCH_SCALE = (3.0 / 7.0) ** 0.5
XX, YY, ZZ, XY, XZ, YZ = range(6)
PAIRS = ((0, 0), (1, 1), (2, 2), (0, 1), (0, 2), (1, 2))


def split_two(values):
    high = values.astype(jnp.bfloat16)
    low = (values - high.astype(jnp.float32)).astype(jnp.bfloat16)
    return high, low


def dot_two(values, weights):
    high, low = split_two(values)
    return jnp.dot(high, weights, preferred_element_type=jnp.float32) + jnp.dot(
        low, weights, preferred_element_type=jnp.float32
    )


def polynomial(terms, value):
    total = terms[-1]
    for term in terms[-2::-1]:
        total = total * value + term
    return total


HALF_SINE = (0.707106764632592, -0.02946274890445726, 3.682656229209654e-4, -2.187710743548062e-6, 7.155278665108425e-9)
HALF_COSINE = (1.414213496564441, -0.17677636064176425, 3.6825754039592376e-3, -3.0612650004537585e-5, 1.2790856262670407e-7)


def sine_cosine(angle):
    square = angle * angle
    sine = angle * polynomial(HALF_SINE, square)
    cosine = polynomial(HALF_COSINE, square)
    return sine * cosine, 1.0 - sine * sine


def fiber_of(azimuth, elevation):
    sin_u, cos_u = sine_cosine(azimuth)
    sin_e, cos_e = sine_cosine(elevation)
    flat = FIBER_SCALE * cos_e
    return cos_u * flat, sin_u * flat, FIBER_SCALE * sin_e


def tensor_of(entries, fiber, sign, wanted):
    def element(i, j):
        return entries[3 * (i % 3) + j % 3]

    adjugate = [
        [
            element(j + 1, i + 1) * element(j + 2, i + 2)
            - element(j + 1, i + 2) * element(j + 2, i + 1)
            for j in range(3)
        ]
        for i in range(3)
    ]
    determinant = (
        element(0, 0) * adjugate[0][0]
        + element(0, 1) * adjugate[1][0]
        + element(0, 2) * adjugate[2][0]
    )
    inverse = 1.0 / determinant
    square = inverse * inverse
    diagonal = (0.3 * 0.5) * square
    mixed = (0.3 * 0.125) * square
    mirrored = (0.3 * 0.125 * sign) * square
    rows = sorted({i for number in wanted for i in PAIRS[number]})
    pulled = {
        i: adjugate[i][0] * fiber[0] + adjugate[i][1] * fiber[1] + adjugate[i][2] * fiber[2]
        for i in rows
    }
    scale = {XX: diagonal, YY: diagonal, ZZ: diagonal, XY: mirrored, XZ: mirrored, YZ: mixed}
    conduct = {}
    for number in wanted:
        i, j = PAIRS[number]
        metric = (
            adjugate[i][0] * adjugate[j][0]
            + adjugate[i][1] * adjugate[j][1]
            + adjugate[i][2] * adjugate[j][2]
        )
        conduct[number] = scale[number] * (metric + pulled[i] * pulled[j])
    return conduct


def excess_of(entries, fiber):
    parts = [
        entries[3 * i] * fiber[0] + entries[3 * i + 1] * fiber[1] + entries[3 * i + 2] * fiber[2]
        for i in range(3)
    ]
    square = parts[0] * parts[0] + parts[1] * parts[1] + parts[2] * parts[2]
    return jnp.maximum(STRETCH_SCALE * (square * lax.rsqrt(square)) - 1.0, 0.0)


class Place:
    def __init__(self, across, down, sizes):
        self.across, self.down, self.sizes = across, down, sizes
        self.gx, self.gy = lax.axis_index("gx"), lax.axis_index("gy")
        self.first_x, self.last_x = self.gx == 0, self.gx == across - 1
        self.first_y, self.last_y = self.gy == 0, self.gy == down - 1
        odd = lax.rem(self.gx, 2)
        self.odd = odd
        self.leave = 2 * odd - 1
        self.leaves = jnp.logical_not(jnp.logical_or(self.first_x, self.last_x))
        self.late = jnp.where(self.leaves, self.leave, -self.leave)
        self.sign = jnp.where(self.late > 0, 1.0, -1.0)

    def slab(self, j):
        last = self.sizes[0] + 1
        return jnp.where(self.late > 0, j, last - j)


def load_rows(ref, at, start, size):
    planes = [ref[(*at, part, slice(start, start + size))] for part in range(ref.shape[-3])]
    return jnp.concatenate(planes, axis=1)


def store_rows(ref, at, start, value):
    for part in range(ref.shape[-3]):
        rows = slice(start, start + value.shape[0])
        ref[(*at, part, rows)] = value[:, part * LANES : (part + 1) * LANES]


def gather_index(place, near_slots, q, offset):
    ey = place.sizes[4]
    low = jnp.where(place.first_y, near_slots[q, 1, 0, 0:1], near_slots[q, 0, 0, ey - 1 : ey])
    high = jnp.where(place.last_y, near_slots[q, 1, 0, ey - 1 : ey], near_slots[q, 2, 0, 0:1])
    pieces = [low] + [near_slots[q, 1, 0, c : c + 1] for c in range(ey)] + [high]
    count = place.sizes[7]
    return jnp.concatenate(pieces, axis=1) - (place.gx + offset) * (place.down * count)


def page_of(index):
    return index >> (LANES.bit_length() - 1)


def keep_page(rows, page):
    kept = lax.broadcasted_iota(jnp.int32, rows.shape, 0) == page
    return jnp.sum(jnp.where(kept, rows, 0.0), axis=0, keepdims=True)


def pick_row(place, held, q, index):
    blocks = place.sizes[7] // LANES
    totals, lasts = [], []
    for t in range(index.shape[1] // LANES):
        lanes = index[:, t * LANES : (t + 1) * LANES]
        page = page_of(lanes)
        spot = jnp.broadcast_to(lanes & (LANES - 1), (8, LANES))

        def take(rows):
            return jnp.take_along_axis(rows, spot, axis=1, mode="promise_in_bounds")

        total = None
        tails = []
        for h in range(place.down):
            tails.append(held[q, h, 8 * blocks : 9 * blocks])
            for b in range(blocks):
                found = take(held[q, h, 8 * b : 8 * b + 8])
                total = found if total is None else jnp.where(page == h * blocks + b, found, total)
        totals.append(total)
        tails = jnp.concatenate(tails, axis=0)
        last = None
        for g in range(0, place.down * blocks, 8):
            part = keep_page(take(tails[g : g + 8]), page - g)
            last = part if last is None else last + part
        lasts.append(last)
    return jnp.concatenate(totals, axis=1), jnp.concatenate(lasts, axis=1)


def refine_row(place, row, weight_y, weight_z, whole):
    by, ez = place.sizes[1], place.sizes[5]
    total, last = row
    span = WINDOW * ez
    spread = []
    for k in range(9):
        values = total[k : k + 1] if k < 8 else last
        for half in range(by // 8):
            at = 2 * half * ez
            spread.append(weight_y[8 * half : 8 * half + 8] * values[:, at : at + span])
        at = (by // 4 - 2) * ez
        rim = lax.broadcasted_iota(jnp.int32, (8, span), 0) < 4
        spread.append(weight_y[by : by + 8] * jnp.where(rim, values[:, 0:span], values[:, at : at + span]))
    spread = jnp.concatenate(spread, axis=0)
    if whole:
        return dot_two(spread, weight_z)
    return jnp.dot(spread.astype(jnp.bfloat16), weight_z, preferred_element_type=jnp.float32)


def rolls(nz, by):
    lane = lax.broadcasted_iota(jnp.int32, (by, nz), 1)

    def ahead(values):
        return pltpu.roll(values, nz - 1, 1)

    def behind(values):
        return pltpu.roll(values, 1, 1)

    return lane, ahead, behind


def grad_z(values):
    nz = values.shape[1]
    lane, ahead, behind = rolls(nz, values.shape[0])
    upper = jnp.where(lane == nz - 1, values, ahead(values))
    lower = jnp.where(lane == 0, values, behind(values))
    return upper - lower


class Slopes:
    def __init__(self, place, volts, slopes, parts_x, parts_y, parts_z):
        self.place, self.volts, self.slopes = place, volts, slopes
        self.parts_x, self.parts_y, self.parts_z = parts_x, parts_y, parts_z

    def volt(self, j, shift=0):
        return load_rows(self.volts, (j,), TOP + shift, self.place.sizes[1])

    def slope_z(self, j, shift=0):
        return load_rows(self.slopes, (j,), TOP + shift, self.place.sizes[1])

    def slope_y(self, j):
        return self.volt(j, 1) - self.volt(j, -1)

    def slope_x(self, j, shift=0):
        return self.volt(j + 1, shift) - self.volt(j - 1, shift)

    def pair(self, values):
        return values + pltpu.roll(values, values.shape[1] - 1, 1)

    def along_x(self, j):
        self.parts_x[j, 0] = self.volt(j + 1) - self.volt(j)
        self.parts_x[j, 1] = self.slope_y(j) + self.slope_y(j + 1)
        self.parts_x[j, 2] = self.slope_z(j) + self.slope_z(j + 1)

    def with_x(self, j):
        for side, shift in enumerate((1, -1)):
            self.parts_y[j - 1, side, 0] = self.slope_x(j) + self.slope_x(j, shift)
        self.parts_z[j - 1, 0] = self.pair(self.slope_x(j))

    def within(self, j):
        here = self.volt(j)
        for side, shift in enumerate((1, -1)):
            self.parts_y[j - 1, side, 1] = shift * (self.volt(j, shift) - here)
            self.parts_y[j - 1, side, 2] = self.slope_z(j) + self.slope_z(j, shift)
        self.parts_z[j - 1, 1] = self.pair(self.slope_y(j))
        self.parts_z[j - 1, 2] = pltpu.roll(here, here.shape[1] - 1, 1) - here


def make_flux(place, parts_x, parts_y, parts_z, early, late, first):
    by, nz = place.sizes[1:3]
    lane, ahead, behind = rolls(nz, by)
    y_row = lax.broadcasted_iota(jnp.int32, (by, nz), 0)

    def tensor(number, j, shift=0):
        at = (number, j) if j < first else (number, j - first)
        return load_rows(early if j < first else late, at, TOP + shift, by)

    def face_x(j):
        terms = [
            (tensor(number, j) + tensor(number, j + 1)) * parts_x[j, part]
            for part, number in enumerate((XX, XY, XZ))
        ]
        return terms[0] + terms[1] + terms[2]

    def face_y(j, side, shift):
        terms = [
            (tensor(number, j) + tensor(number, j, shift)) * parts_y[j - 1, side, part]
            for part, number in enumerate((XY, YY, YZ))
        ]
        return terms[0] + terms[1] + terms[2]

    def across_yz(j):
        upper = jnp.where(jnp.logical_and(y_row == by - 1, place.last_y), 0.0, face_y(j, 0, 1))
        lower = jnp.where(jnp.logical_and(y_row == 0, place.first_y), 0.0, face_y(j, 1, -1))
        terms = []
        for part, number in enumerate((XZ, YZ, ZZ)):
            mine = tensor(number, j)
            terms.append((mine + ahead(mine)) * parts_z[j - 1, part])
        face_z = jnp.where(lane == nz - 1, 0.0, terms[0] + terms[1] + terms[2])
        return (upper - lower) + (face_z - behind(face_z))

    return face_x, across_yz


def put_tensors(place, conducts, slot, mid, side, weight, fiber_at, halo, note):
    by = place.sizes[1]
    tall = by + 8
    for half in range(by // 8):
        rows = slice(8 * half, 8 * half + 8)
        entries = []
        for k in range(9):
            at = tall * k + 8 * half
            entries.append(mid(at) + weight * side(at))
        fiber = fiber_at(rows)
        wanted = (XX, XY, XZ) if halo else tuple(range(6))
        for number, value in tensor_of(entries, fiber, place.sign, wanted).items():
            store_rows(conducts, (number, slot), TOP + 8 * half, value)
        if not halo:
            note(rows, excess_of(entries, fiber))


def put_rims(place, conducts, slabs, mid, side, rim_fiber, share):
    bx, by, nz = place.sizes[:3]
    tall = by + 8
    row = lax.rem(lax.broadcasted_iota(jnp.int32, (8, nz), 0), bx)
    weight = jnp.zeros((8, nz), jnp.float32)
    for j in slabs.values():
        weight = jnp.where(row == j - 1, share * abs((j - 0.5) / RATIO - 0.5), weight)
    entries = []
    for k in range(9):
        entries.append(mid(tall * k + by) + weight * side(tall * k + by))
    for number, value in tensor_of(entries, rim_fiber, place.sign, (YY, XY, YZ)).items():
        for slot, j in slabs.items():
            store_rows(conducts, (number, slot), TOP - 1, value[j - 1 : j])
            store_rows(conducts, (number, slot), TOP + by, value[bx + j - 1 : bx + j])


def put_volts(place, cells, volts, slopes, spot, slot):
    by = place.sizes[1]
    own = cells[0, spot, TOP : TOP + by]
    low, high = cells[0, spot, TOP - 1 : TOP], cells[0, spot, TOP + by : TOP + by + 1]
    low = jnp.where(place.first_y, own[0:1], low)
    high = jnp.where(place.last_y, own[by - 1 : by], high)
    for start, value in ((TOP, own), (TOP - 1, low), (TOP + by, high)):
        store_rows(volts, (slot,), start, value)
        store_rows(slopes, (slot,), start, grad_z(value))


def exchange(
    across,
    down,
    sizes,
    potential,
    recovery,
    angles,
    deform,
    slots,
    fibers,
    rim_fibers,
    refined,
    diffs,
    volts,
    slopes,
    parts_x,
    parts_y,
    parts_z,
    partial,
    base,
    next_recovery,
    conducts,
    cells,
    held,
    near_slots,
    rest_in,
    spread_y,
    spread_z,
    middle,
    gauge,
    slot_gauge,
    send_sem,
    slot_sem,
    near_sem,
    local_sem,
    plane_ready,
    leave_ready,
    equal_ready,
):
    bx, by, nz, ex, ey, ez, parts, count = sizes
    blocks = count // LANES
    place = Place(across, down, sizes)
    half = RATIO // 2
    gx, gy = place.gx, place.gy
    first_y, last_y, leave = place.first_y, place.last_y, place.leave
    for b in range(blocks):
        columns = pl.ds(b * LANES, LANES)
        pltpu.make_async_copy(
            deform.at[pl.ds(0, 8), columns], held.at[1, gy, pl.ds(8 * b, 8)], local_sem.at[0]
        ).start()
        pltpu.make_async_copy(
            deform.at[pl.ds(8, 1), columns], held.at[1, gy, pl.ds(8 * blocks + b, 1)], local_sem.at[0]
        ).start()
    inside = pl.ds(TOP, by)
    pltpu.make_async_copy(slots, near_slots.at[1, 1], local_sem.at[2]).start()
    pltpu.make_async_copy(potential, cells.at[0, pl.ds(1, bx), inside], local_sem.at[1]).start()
    pltpu.make_async_copy(angles, cells.at[pl.ds(1, 2), pl.ds(1, bx), inside], local_sem.at[1]).start()
    pltpu.make_async_copy(recovery, rest_in, local_sem.at[1]).start()

    sides = ((leave, place.leaves), (-leave, None))

    def when(check, act):
        if check is None:
            act()
        else:
            pl.when(check)(act)

    bits = max(down - 1, 1).bit_length()
    odd = place.odd

    def hops_of(column):
        if isinstance(column, int):
            return column.bit_count()
        hops = 0
        for _ in range(bits):
            halved = column // 2
            hops = hops + column - 2 * halved
            column = halved
        return hops

    own_hops = hops_of(gy)

    def above_of(dx, hops):
        chips = leave if dx is leave else 0
        return 4 * (chips + hops - own_hops) + chips

    columns_by_hops = sorted(range(down), key=lambda column: (column.bit_count(), column))

    def peers(act, groups):
        for group in groups:
            rows = ((leave,),) if group else ((-leave, 0),)

            def visit(rows=rows[0]):
                for column in columns_by_hops:
                    for dx in rows:
                        act(dx, column, above_of(dx, hops_of(column)))

            when(place.leaves if group else None, visit)

    def other(dx, column):
        return column != gy if isinstance(dx, int) else True

    def guarded(test, act):
        def visit(dx, column, above):
            pl.when(jnp.logical_and(test(above), other(dx, column)))(functools.partial(act, dx, column))

        return visit

    upper_core = odd == 1

    def meets(dx, above, column):
        even_row = odd == 0 if isinstance(dx, int) else odd == 1
        return jnp.logical_or(above < 0, jnp.logical_and(above == 0, jnp.logical_or(jnp.logical_not(even_row), column == gy)))

    def lower(act):
        def visit(dx, column, above):
            here = jnp.logical_and(meets(0, above, column), other(dx, column))
            pl.when(here)(functools.partial(act, dx, column))

        return visit

    def level(act):
        def visit(dx, column, above):
            there = jnp.logical_and(meets(dx, -above, column), other(dx, column))
            pl.when(there)(functools.partial(act, dx, column))

        return visit

    def equal(act):
        def visit(dx, column, above):
            pl.when(jnp.logical_and(above == 0, column != gy))(functools.partial(act, dx, column))

        return visit

    def beneath(act):
        return guarded(lambda above: above < 0, act)

    def higher(act):
        return guarded(lambda above: above > 0, act)

    near_hops = {dy: hops_of(gy + dy) for dy in (-1, 0, 1)}
    barrier = pltpu.get_barrier_semaphore()

    def tell(sem, dx, column):
        pl.semaphore_signal(sem, inc=1, device_id=(gx + dx, column), device_id_type=MESH)

    peers(level(functools.partial(tell, barrier)), (0, 1))
    below = 0
    equals = 0
    plane_above, leave_above = [], []
    for column in range(down):
        higher_here = 0
        for dx in (-leave, 0):
            above = above_of(dx, hops_of(column))
            below = below + jnp.where(jnp.logical_and(meets(0, above, column), other(dx, column)), 1, 0)
            higher_here = higher_here + jnp.where(above > 0, 1, 0)
            equals = equals + jnp.where(jnp.logical_and(above == 0, column != gy), 1, 0)
        plane_above.append(higher_here)
        above = above_of(leave, hops_of(column))
        below = below + jnp.where(jnp.logical_and(place.leaves, meets(0, above, column)), 1, 0)
        leave_above.append(jnp.where(jnp.logical_and(place.leaves, above > 0), 1, 0))

    pl.semaphore_wait(barrier, below)
    pl.when(upper_core)(lambda: tell(equal_ready, -1, gy))
    peers(beneath(functools.partial(tell, leave_ready.at[gy])), (1,))
    peers(beneath(functools.partial(tell, plane_ready.at[gy])), (0,))

    def drain(ref, sem):
        pltpu.make_async_copy(ref, ref, sem).wait()

    rows = pl.ds(0, 9 * blocks)
    line = 4 * nz

    def drain_bytes(amount, sem):
        assert amount % line == 0
        drain(gauge.at[pl.ds(0, amount // line)], sem)

    def drain_slots(amount, sem):
        drain(slot_gauge.at[pl.ds(0, amount)], sem)

    drain(held.at[1, gy, rows], local_sem.at[0])
    drain_slots(1, local_sem.at[2])

    def put(source, target, sem, dx, where):
        pltpu.make_async_remote_copy(
            src_ref=source,
            dst_ref=target,
            send_sem=send_sem.at[0],
            recv_sem=sem,
            device_id=(gx + dx, where),
            device_id_type=MESH,
        ).start()

    def near_of(dx):
        return 0 if isinstance(dx, int) else jnp.where(dx == leave, 1, 0)

    def table_of(dx):
        return 2 if isinstance(dx, int) else jnp.where(dx == leave, 1, 2)

    def send_deform(dx, column):
        q = 1 - dx
        put(held.at[1, gy, rows], held.at[q, gy, rows], near_sem.at[table_of(dx)], dx, column)

    def send_slots(dx, dy):
        put(near_slots.at[1, 1], near_slots.at[1 - dx, 1 - dy], slot_sem.at[near_of(dx)], dx, gy + dy)

    def send_cells(dx, dy):
        y_source = inside if dy == 0 else pl.ds(TOP if dy < 0 else TOP + by - 1, 1)
        y_target = inside if dy == 0 else pl.ds(TOP + by if dy < 0 else TOP - 1, 1)
        if isinstance(dx, int):
            x_source = x_target = pl.ds(1, bx)
        else:
            x_source = pl.ds(jnp.where(dx < 0, 1, bx), 1)
            x_target = pl.ds(jnp.where(dx < 0, bx + 1, 0), 1)
        corner = dy != 0 and not isinstance(dx, int)
        fields = pl.ds(0, 1 if corner else 3)
        source, target = cells.at[fields, x_source, y_source], cells.at[fields, x_target, y_target]
        put(source, target, near_sem.at[near_of(dx)], dx, gy + dy)

    def neighbours(act, group, sign, column=None):
        for dx in (leave,) if group else (-leave, 0):
            for dy in (-1, 0, 1):
                if isinstance(dx, int) and dy == 0:
                    continue
                above = above_of(dx, near_hops[dy])
                if sign > 0:
                    check = above > 0
                elif sign < 0:
                    check = meets(0, above, gy + dy)
                else:
                    check = jnp.logical_and(above == 0, dy != 0)
                if column is not None:
                    check = jnp.logical_and(check, gy + dy == column)
                if dy:
                    check = jnp.logical_and(check, jnp.logical_not(first_y if dy < 0 else last_y))
                if group:
                    check = jnp.logical_and(check, place.leaves)
                pl.when(check)(functools.partial(act, dx, dy))

    def local_work():
        width = WINDOW * ez
        row = lax.broadcasted_iota(jnp.int32, (by + 8, width), 0)
        lane = lax.broadcasted_iota(jnp.int32, (by + 8, width), 1)
        low = row < by + bx
        cell = jnp.where(row < by, row, jnp.where(low, -1, by))
        start = jnp.where(row < by, 2 * (row // 8), jnp.where(low, 0, ey - 2))
        spot = (cell.astype(jnp.float32) + 0.5) * (1.0 / RATIO) - 0.5
        coarse = (lane // ez + start - 1).astype(jnp.float32)
        spread_y[...] = jnp.maximum(1.0 - jnp.abs(spot - coarse), 0.0)
        row = lax.broadcasted_iota(jnp.int32, (width, nz), 0)
        lane = lax.broadcasted_iota(jnp.int32, (width, nz), 1)
        spot = jnp.clip((lane.astype(jnp.float32) + 0.5) * (1.0 / RATIO) - 0.5, 0.0, ez - 1.0)
        weight = jnp.maximum(1.0 - jnp.abs(spot - lax.rem(row, ez).astype(jnp.float32)), 0.0)
        spread_z[...] = weight.astype(jnp.bfloat16)
        for s in range(bx):
            own = [cells[number, s + 1, TOP : TOP + by] for number in (1, 2)]
            for number, part in enumerate(fiber_of(*own)):
                fibers[number, s] = part
            voltage = cells[0, s + 1, TOP : TOP + by]
            resting = rest_in[s]
            next_recovery[s] = resting + 0.05 * (-resting - 8.0 * voltage * (voltage - 1.15))
            current = 8.0 * voltage * (voltage - 0.15) * (voltage - 1.0) + voltage * resting
            base[s] = voltage - 0.1 * current

    peers(lower(send_deform), (1, 0))
    for group in (0, 1):
        neighbours(send_slots, group, -1)
    drain_bytes(4 * bx * by * line, local_sem.at[1])
    for group in (1, 0):
        neighbours(send_cells, group, -1)
    local_work()

    def send_near(dx, dy):
        send_slots(dx, dy)
        send_cells(dx, dy)

    @pl.when(jnp.logical_not(upper_core))
    def _():
        pl.semaphore_wait(equal_ready, 1)

        @pl.when(equals > 0)
        def _():
            peers(equal(send_deform), (0,))
            neighbours(send_near, 0, 0)

    for group, ready, counts in ((0, plane_ready, plane_above), (1, leave_ready, leave_above)):
        for column in columns_by_hops:

            @pl.when(counts[column] > 0)
            def _(group=group, ready=ready, counts=counts, column=column):
                pl.semaphore_wait(ready.at[column], counts[column])
                for dx in (leave,) if group else (-leave, 0):
                    higher(send_deform)(dx, column, above_of(dx, hops_of(column)))
                neighbours(send_near, group, 1, column)

    middle_y = jnp.logical_not(jnp.logical_or(first_y, last_y))
    some_y = jnp.logical_xor(first_y, last_y)
    no_y = jnp.logical_and(first_y, last_y)

    def over_y(act):
        pl.when(middle_y)(functools.partial(act, 2))
        pl.when(some_y)(functools.partial(act, 1))
        pl.when(no_y)(functools.partial(act, 0))

    table = 4 * parts * count

    def wait_leave_near(slot, near):
        over_y(lambda n: drain_slots(n + 1, slot))
        over_y(lambda n: drain_bytes(down * table + (3 * by + n) * line, near))

    def wait_plane_slots(sem):
        over_y(lambda n: drain_slots(2 * n + 1, sem))

    def wait_plane(sem):
        over_y(lambda n: drain_bytes((3 * by + n * (3 * bx + 1)) * line, sem))

    wait_plane_slots(slot_sem.at[0])
    wait_plane(near_sem.at[0])
    index_middle = gather_index(place, near_slots, 1, 0)
    index_side = gather_index(place, near_slots, 1 - leave, -leave)
    for j in range(bx + 1):
        spot = place.slab(j) if j else jnp.where(place.leaves, place.slab(0), place.slab(1))
        put_volts(place, cells, volts, slopes, spot, j)
    slope = Slopes(place, volts, slopes, parts_x, parts_y, parts_z)

    def rim_of(number):
        pieces = [cells[number, place.slab(j), row : row + 1] for row in (TOP - 1, TOP + by) for j in range(1, bx + 1)]
        return jnp.concatenate(pieces, axis=0)

    rim_fiber = fiber_of(rim_of(1), rim_of(2))
    for number, value in enumerate(rim_fiber):
        rim_fibers[number] = value

    for j in range(bx):
        slope.along_x(j)
        slope.within(j + 1)
    for j in range(1, bx):
        slope.with_x(j)

    drain_bytes((2 * down - 1) * table, near_sem.at[2])
    weight_y, weight_z = spread_y[...], spread_z[...]
    middle_row = pick_row(place, held, 1, index_middle)
    refined[...] = refine_row(place, middle_row, weight_y, weight_z, True)
    middle[0:8] = middle_row[0]
    middle[8:9] = middle_row[1]
    side_row = pick_row(place, held, 1 - leave, index_side)
    side_row = [a - b for a, b in zip(side_row, middle_row)]
    diffs[0] = refine_row(place, side_row, weight_y, weight_z, False)

    def mid(at):
        return refined[at : at + 8]

    def side(at):
        return diffs[0, at : at + 8]

    share = jnp.where(place.leaves, 1.0, 0.0)
    def early_slab(j):
        spot = place.slab(j)

        def fiber_at(rows):
            if j:
                return [fibers[number, spot - 1, rows] for number in range(3)]
            start = TOP + rows.start
            return fiber_of(*(cells[number, spot, start : start + 8] for number in (1, 2)))

        def note(rows, excess):
            voltage = load_rows(volts, (j,), TOP + rows.start, 8)
            partial[j - 1, rows] = base[spot - 1, rows] - excess * (voltage - 0.6)

        weight = share * abs((j - 0.5) / RATIO - 0.5)
        put_tensors(place, conducts, j, mid, side, weight, fiber_at, j == 0, note)

    for j in range(1, half + 1):
        early_slab(j)
    put_rims(place, conducts, {j: j for j in range(1, half + 1)}, mid, side, rim_fiber, share)
    out = send_sem.at[0]
    wait_plane_slots(out)
    wait_plane(out)
    drain_bytes((2 * down - 1) * table, out)

    @pl.when(place.leaves)
    def _():
        wait_leave_near(out, out)

    @pl.when(place.leaves)
    def _():
        wait_leave_near(slot_sem.at[1], near_sem.at[1])
        index = gather_index(place, near_slots, 1 + leave, leave)
        row = pick_row(place, held, 1 + leave, index)
        row = [a - b for a, b in zip(row, (middle[0:8], middle[8:9]))]
        diffs[1] = refine_row(place, row, spread_y[...], spread_z[...], False)
        early_slab(0)


def compute(
    across,
    down,
    sizes,
    fibers,
    rim_fibers,
    refined,
    diffs,
    volts,
    slopes,
    parts_x,
    parts_y,
    parts_z,
    partial,
    base,
    recovered,
    early_conducts,
    cells,
    next_potential,
    next_recovery,
    conducts,
    result,
    out_sem,
):
    bx, by, nz = sizes[:3]
    place = Place(across, down, sizes)
    half = RATIO // 2

    pltpu.make_async_copy(recovered, next_recovery, out_sem.at[0]).start()

    which = jnp.where(place.leaves, 1, 0)
    put_volts(place, cells, volts, slopes, place.slab(bx + 1), bx + 1)
    slope = Slopes(place, volts, slopes, parts_x, parts_y, parts_z)
    slope.along_x(bx)
    slope.with_x(bx)

    def finish(j):
        target = next_potential.at[place.slab(j) - 1]
        pltpu.make_async_copy(result.at[j - 1], target, out_sem.at[0]).start()

    def mid(at):
        return refined[at : at + 8]

    def side(at):
        return diffs[which, at : at + 8]

    for j in range(half + 1, bx + 2):
        spot = place.slab(j)

        def fiber_at(rows, j=j, spot=spot):
            if j <= bx:
                return [fibers[number, spot - 1, rows] for number in range(3)]
            start = TOP + rows.start
            return fiber_of(*(cells[number, spot, start : start + 8] for number in (1, 2)))

        def note(rows, excess, j=j, spot=spot):
            voltage = load_rows(volts, (j,), TOP + rows.start, 8)
            result[j - 1, rows] = base[spot - 1, rows] - excess * (voltage - 0.6)

        weight = abs((j - 0.5) / RATIO - 0.5)
        put_tensors(place, conducts, j - half - 1, mid, side, weight, fiber_at, j == bx + 1, note)
    rim_fiber = [rim_fibers[number] for number in range(3)]
    put_rims(place, conducts, {j - half - 1: j for j in range(half + 1, bx + 1)}, mid, side, rim_fiber, 1.0)
    face_x, across_yz = make_flux(place, parts_x, parts_y, parts_z, early_conducts, conducts, half + 1)
    faces = [face_x(j) for j in range(bx + 1)]
    faces[0] = jnp.where(place.leaves, faces[0], 0.0)
    for j in range(1, bx + 1):
        local = partial[j - 1] if j <= half else result[j - 1]
        result[j - 1] = local + 0.1 * (across_yz(j) + (faces[j] - faces[j - 1]))
        finish(j)
    both = fibers.at[pl.ds(0, 2)]
    pltpu.make_async_copy(both, both, out_sem.at[0]).wait()


def solution(mesh):
    across, down = mesh.shape["gx"], mesh.shape["gy"]

    def local(potential, recovery, angles, deform, slots):
        bx, by, nz = potential.shape
        ex, ey, ez = slots.shape
        parts, count = deform.shape
        assert ex == 1 and bx == RATIO and by == RATIO * ey and by % 8 == 0
        assert count % LANES == 0 and parts == 9 and across % 2 == 0 and (2 * ez) % LANES == 0
        sizes = (bx, by, nz, ex, ey, ez, parts, count)
        blocks = count // LANES
        f32 = jnp.float32
        half = RATIO // 2
        shape = jax.ShapeDtypeStruct(potential.shape, f32)
        anywhere = pl.BlockSpec(memory_space=pl.ANY)
        in_vmem = pl.BlockSpec(memory_space=pltpu.VMEM)
        planes = nz // LANES
        fine = 9 * (by + 8)
        planes = nz // LANES
        fine = 9 * (by + 8)
        rows = pltpu.VMEM((bx + 2, planes, by + 16, LANES), f32)
        passed = (
            pltpu.VMEM((3, bx, by, nz), f32),
            pltpu.VMEM((3, 2 * bx, nz), f32),
            pltpu.VMEM((fine, nz), f32),
            pltpu.VMEM((2, fine, nz), f32),
            rows,
            rows,
            pltpu.VMEM((bx + 1, 3, by, nz), f32),
            pltpu.VMEM((bx, 2, 3, by, nz), f32),
            pltpu.VMEM((bx, 3, by, nz), f32),
            pltpu.VMEM((half, by, nz), f32),
            pltpu.VMEM((bx, by, nz), f32),
            pltpu.VMEM((bx, by, nz), f32),
            pltpu.VMEM((6, half + 1, planes, by + 16, LANES), f32),
            pltpu.VMEM((3, bx + 2, by + 16, nz), f32),
        )
        arrived = pl.pallas_call(
            functools.partial(exchange, across, down, sizes),
            out_shape=passed,
            in_specs=[pl.BlockSpec(memory_space=pltpu.MemorySpace.HBM)] * 5,
            out_specs=(in_vmem,) * len(passed),
            scratch_shapes=[
                pltpu.VMEM((3, down, 8 * blocks + 8, LANES), f32),
                pltpu.VMEM((3, 3, ex, ey, ez), jnp.int32),
                pltpu.VMEM(recovery.shape, f32),
                pltpu.VMEM((by + 8, WINDOW * ez), f32),
                pltpu.VMEM((WINDOW * ez, nz), jnp.bfloat16),
                pltpu.VMEM((16, (ey + 2) * ez), f32),
                pltpu.VMEM((4 * bx * by + 2 * down * parts * count // nz, 1, nz), f32),
                pltpu.VMEM((5, ex, ey, ez), jnp.int32),
                pltpu.SemaphoreType.DMA((1,)),
                pltpu.SemaphoreType.DMA((2,)),
                pltpu.SemaphoreType.DMA((3,)),
                pltpu.SemaphoreType.DMA((3,)),
                pltpu.SemaphoreType.REGULAR((down,)),
                pltpu.SemaphoreType.REGULAR((down,)),
                pltpu.SemaphoreType.REGULAR,
            ],
            compiler_params=pltpu.CompilerParams(
                collective_id=0, has_side_effects=True, vmem_limit_bytes=VMEM_LIMIT
            ),
        )(*(pltpu.with_memory_space_constraint(x, pltpu.MemorySpace.HBM) for x in (potential, recovery, angles, deform, slots)))
        return pl.pallas_call(
            functools.partial(compute, across, down, sizes),
            out_shape=(shape, shape),
            in_specs=[in_vmem] * len(passed),
            out_specs=(anywhere,) * 2,
            scratch_shapes=[
                pltpu.VMEM((6, half + 1, planes, by + 16, LANES), f32),
                pltpu.VMEM((bx, by, nz), f32),
                pltpu.SemaphoreType.DMA((1,)),
            ],
            compiler_params=pltpu.CompilerParams(vmem_limit_bytes=VMEM_LIMIT),
        )(*arrived)

    return jax.shard_map(
        local,
        mesh=mesh,
        in_specs=(
            P("gx", "gy", None),
            P("gx", "gy", None),
            P(None, "gx", "gy", None),
            P(None, ("gx", "gy")),
            P("gx", "gy", None),
        ),
        out_specs=(P("gx", "gy", None), P("gx", "gy", None)),
        check_vma=False,
    )
```

```python
import functools

import jax
import jax.numpy as jnp
from jax import lax
from jax.experimental import pallas as pl
from jax.experimental.pallas import tpu as pltpu
from jax.sharding import PartitionSpec as P

MESH = pl.DeviceIdType.MESH
RATIO = 4
LANES = 128
VMEM_LIMIT = 16 * 1024 * 1024
TOP = 8
WINDOW = 4
FIBER_SCALE = (7.0 / 3.0) ** 0.5
STRETCH_SCALE = (3.0 / 7.0) ** 0.5
XX, YY, ZZ, XY, XZ, YZ = range(6)
PAIRS = ((0, 0), (1, 1), (2, 2), (0, 1), (0, 2), (1, 2))


def split_two(values):
    high = values.astype(jnp.bfloat16)
    low = (values - high.astype(jnp.float32)).astype(jnp.bfloat16)
    return high, low


def dot_two(values, weights):
    high, low = split_two(values)
    return jnp.dot(high, weights, preferred_element_type=jnp.float32) + jnp.dot(
        low, weights, preferred_element_type=jnp.float32
    )


def polynomial(terms, value):
    total = terms[-1]
    for term in terms[-2::-1]:
        total = total * value + term
    return total


HALF_SINE = (0.707106764632592, -0.02946274890445726, 3.682656229209654e-4, -2.187710743548062e-6, 7.155278665108425e-9)
HALF_COSINE = (1.414213496564441, -0.17677636064176425, 3.6825754039592376e-3, -3.0612650004537585e-5, 1.2790856262670407e-7)


def sine_cosine(angle):
    square = angle * angle
    sine = angle * polynomial(HALF_SINE, square)
    cosine = polynomial(HALF_COSINE, square)
    return sine * cosine, 1.0 - sine * sine


def fiber_of(azimuth, elevation):
    sin_u, cos_u = sine_cosine(azimuth)
    sin_e, cos_e = sine_cosine(elevation)
    flat = FIBER_SCALE * cos_e
    return cos_u * flat, sin_u * flat, FIBER_SCALE * sin_e


def tensor_of(entries, fiber, sign, wanted):
    def element(i, j):
        return entries[3 * (i % 3) + j % 3]

    adjugate = [
        [
            element(j + 1, i + 1) * element(j + 2, i + 2)
            - element(j + 1, i + 2) * element(j + 2, i + 1)
            for j in range(3)
        ]
        for i in range(3)
    ]
    determinant = (
        element(0, 0) * adjugate[0][0]
        + element(0, 1) * adjugate[1][0]
        + element(0, 2) * adjugate[2][0]
    )
    inverse = 1.0 / determinant
    square = inverse * inverse
    diagonal = (0.3 * 0.5) * square
    mixed = (0.3 * 0.125) * square
    mirrored = (0.3 * 0.125 * sign) * square
    rows = sorted({i for number in wanted for i in PAIRS[number]})
    pulled = {
        i: adjugate[i][0] * fiber[0] + adjugate[i][1] * fiber[1] + adjugate[i][2] * fiber[2]
        for i in rows
    }
    scale = {XX: diagonal, YY: diagonal, ZZ: diagonal, XY: mirrored, XZ: mirrored, YZ: mixed}
    conduct = {}
    for number in wanted:
        i, j = PAIRS[number]
        metric = (
            adjugate[i][0] * adjugate[j][0]
            + adjugate[i][1] * adjugate[j][1]
            + adjugate[i][2] * adjugate[j][2]
        )
        conduct[number] = scale[number] * (metric + pulled[i] * pulled[j])
    return conduct


def excess_of(entries, fiber):
    parts = [
        entries[3 * i] * fiber[0] + entries[3 * i + 1] * fiber[1] + entries[3 * i + 2] * fiber[2]
        for i in range(3)
    ]
    square = parts[0] * parts[0] + parts[1] * parts[1] + parts[2] * parts[2]
    return jnp.maximum(STRETCH_SCALE * (square * lax.rsqrt(square)) - 1.0, 0.0)


class Place:
    def __init__(self, across, down, sizes):
        self.across, self.down, self.sizes = across, down, sizes
        self.gx, self.gy = lax.axis_index("gx"), lax.axis_index("gy")
        self.first_x, self.last_x = self.gx == 0, self.gx == across - 1
        self.first_y, self.last_y = self.gy == 0, self.gy == down - 1
        odd = lax.rem(self.gx, 2)
        self.odd = odd
        self.leave = 2 * odd - 1
        self.leaves = jnp.logical_not(jnp.logical_or(self.first_x, self.last_x))
        self.late = jnp.where(self.leaves, self.leave, -self.leave)
        self.sign = jnp.where(self.late > 0, 1.0, -1.0)

    def slab(self, j):
        last = self.sizes[0] + 1
        return jnp.where(self.late > 0, j, last - j)


def load_rows(ref, at, start, size):
    planes = [ref[(*at, part, slice(start, start + size))] for part in range(ref.shape[-3])]
    return jnp.concatenate(planes, axis=1)


def store_rows(ref, at, start, value):
    for part in range(ref.shape[-3]):
        rows = slice(start, start + value.shape[0])
        ref[(*at, part, rows)] = value[:, part * LANES : (part + 1) * LANES]


def gather_index(place, near_slots, q, offset):
    ey = place.sizes[4]
    low = jnp.where(place.first_y, near_slots[q, 1, 0, 0:1], near_slots[q, 0, 0, ey - 1 : ey])
    high = jnp.where(place.last_y, near_slots[q, 1, 0, ey - 1 : ey], near_slots[q, 2, 0, 0:1])
    pieces = [low] + [near_slots[q, 1, 0, c : c + 1] for c in range(ey)] + [high]
    count = place.sizes[7]
    return jnp.concatenate(pieces, axis=1) - (place.gx + offset) * (place.down * count)


def page_of(index):
    return index >> (LANES.bit_length() - 1)


def keep_page(rows, page):
    kept = lax.broadcasted_iota(jnp.int32, rows.shape, 0) == page
    return jnp.sum(jnp.where(kept, rows, 0.0), axis=0, keepdims=True)


def pick_row(place, held, q, index):
    blocks = place.sizes[7] // LANES
    totals, lasts = [], []
    for t in range(index.shape[1] // LANES):
        lanes = index[:, t * LANES : (t + 1) * LANES]
        page = page_of(lanes)
        spot = jnp.broadcast_to(lanes & (LANES - 1), (8, LANES))

        def take(rows):
            return jnp.take_along_axis(rows, spot, axis=1, mode="promise_in_bounds")

        total = None
        tails = []
        for h in range(place.down):
            tails.append(held[q, h, 8 * blocks : 9 * blocks])
            for b in range(blocks):
                found = take(held[q, h, 8 * b : 8 * b + 8])
                total = found if total is None else jnp.where(page == h * blocks + b, found, total)
        totals.append(total)
        tails = jnp.concatenate(tails, axis=0)
        last = None
        for g in range(0, place.down * blocks, 8):
            part = keep_page(take(tails[g : g + 8]), page - g)
            last = part if last is None else last + part
        lasts.append(last)
    return jnp.concatenate(totals, axis=1), jnp.concatenate(lasts, axis=1)


def refine_row(place, row, weight_y, weight_z, whole):
    by, ez = place.sizes[1], place.sizes[5]
    total, last = row
    span = WINDOW * ez
    spread = []
    for k in range(9):
        values = total[k : k + 1] if k < 8 else last
        for half in range(by // 8):
            at = 2 * half * ez
            spread.append(weight_y[8 * half : 8 * half + 8] * values[:, at : at + span])
        at = (by // 4 - 2) * ez
        rim = lax.broadcasted_iota(jnp.int32, (8, span), 0) < 4
        spread.append(weight_y[by : by + 8] * jnp.where(rim, values[:, 0:span], values[:, at : at + span]))
    spread = jnp.concatenate(spread, axis=0)
    if whole:
        return dot_two(spread, weight_z)
    return jnp.dot(spread.astype(jnp.bfloat16), weight_z, preferred_element_type=jnp.float32)


def rolls(nz, by):
    lane = lax.broadcasted_iota(jnp.int32, (by, nz), 1)

    def ahead(values):
        return pltpu.roll(values, nz - 1, 1)

    def behind(values):
        return pltpu.roll(values, 1, 1)

    return lane, ahead, behind


def grad_z(values):
    nz = values.shape[1]
    lane, ahead, behind = rolls(nz, values.shape[0])
    upper = jnp.where(lane == nz - 1, values, ahead(values))
    lower = jnp.where(lane == 0, values, behind(values))
    return upper - lower


class Slopes:
    def __init__(self, place, volts, slopes, parts_x, parts_y, parts_z):
        self.place, self.volts, self.slopes = place, volts, slopes
        self.parts_x, self.parts_y, self.parts_z = parts_x, parts_y, parts_z

    def volt(self, j, shift=0):
        return load_rows(self.volts, (j,), TOP + shift, self.place.sizes[1])

    def slope_z(self, j, shift=0):
        return load_rows(self.slopes, (j,), TOP + shift, self.place.sizes[1])

    def slope_y(self, j):
        return self.volt(j, 1) - self.volt(j, -1)

    def slope_x(self, j, shift=0):
        return self.volt(j + 1, shift) - self.volt(j - 1, shift)

    def pair(self, values):
        return values + pltpu.roll(values, values.shape[1] - 1, 1)

    def along_x(self, j):
        self.parts_x[j, 0] = self.volt(j + 1) - self.volt(j)
        self.parts_x[j, 1] = self.slope_y(j) + self.slope_y(j + 1)
        self.parts_x[j, 2] = self.slope_z(j) + self.slope_z(j + 1)

    def with_x(self, j):
        for side, shift in enumerate((1, -1)):
            self.parts_y[j - 1, side, 0] = self.slope_x(j) + self.slope_x(j, shift)
        self.parts_z[j - 1, 0] = self.pair(self.slope_x(j))

    def within(self, j):
        here = self.volt(j)
        for side, shift in enumerate((1, -1)):
            self.parts_y[j - 1, side, 1] = shift * (self.volt(j, shift) - here)
            self.parts_y[j - 1, side, 2] = self.slope_z(j) + self.slope_z(j, shift)
        self.parts_z[j - 1, 1] = self.pair(self.slope_y(j))
        self.parts_z[j - 1, 2] = pltpu.roll(here, here.shape[1] - 1, 1) - here


def make_flux(place, parts_x, parts_y, parts_z, early, late, first):
    by, nz = place.sizes[1:3]
    lane, ahead, behind = rolls(nz, by)
    y_row = lax.broadcasted_iota(jnp.int32, (by, nz), 0)

    def tensor(number, j, shift=0):
        at = (number, j) if j < first else (number, j - first)
        return load_rows(early if j < first else late, at, TOP + shift, by)

    def face_x(j):
        terms = [
            (tensor(number, j) + tensor(number, j + 1)) * parts_x[j, part]
            for part, number in enumerate((XX, XY, XZ))
        ]
        return terms[0] + terms[1] + terms[2]

    def face_y(j, side, shift):
        terms = [
            (tensor(number, j) + tensor(number, j, shift)) * parts_y[j - 1, side, part]
            for part, number in enumerate((XY, YY, YZ))
        ]
        return terms[0] + terms[1] + terms[2]

    def across_yz(j):
        upper = jnp.where(jnp.logical_and(y_row == by - 1, place.last_y), 0.0, face_y(j, 0, 1))
        lower = jnp.where(jnp.logical_and(y_row == 0, place.first_y), 0.0, face_y(j, 1, -1))
        terms = []
        for part, number in enumerate((XZ, YZ, ZZ)):
            mine = tensor(number, j)
            terms.append((mine + ahead(mine)) * parts_z[j - 1, part])
        face_z = jnp.where(lane == nz - 1, 0.0, terms[0] + terms[1] + terms[2])
        return (upper - lower) + (face_z - behind(face_z))

    return face_x, across_yz


def put_tensors(place, conducts, slot, mid, side, weight, fiber_at, halo, note):
    by = place.sizes[1]
    tall = by + 8
    for half in range(by // 8):
        rows = slice(8 * half, 8 * half + 8)
        entries = []
        for k in range(9):
            at = tall * k + 8 * half
            entries.append(mid(at) + weight * side(at))
        fiber = fiber_at(rows)
        wanted = (XX, XY, XZ) if halo else tuple(range(6))
        for number, value in tensor_of(entries, fiber, place.sign, wanted).items():
            store_rows(conducts, (number, slot), TOP + 8 * half, value)
        if not halo:
            note(rows, excess_of(entries, fiber))


def put_rims(place, conducts, slabs, mid, side, rim_fiber, share):
    bx, by, nz = place.sizes[:3]
    tall = by + 8
    row = lax.rem(lax.broadcasted_iota(jnp.int32, (8, nz), 0), bx)
    weight = jnp.zeros((8, nz), jnp.float32)
    for j in slabs.values():
        weight = jnp.where(row == j - 1, share * abs((j - 0.5) / RATIO - 0.5), weight)
    entries = []
    for k in range(9):
        entries.append(mid(tall * k + by) + weight * side(tall * k + by))
    for number, value in tensor_of(entries, rim_fiber, place.sign, (YY, XY, YZ)).items():
        for slot, j in slabs.items():
            store_rows(conducts, (number, slot), TOP - 1, value[j - 1 : j])
            store_rows(conducts, (number, slot), TOP + by, value[bx + j - 1 : bx + j])


def put_volts(place, cells, volts, slopes, spot, slot):
    by = place.sizes[1]
    own = cells[0, spot, TOP : TOP + by]
    low, high = cells[0, spot, TOP - 1 : TOP], cells[0, spot, TOP + by : TOP + by + 1]
    low = jnp.where(place.first_y, own[0:1], low)
    high = jnp.where(place.last_y, own[by - 1 : by], high)
    for start, value in ((TOP, own), (TOP - 1, low), (TOP + by, high)):
        store_rows(volts, (slot,), start, value)
        store_rows(slopes, (slot,), start, grad_z(value))


def exchange(
    across,
    down,
    sizes,
    potential,
    recovery,
    angles,
    deform,
    slots,
    fibers,
    rim_fibers,
    refined,
    diffs,
    volts,
    slopes,
    parts_x,
    parts_y,
    parts_z,
    partial,
    base,
    next_recovery,
    conducts,
    cells,
    held,
    near_slots,
    rest_in,
    spread_y,
    spread_z,
    middle,
    gauge,
    slot_gauge,
    send_sem,
    slot_sem,
    near_sem,
    local_sem,
    plane_ready,
    leave_ready,
    equal_ready,
):
    bx, by, nz, ex, ey, ez, parts, count = sizes
    blocks = count // LANES
    place = Place(across, down, sizes)
    half = RATIO // 2
    gx, gy = place.gx, place.gy
    first_y, last_y, leave = place.first_y, place.last_y, place.leave
    for b in range(blocks):
        columns = pl.ds(b * LANES, LANES)
        pltpu.make_async_copy(
            deform.at[pl.ds(0, 8), columns], held.at[1, gy, pl.ds(8 * b, 8)], local_sem.at[0]
        ).start()
        pltpu.make_async_copy(
            deform.at[pl.ds(8, 1), columns], held.at[1, gy, pl.ds(8 * blocks + b, 1)], local_sem.at[0]
        ).start()
    inside = pl.ds(TOP, by)
    pltpu.make_async_copy(slots, near_slots.at[1, 1], local_sem.at[2]).start()
    pltpu.make_async_copy(potential, cells.at[0, pl.ds(1, bx), inside], local_sem.at[1]).start()
    pltpu.make_async_copy(angles, cells.at[pl.ds(1, 2), pl.ds(1, bx), inside], local_sem.at[1]).start()
    pltpu.make_async_copy(recovery, rest_in, local_sem.at[1]).start()

    sides = ((leave, place.leaves), (-leave, None))

    def when(check, act):
        if check is None:
            act()
        else:
            pl.when(check)(act)

    bits = max(down - 1, 1).bit_length()
    odd = place.odd

    def hops_of(column):
        if isinstance(column, int):
            return column.bit_count()
        hops = 0
        for _ in range(bits):
            halved = column // 2
            hops = hops + column - 2 * halved
            column = halved
        return hops

    own_hops = hops_of(gy)

    def above_of(dx, hops):
        chips = leave if dx is leave else 0
        return 4 * (chips + hops - own_hops) + chips

    columns_by_hops = sorted(range(down), key=lambda column: (column.bit_count(), column))

    def peers(act, groups):
        for group in groups:
            rows = ((leave,),) if group else ((-leave, 0),)

            def visit(rows=rows[0]):
                for column in columns_by_hops:
                    for dx in rows:
                        act(dx, column, above_of(dx, hops_of(column)))

            when(place.leaves if group else None, visit)

    relayed = down == 4

    def apart(dx, column):
        if not relayed or dx is not leave or column not in (0, down - 1):
            return True
        here = jnp.logical_and(odd == 1, gy == down - 1) if column == 0 else jnp.logical_and(odd == 0, gy == 0)
        return jnp.logical_not(here)

    relays_table = jnp.logical_and(place.leaves, jnp.logical_and(odd == 1, gy == down - 1)) if relayed else False
    sends_less = jnp.logical_and(place.leaves, jnp.logical_and(odd == 1, gy == down - 1))
    forwards = jnp.logical_and(place.leaves, jnp.logical_and(odd == 1, gy == 0))
    announces = jnp.logical_and(gx >= 3, jnp.logical_and(odd == 1, gy == 0))

    def other(dx, column):
        return column != gy if isinstance(dx, int) else True

    def guarded(test, act):
        def visit(dx, column, above):
            here = jnp.logical_and(test(above), other(dx, column))
            pl.when(here)(functools.partial(act, dx, column))

        return visit

    upper_core = odd == 1

    def meets(dx, above, column):
        even_row = odd == 0 if isinstance(dx, int) else odd == 1
        return jnp.logical_or(above < 0, jnp.logical_and(above == 0, jnp.logical_or(jnp.logical_not(even_row), column == gy)))

    def lower(act):
        def visit(dx, column, above):
            here = jnp.logical_and(meets(0, above, column), jnp.logical_and(other(dx, column), apart(dx, column)))
            pl.when(here)(functools.partial(act, dx, column))

        return visit

    def level(act):
        def visit(dx, column, above):
            there = jnp.logical_and(meets(dx, -above, column), jnp.logical_and(other(dx, column), apart(dx, column)))
            pl.when(there)(functools.partial(act, dx, column))

        return visit

    def equal(act):
        def visit(dx, column, above):
            pl.when(jnp.logical_and(above == 0, column != gy))(functools.partial(act, dx, column))

        return visit

    def beneath(act):
        def visit(dx, column, above):
            pl.when(jnp.logical_and(above < 0, apart(dx, column)))(functools.partial(act, dx, column))

        return visit

    def higher(act):
        return guarded(lambda above: above > 0, act)

    near_hops = {dy: hops_of(gy + dy) for dy in (-1, 0, 1)}
    barrier = pltpu.get_barrier_semaphore()

    def tell(sem, dx, column):
        pl.semaphore_signal(sem, inc=1, device_id=(gx + dx, column), device_id_type=MESH)

    peers(level(functools.partial(tell, barrier)), (0, 1))
    below = 0
    equals = 0
    plane_above, leave_above = [], []
    for column in range(down):
        higher_here = 0
        for dx in (-leave, 0):
            above = above_of(dx, hops_of(column))
            below = below + jnp.where(jnp.logical_and(meets(0, above, column), other(dx, column)), 1, 0)
            higher_here = higher_here + jnp.where(above > 0, 1, 0)
            equals = equals + jnp.where(jnp.logical_and(above == 0, column != gy), 1, 0)
        plane_above.append(higher_here)
        above = above_of(leave, hops_of(column))
        met = jnp.logical_and(meets(0, above, column), apart(leave, column))
        below = below + jnp.where(jnp.logical_and(place.leaves, met), 1, 0)
        leave_above.append(jnp.where(jnp.logical_and(place.leaves, above > 0), 1, 0))

    if relayed:
        below = below + jnp.where(announces, 1, 0)
        pl.when(sends_less)(lambda: tell(barrier, 2, 0))
    pl.semaphore_wait(barrier, below)
    if relayed:
        pl.when(announces)(lambda: tell(leave_ready.at[down - 1], -1, 0))
    pl.when(upper_core)(lambda: tell(equal_ready, -1, gy))
    peers(beneath(functools.partial(tell, leave_ready.at[gy])), (1,))
    peers(beneath(functools.partial(tell, plane_ready.at[gy])), (0,))

    def drain(ref, sem):
        pltpu.make_async_copy(ref, ref, sem).wait()

    rows = pl.ds(0, 9 * blocks)
    line = 4 * nz

    def drain_bytes(amount, sem):
        assert amount % line == 0
        drain(gauge.at[pl.ds(0, amount // line)], sem)

    def drain_slots(amount, sem):
        drain(slot_gauge.at[pl.ds(0, amount)], sem)

    drain(held.at[1, gy, rows], local_sem.at[0])
    drain_slots(1, local_sem.at[2])

    def put(source, target, sem, dx, where):
        pltpu.make_async_remote_copy(
            src_ref=source,
            dst_ref=target,
            send_sem=send_sem.at[0],
            recv_sem=sem,
            device_id=(gx + dx, where),
            device_id_type=MESH,
        ).start()

    def near_of(dx):
        return 0 if isinstance(dx, int) else jnp.where(dx == leave, 1, 0)

    def table_of(dx, column):
        if isinstance(dx, int):
            return jnp.where(relays_table, 3, 2) if column == 0 else 2
        return jnp.where(dx == leave, 1, 2)

    def send_deform(dx, column):
        q = 1 - dx
        put(held.at[1, gy, rows], held.at[q, gy, rows], near_sem.at[table_of(dx, column)], dx, column)

    def send_slots(dx, dy):
        put(near_slots.at[1, 1], near_slots.at[1 - dx, 1 - dy], slot_sem.at[near_of(dx)], dx, gy + dy)

    def send_cells(dx, dy):
        y_source = inside if dy == 0 else pl.ds(TOP if dy < 0 else TOP + by - 1, 1)
        y_target = inside if dy == 0 else pl.ds(TOP + by if dy < 0 else TOP - 1, 1)
        if isinstance(dx, int):
            x_source = x_target = pl.ds(1, bx)
        else:
            x_source = pl.ds(jnp.where(dx < 0, 1, bx), 1)
            x_target = pl.ds(jnp.where(dx < 0, bx + 1, 0), 1)
        corner = dy != 0 and not isinstance(dx, int)
        fields = pl.ds(0, 1 if corner else 3)
        source, target = cells.at[fields, x_source, y_source], cells.at[fields, x_target, y_target]
        put(source, target, near_sem.at[near_of(dx)], dx, gy + dy)

    def neighbours(act, group, sign, column=None):
        for dx in (leave,) if group else (-leave, 0):
            for dy in (-1, 0, 1):
                if isinstance(dx, int) and dy == 0:
                    continue
                above = above_of(dx, near_hops[dy])
                if sign > 0:
                    check = above > 0
                elif sign < 0:
                    check = meets(0, above, gy + dy)
                    if dy:
                        check = jnp.logical_and(check, above < 0)
                else:
                    check = jnp.logical_and(above == 0, dy != 0)
                if column is not None:
                    check = jnp.logical_and(check, gy + dy == column)
                if dy:
                    check = jnp.logical_and(check, jnp.logical_not(first_y if dy < 0 else last_y))
                if group:
                    check = jnp.logical_and(check, place.leaves)
                pl.when(check)(functools.partial(act, dx, dy))

    def local_work():
        width = WINDOW * ez
        row = lax.broadcasted_iota(jnp.int32, (by + 8, width), 0)
        lane = lax.broadcasted_iota(jnp.int32, (by + 8, width), 1)
        low = row < by + bx
        cell = jnp.where(row < by, row, jnp.where(low, -1, by))
        start = jnp.where(row < by, 2 * (row // 8), jnp.where(low, 0, ey - 2))
        spot = (cell.astype(jnp.float32) + 0.5) * (1.0 / RATIO) - 0.5
        coarse = (lane // ez + start - 1).astype(jnp.float32)
        spread_y[...] = jnp.maximum(1.0 - jnp.abs(spot - coarse), 0.0)
        row = lax.broadcasted_iota(jnp.int32, (width, nz), 0)
        lane = lax.broadcasted_iota(jnp.int32, (width, nz), 1)
        spot = jnp.clip((lane.astype(jnp.float32) + 0.5) * (1.0 / RATIO) - 0.5, 0.0, ez - 1.0)
        weight = jnp.maximum(1.0 - jnp.abs(spot - lax.rem(row, ez).astype(jnp.float32)), 0.0)
        spread_z[...] = weight.astype(jnp.bfloat16)
        for s in range(bx):
            own = [cells[number, s + 1, TOP : TOP + by] for number in (1, 2)]
            for number, part in enumerate(fiber_of(*own)):
                fibers[number, s] = part
            voltage = cells[0, s + 1, TOP : TOP + by]
            resting = rest_in[s]
            next_recovery[s] = resting + 0.05 * (-resting - 8.0 * voltage * (voltage - 1.15))
            current = 8.0 * voltage * (voltage - 0.15) * (voltage - 1.0) + voltage * resting
            base[s] = voltage - 0.1 * current

    def send_near(dx, dy):
        send_slots(dx, dy)
        send_cells(dx, dy)

    def wait_cells():
        drain_bytes(4 * bx * by * line, local_sem.at[1])

    meets_equals = jnp.logical_and(upper_core, equals > 0)

    def split_equals(strict):
        def visit(dx, column, above):
            test = above < 0 if strict else above == 0
            lower(lambda *peer: pl.when(test)(functools.partial(send_deform, *peer)))(dx, column, above)

        return visit

    @pl.when(meets_equals)
    def _():
        wait_cells()
        for group in (0, 1):
            neighbours(send_near, group, -1)

    pl.when(meets_equals)(lambda: neighbours(send_near, 0, 0))
    peers(split_equals(False), (0,))
    peers(split_equals(True), (1, 0))

    @pl.when(jnp.logical_not(meets_equals))
    def _():
        for group in (0, 1):
            neighbours(send_slots, group, -1)
        wait_cells()
        for group in (1, 0):
            neighbours(send_cells, group, -1)

    local_work()

    @pl.when(jnp.logical_not(upper_core))
    def _():
        pl.semaphore_wait(equal_ready, 1)

        @pl.when(equals > 0)
        def _():
            neighbours(send_near, 0, 0)
            peers(equal(send_deform), (0,))

    for group, ready, counts in ((0, plane_ready, plane_above), (1, leave_ready, leave_above)):
        for column in columns_by_hops:

            @pl.when(counts[column] > 0)
            def _(group=group, ready=ready, counts=counts, column=column):
                pl.semaphore_wait(ready.at[column], counts[column])
                for dx in (leave,) if group else (-leave, 0):
                    higher(send_deform)(dx, column, above_of(dx, hops_of(column)))
                neighbours(send_near, group, 1, column)

    middle_y = jnp.logical_not(jnp.logical_or(first_y, last_y))
    some_y = jnp.logical_xor(first_y, last_y)
    no_y = jnp.logical_and(first_y, last_y)

    def over_y(act):
        pl.when(middle_y)(functools.partial(act, 2))
        pl.when(some_y)(functools.partial(act, 1))
        pl.when(no_y)(functools.partial(act, 0))

    table = 4 * parts * count

    def wait_leave_near(slot, near, tables=down):
        over_y(lambda n: drain_slots(n + 1, slot))
        over_y(lambda n: drain_bytes(tables * table + (3 * by + n) * line, near))

    def wait_plane_slots(sem):
        over_y(lambda n: drain_slots(2 * n + 1, sem))

    def wait_plane(sem):
        over_y(lambda n: drain_bytes((3 * by + n * (3 * bx + 1)) * line, sem))

    if relayed:

        @pl.when(forwards)
        def _():
            drain_bytes(table, near_sem.at[3])
            source = held.at[1, down - 1, rows]
            put(source, held.at[0, down - 1, rows], near_sem.at[1], leave, 0)

    wait_plane(near_sem.at[0])
    for j in range(bx + 1):
        spot = place.slab(j) if j else jnp.where(place.leaves, place.slab(0), place.slab(1))
        put_volts(place, cells, volts, slopes, spot, j)
    slope = Slopes(place, volts, slopes, parts_x, parts_y, parts_z)

    def rim_of(number):
        pieces = [cells[number, place.slab(j), row : row + 1] for row in (TOP - 1, TOP + by) for j in range(1, bx + 1)]
        return jnp.concatenate(pieces, axis=0)

    rim_fiber = fiber_of(rim_of(1), rim_of(2))
    for number, value in enumerate(rim_fiber):
        rim_fibers[number] = value

    for j in range(bx):
        slope.along_x(j)
        slope.within(j + 1)
    for j in range(1, bx):
        slope.with_x(j)

    wait_plane_slots(slot_sem.at[0])
    if relayed:
        pl.when(jnp.logical_not(forwards))(lambda: drain_bytes((2 * down - 1) * table, near_sem.at[2]))
        pl.when(forwards)(lambda: drain_bytes((2 * down - 2) * table, near_sem.at[2]))
    else:
        drain_bytes((2 * down - 1) * table, near_sem.at[2])
    index_middle = gather_index(place, near_slots, 1, 0)
    index_side = gather_index(place, near_slots, 1 - leave, -leave)
    weight_y, weight_z = spread_y[...], spread_z[...]
    middle_row = pick_row(place, held, 1, index_middle)
    refined[...] = refine_row(place, middle_row, weight_y, weight_z, True)
    middle[0:8] = middle_row[0]
    middle[8:9] = middle_row[1]
    side_row = pick_row(place, held, 1 - leave, index_side)
    side_row = [a - b for a, b in zip(side_row, middle_row)]
    diffs[0] = refine_row(place, side_row, weight_y, weight_z, False)

    def mid(at):
        return refined[at : at + 8]

    def side(at):
        return diffs[0, at : at + 8]

    share = jnp.where(place.leaves, 1.0, 0.0)
    def early_slab(j):
        spot = place.slab(j)

        def fiber_at(rows):
            if j:
                return [fibers[number, spot - 1, rows] for number in range(3)]
            start = TOP + rows.start
            return fiber_of(*(cells[number, spot, start : start + 8] for number in (1, 2)))

        def note(rows, excess):
            voltage = load_rows(volts, (j,), TOP + rows.start, 8)
            partial[j - 1, rows] = base[spot - 1, rows] - excess * (voltage - 0.6)

        weight = share * abs((j - 0.5) / RATIO - 0.5)
        put_tensors(place, conducts, j, mid, side, weight, fiber_at, j == 0, note)

    for j in range(1, half + 1):
        early_slab(j)
    put_rims(place, conducts, {j: j for j in range(1, half + 1)}, mid, side, rim_fiber, share)
    out = send_sem.at[0]
    wait_plane_slots(out)
    wait_plane(out)
    drain_bytes((2 * down - 1) * table, out)

    @pl.when(place.leaves)
    def _():
        wait_leave_near(out, out, down - 1)
        if relayed:
            pl.when(jnp.logical_not(sends_less))(lambda: drain_bytes(table, out))
            pl.when(forwards)(lambda: drain_bytes(table, out))
        else:
            drain_bytes(table, out)

    @pl.when(place.leaves)
    def _():
        wait_leave_near(slot_sem.at[1], near_sem.at[1])
        index = gather_index(place, near_slots, 1 + leave, leave)
        row = pick_row(place, held, 1 + leave, index)
        row = [a - b for a, b in zip(row, (middle[0:8], middle[8:9]))]
        diffs[1] = refine_row(place, row, spread_y[...], spread_z[...], False)
        early_slab(0)


def compute(
    across,
    down,
    sizes,
    fibers,
    rim_fibers,
    refined,
    diffs,
    volts,
    slopes,
    parts_x,
    parts_y,
    parts_z,
    partial,
    base,
    recovered,
    early_conducts,
    cells,
    next_potential,
    next_recovery,
    conducts,
    result,
    out_sem,
):
    bx, by, nz = sizes[:3]
    place = Place(across, down, sizes)
    half = RATIO // 2

    pltpu.make_async_copy(recovered, next_recovery, out_sem.at[0]).start()

    which = jnp.where(place.leaves, 1, 0)
    put_volts(place, cells, volts, slopes, place.slab(bx + 1), bx + 1)
    slope = Slopes(place, volts, slopes, parts_x, parts_y, parts_z)
    slope.along_x(bx)
    slope.with_x(bx)

    def finish(j):
        target = next_potential.at[place.slab(j) - 1]
        pltpu.make_async_copy(result.at[j - 1], target, out_sem.at[0]).start()

    def mid(at):
        return refined[at : at + 8]

    def side(at):
        return diffs[which, at : at + 8]

    for j in range(half + 1, bx + 2):
        spot = place.slab(j)

        def fiber_at(rows, j=j, spot=spot):
            if j <= bx:
                return [fibers[number, spot - 1, rows] for number in range(3)]
            start = TOP + rows.start
            return fiber_of(*(cells[number, spot, start : start + 8] for number in (1, 2)))

        def note(rows, excess, j=j, spot=spot):
            voltage = load_rows(volts, (j,), TOP + rows.start, 8)
            result[j - 1, rows] = base[spot - 1, rows] - excess * (voltage - 0.6)

        weight = abs((j - 0.5) / RATIO - 0.5)
        put_tensors(place, conducts, j - half - 1, mid, side, weight, fiber_at, j == bx + 1, note)
    rim_fiber = [rim_fibers[number] for number in range(3)]
    put_rims(place, conducts, {j - half - 1: j for j in range(half + 1, bx + 1)}, mid, side, rim_fiber, 1.0)
    face_x, across_yz = make_flux(place, parts_x, parts_y, parts_z, early_conducts, conducts, half + 1)
    faces = [face_x(j) for j in range(bx + 1)]
    faces[0] = jnp.where(place.leaves, faces[0], 0.0)
    for j in range(1, bx + 1):
        local = partial[j - 1] if j <= half else result[j - 1]
        result[j - 1] = local + 0.1 * (across_yz(j) + (faces[j] - faces[j - 1]))
        finish(j)
    both = fibers.at[pl.ds(0, 2)]
    pltpu.make_async_copy(both, both, out_sem.at[0]).wait()


def solution(mesh):
    across, down = mesh.shape["gx"], mesh.shape["gy"]

    def local(potential, recovery, angles, deform, slots):
        bx, by, nz = potential.shape
        ex, ey, ez = slots.shape
        parts, count = deform.shape
        assert ex == 1 and bx == RATIO and by == RATIO * ey and by % 8 == 0
        assert count % LANES == 0 and parts == 9 and across % 2 == 0 and (2 * ez) % LANES == 0
        sizes = (bx, by, nz, ex, ey, ez, parts, count)
        blocks = count // LANES
        f32 = jnp.float32
        half = RATIO // 2
        shape = jax.ShapeDtypeStruct(potential.shape, f32)
        anywhere = pl.BlockSpec(memory_space=pl.ANY)
        in_vmem = pl.BlockSpec(memory_space=pltpu.VMEM)
        planes = nz // LANES
        fine = 9 * (by + 8)
        planes = nz // LANES
        fine = 9 * (by + 8)
        rows = pltpu.VMEM((bx + 2, planes, by + 16, LANES), f32)
        passed = (
            pltpu.VMEM((3, bx, by, nz), f32),
            pltpu.VMEM((3, 2 * bx, nz), f32),
            pltpu.VMEM((fine, nz), f32),
            pltpu.VMEM((2, fine, nz), f32),
            rows,
            rows,
            pltpu.VMEM((bx + 1, 3, by, nz), f32),
            pltpu.VMEM((bx, 2, 3, by, nz), f32),
            pltpu.VMEM((bx, 3, by, nz), f32),
            pltpu.VMEM((half, by, nz), f32),
            pltpu.VMEM((bx, by, nz), f32),
            pltpu.VMEM((bx, by, nz), f32),
            pltpu.VMEM((6, half + 1, planes, by + 16, LANES), f32),
            pltpu.VMEM((3, bx + 2, by + 16, nz), f32),
        )
        arrived = pl.pallas_call(
            functools.partial(exchange, across, down, sizes),
            out_shape=passed,
            in_specs=[pl.BlockSpec(memory_space=pltpu.MemorySpace.HBM)] * 5,
            out_specs=(in_vmem,) * len(passed),
            scratch_shapes=[
                pltpu.VMEM((3, down, 8 * blocks + 8, LANES), f32),
                pltpu.VMEM((3, 3, ex, ey, ez), jnp.int32),
                pltpu.VMEM(recovery.shape, f32),
                pltpu.VMEM((by + 8, WINDOW * ez), f32),
                pltpu.VMEM((WINDOW * ez, nz), jnp.bfloat16),
                pltpu.VMEM((16, (ey + 2) * ez), f32),
                pltpu.VMEM((4 * bx * by + 2 * down * parts * count // nz, 1, nz), f32),
                pltpu.VMEM((5, ex, ey, ez), jnp.int32),
                pltpu.SemaphoreType.DMA((1,)),
                pltpu.SemaphoreType.DMA((2,)),
                pltpu.SemaphoreType.DMA((4,)),
                pltpu.SemaphoreType.DMA((3,)),
                pltpu.SemaphoreType.REGULAR((down,)),
                pltpu.SemaphoreType.REGULAR((down,)),
                pltpu.SemaphoreType.REGULAR,
            ],
            compiler_params=pltpu.CompilerParams(
                collective_id=0, has_side_effects=True, vmem_limit_bytes=VMEM_LIMIT
            ),
        )(*(pltpu.with_memory_space_constraint(x, pltpu.MemorySpace.HBM) for x in (potential, recovery, angles, deform, slots)))
        return pl.pallas_call(
            functools.partial(compute, across, down, sizes),
            out_shape=(shape, shape),
            in_specs=[in_vmem] * len(passed),
            out_specs=(anywhere,) * 2,
            scratch_shapes=[
                pltpu.VMEM((6, half + 1, planes, by + 16, LANES), f32),
                pltpu.VMEM((bx, by, nz), f32),
                pltpu.SemaphoreType.DMA((1,)),
            ],
            compiler_params=pltpu.CompilerParams(vmem_limit_bytes=VMEM_LIMIT),
        )(*arrived)

    return jax.shard_map(
        local,
        mesh=mesh,
        in_specs=(
            P("gx", "gy", None),
            P("gx", "gy", None),
            P(None, "gx", "gy", None),
            P(None, ("gx", "gy")),
            P("gx", "gy", None),
        ),
        out_specs=(P("gx", "gy", None), P("gx", "gy", None)),
        check_vma=False,
    )
```

```python
import functools

import jax
import jax.numpy as jnp
from jax import lax
from jax.experimental import pallas as pl
from jax.experimental.pallas import tpu as pltpu
from jax.sharding import PartitionSpec as P

MESH = pl.DeviceIdType.MESH
RATIO = 4
LANES = 128
VMEM_LIMIT = 16 * 1024 * 1024
TOP = 8
WINDOW = 4
FIBER_SCALE = (7.0 / 3.0) ** 0.5
STRETCH_SCALE = (3.0 / 7.0) ** 0.5
XX, YY, ZZ, XY, XZ, YZ = range(6)
PAIRS = ((0, 0), (1, 1), (2, 2), (0, 1), (0, 2), (1, 2))


def split_two(values):
    high = values.astype(jnp.bfloat16)
    low = (values - high.astype(jnp.float32)).astype(jnp.bfloat16)
    return high, low


def dot_two(values, weights):
    high, low = split_two(values)
    return jnp.dot(high, weights, preferred_element_type=jnp.float32) + jnp.dot(
        low, weights, preferred_element_type=jnp.float32
    )


def polynomial(terms, value):
    total = terms[-1]
    for term in terms[-2::-1]:
        total = total * value + term
    return total


HALF_SINE = (0.707106764632592, -0.02946274890445726, 3.682656229209654e-4, -2.187710743548062e-6, 7.155278665108425e-9)
HALF_COSINE = (1.414213496564441, -0.17677636064176425, 3.6825754039592376e-3, -3.0612650004537585e-5, 1.2790856262670407e-7)


def sine_cosine(angle):
    square = angle * angle
    sine = angle * polynomial(HALF_SINE, square)
    cosine = polynomial(HALF_COSINE, square)
    return sine * cosine, 1.0 - sine * sine


def fiber_of(azimuth, elevation):
    sin_u, cos_u = sine_cosine(azimuth)
    sin_e, cos_e = sine_cosine(elevation)
    flat = FIBER_SCALE * cos_e
    return cos_u * flat, sin_u * flat, FIBER_SCALE * sin_e


def tensor_of(entries, fiber, sign, wanted):
    def element(i, j):
        return entries[3 * (i % 3) + j % 3]

    adjugate = [
        [
            element(j + 1, i + 1) * element(j + 2, i + 2)
            - element(j + 1, i + 2) * element(j + 2, i + 1)
            for j in range(3)
        ]
        for i in range(3)
    ]
    determinant = (
        element(0, 0) * adjugate[0][0]
        + element(0, 1) * adjugate[1][0]
        + element(0, 2) * adjugate[2][0]
    )
    inverse = 1.0 / determinant
    square = inverse * inverse
    diagonal = (0.3 * 0.5) * square
    mixed = (0.3 * 0.125) * square
    mirrored = (0.3 * 0.125 * sign) * square
    rows = sorted({i for number in wanted for i in PAIRS[number]})
    pulled = {
        i: adjugate[i][0] * fiber[0] + adjugate[i][1] * fiber[1] + adjugate[i][2] * fiber[2]
        for i in rows
    }
    scale = {XX: diagonal, YY: diagonal, ZZ: diagonal, XY: mirrored, XZ: mirrored, YZ: mixed}
    conduct = {}
    for number in wanted:
        i, j = PAIRS[number]
        metric = (
            adjugate[i][0] * adjugate[j][0]
            + adjugate[i][1] * adjugate[j][1]
            + adjugate[i][2] * adjugate[j][2]
        )
        conduct[number] = scale[number] * (metric + pulled[i] * pulled[j])
    return conduct


def excess_of(entries, fiber):
    parts = [
        entries[3 * i] * fiber[0] + entries[3 * i + 1] * fiber[1] + entries[3 * i + 2] * fiber[2]
        for i in range(3)
    ]
    square = parts[0] * parts[0] + parts[1] * parts[1] + parts[2] * parts[2]
    return jnp.maximum(STRETCH_SCALE * (square * lax.rsqrt(square)) - 1.0, 0.0)


class Place:
    def __init__(self, across, down, sizes):
        self.across, self.down, self.sizes = across, down, sizes
        self.gx, self.gy = lax.axis_index("gx"), lax.axis_index("gy")
        self.first_x, self.last_x = self.gx == 0, self.gx == across - 1
        self.first_y, self.last_y = self.gy == 0, self.gy == down - 1
        odd = lax.rem(self.gx, 2)
        self.odd = odd
        self.leave = 2 * odd - 1
        self.leaves = jnp.logical_not(jnp.logical_or(self.first_x, self.last_x))
        self.late = jnp.where(self.leaves, self.leave, -self.leave)
        self.sign = jnp.where(self.late > 0, 1.0, -1.0)

    def slab(self, j):
        last = self.sizes[0] + 1
        return jnp.where(self.late > 0, j, last - j)


def load_rows(ref, at, start, size):
    planes = [ref[(*at, part, slice(start, start + size))] for part in range(ref.shape[-3])]
    return jnp.concatenate(planes, axis=1)


def store_rows(ref, at, start, value):
    for part in range(ref.shape[-3]):
        rows = slice(start, start + value.shape[0])
        ref[(*at, part, rows)] = value[:, part * LANES : (part + 1) * LANES]


def gather_index(place, near_slots, q, offset):
    ey = place.sizes[4]
    low = jnp.where(place.first_y, near_slots[q, 1, 0, 0:1], near_slots[q, 0, 0, ey - 1 : ey])
    high = jnp.where(place.last_y, near_slots[q, 1, 0, ey - 1 : ey], near_slots[q, 2, 0, 0:1])
    pieces = [low] + [near_slots[q, 1, 0, c : c + 1] for c in range(ey)] + [high]
    count = place.sizes[7]
    return jnp.concatenate(pieces, axis=1) - (place.gx + offset) * (place.down * count)


def page_of(index):
    return index >> (LANES.bit_length() - 1)


def keep_page(rows, page):
    kept = lax.broadcasted_iota(jnp.int32, rows.shape, 0) == page
    return jnp.sum(jnp.where(kept, rows, 0.0), axis=0, keepdims=True)


def pick_row(place, held, q, index):
    blocks = place.sizes[7] // LANES
    totals, lasts = [], []
    for t in range(index.shape[1] // LANES):
        lanes = index[:, t * LANES : (t + 1) * LANES]
        page = page_of(lanes)
        spot = jnp.broadcast_to(lanes & (LANES - 1), (8, LANES))

        def take(rows):
            return jnp.take_along_axis(rows, spot, axis=1, mode="promise_in_bounds")

        total = None
        tails = []
        for h in range(place.down):
            tails.append(held[q, h, 8 * blocks : 9 * blocks])
            for b in range(blocks):
                found = take(held[q, h, 8 * b : 8 * b + 8])
                total = found if total is None else jnp.where(page == h * blocks + b, found, total)
        totals.append(total)
        tails = jnp.concatenate(tails, axis=0)
        last = None
        for g in range(0, place.down * blocks, 8):
            part = keep_page(take(tails[g : g + 8]), page - g)
            last = part if last is None else last + part
        lasts.append(last)
    return jnp.concatenate(totals, axis=1), jnp.concatenate(lasts, axis=1)


def refine_row(place, row, weight_y, weight_z, whole):
    by, ez = place.sizes[1], place.sizes[5]
    total, last = row
    span = WINDOW * ez
    spread = []
    for k in range(9):
        values = total[k : k + 1] if k < 8 else last
        for half in range(by // 8):
            at = 2 * half * ez
            spread.append(weight_y[8 * half : 8 * half + 8] * values[:, at : at + span])
        at = (by // 4 - 2) * ez
        rim = lax.broadcasted_iota(jnp.int32, (8, span), 0) < 4
        spread.append(weight_y[by : by + 8] * jnp.where(rim, values[:, 0:span], values[:, at : at + span]))
    spread = jnp.concatenate(spread, axis=0)
    if whole:
        return dot_two(spread, weight_z)
    return jnp.dot(spread.astype(jnp.bfloat16), weight_z, preferred_element_type=jnp.float32)


def rolls(nz, by):
    lane = lax.broadcasted_iota(jnp.int32, (by, nz), 1)

    def ahead(values):
        return pltpu.roll(values, nz - 1, 1)

    def behind(values):
        return pltpu.roll(values, 1, 1)

    return lane, ahead, behind


def grad_z(values):
    nz = values.shape[1]
    lane, ahead, behind = rolls(nz, values.shape[0])
    upper = jnp.where(lane == nz - 1, values, ahead(values))
    lower = jnp.where(lane == 0, values, behind(values))
    return upper - lower


class Slopes:
    def __init__(self, place, volts, slopes, parts_x, parts_y, parts_z):
        self.place, self.volts, self.slopes = place, volts, slopes
        self.parts_x, self.parts_y, self.parts_z = parts_x, parts_y, parts_z

    def volt(self, j, shift=0):
        return load_rows(self.volts, (j,), TOP + shift, self.place.sizes[1])

    def slope_z(self, j, shift=0):
        return load_rows(self.slopes, (j,), TOP + shift, self.place.sizes[1])

    def slope_y(self, j):
        return self.volt(j, 1) - self.volt(j, -1)

    def slope_x(self, j, shift=0):
        return self.volt(j + 1, shift) - self.volt(j - 1, shift)

    def pair(self, values):
        return values + pltpu.roll(values, values.shape[1] - 1, 1)

    def along_x(self, j):
        self.parts_x[j, 0] = self.volt(j + 1) - self.volt(j)
        self.parts_x[j, 1] = self.slope_y(j) + self.slope_y(j + 1)
        self.parts_x[j, 2] = self.slope_z(j) + self.slope_z(j + 1)

    def with_x(self, j):
        for side, shift in enumerate((1, -1)):
            self.parts_y[j - 1, side, 0] = self.slope_x(j) + self.slope_x(j, shift)
        self.parts_z[j - 1, 0] = self.pair(self.slope_x(j))

    def within(self, j):
        here = self.volt(j)
        for side, shift in enumerate((1, -1)):
            self.parts_y[j - 1, side, 1] = shift * (self.volt(j, shift) - here)
            self.parts_y[j - 1, side, 2] = self.slope_z(j) + self.slope_z(j, shift)
        self.parts_z[j - 1, 1] = self.pair(self.slope_y(j))
        self.parts_z[j - 1, 2] = pltpu.roll(here, here.shape[1] - 1, 1) - here


def make_flux(place, parts_x, parts_y, parts_z, early, late, first):
    by, nz = place.sizes[1:3]
    lane, ahead, behind = rolls(nz, by)
    y_row = lax.broadcasted_iota(jnp.int32, (by, nz), 0)

    def tensor(number, j, shift=0):
        at = (number, j) if j < first else (number, j - first)
        return load_rows(early if j < first else late, at, TOP + shift, by)

    def face_x(j):
        terms = [
            (tensor(number, j) + tensor(number, j + 1)) * parts_x[j, part]
            for part, number in enumerate((XX, XY, XZ))
        ]
        return terms[0] + terms[1] + terms[2]

    def face_y(j, side, shift):
        terms = [
            (tensor(number, j) + tensor(number, j, shift)) * parts_y[j - 1, side, part]
            for part, number in enumerate((XY, YY, YZ))
        ]
        return terms[0] + terms[1] + terms[2]

    def across_yz(j):
        upper = jnp.where(jnp.logical_and(y_row == by - 1, place.last_y), 0.0, face_y(j, 0, 1))
        lower = jnp.where(jnp.logical_and(y_row == 0, place.first_y), 0.0, face_y(j, 1, -1))
        terms = []
        for part, number in enumerate((XZ, YZ, ZZ)):
            mine = tensor(number, j)
            terms.append((mine + ahead(mine)) * parts_z[j - 1, part])
        face_z = jnp.where(lane == nz - 1, 0.0, terms[0] + terms[1] + terms[2])
        return (upper - lower) + (face_z - behind(face_z))

    return face_x, across_yz


def put_tensors(place, conducts, slot, mid, side, weight, fiber_at, halo, note):
    by = place.sizes[1]
    tall = by + 8
    for half in range(by // 8):
        rows = slice(8 * half, 8 * half + 8)
        entries = []
        for k in range(9):
            at = tall * k + 8 * half
            entries.append(mid(at) + weight * side(at))
        fiber = fiber_at(rows)
        wanted = (XX, XY, XZ) if halo else tuple(range(6))
        for number, value in tensor_of(entries, fiber, place.sign, wanted).items():
            store_rows(conducts, (number, slot), TOP + 8 * half, value)
        if not halo:
            note(rows, excess_of(entries, fiber))


def put_rims(place, conducts, slabs, mid, side, rim_fiber, share):
    bx, by, nz = place.sizes[:3]
    tall = by + 8
    row = lax.rem(lax.broadcasted_iota(jnp.int32, (8, nz), 0), bx)
    weight = jnp.zeros((8, nz), jnp.float32)
    for j in slabs.values():
        weight = jnp.where(row == j - 1, share * abs((j - 0.5) / RATIO - 0.5), weight)
    entries = []
    for k in range(9):
        entries.append(mid(tall * k + by) + weight * side(tall * k + by))
    for number, value in tensor_of(entries, rim_fiber, place.sign, (YY, XY, YZ)).items():
        for slot, j in slabs.items():
            store_rows(conducts, (number, slot), TOP - 1, value[j - 1 : j])
            store_rows(conducts, (number, slot), TOP + by, value[bx + j - 1 : bx + j])


def put_volts(place, cells, volts, slopes, spot, slot):
    by = place.sizes[1]
    own = cells[0, spot, TOP : TOP + by]
    low, high = cells[0, spot, TOP - 1 : TOP], cells[0, spot, TOP + by : TOP + by + 1]
    low = jnp.where(place.first_y, own[0:1], low)
    high = jnp.where(place.last_y, own[by - 1 : by], high)
    for start, value in ((TOP, own), (TOP - 1, low), (TOP + by, high)):
        store_rows(volts, (slot,), start, value)
        store_rows(slopes, (slot,), start, grad_z(value))


def exchange(
    across,
    down,
    sizes,
    potential,
    recovery,
    angles,
    deform,
    slots,
    fibers,
    rim_fibers,
    refined,
    diffs,
    volts,
    slopes,
    parts_x,
    parts_y,
    parts_z,
    partial,
    base,
    next_recovery,
    conducts,
    cells,
    held,
    near_slots,
    rest_in,
    spread_y,
    spread_z,
    middle,
    gauge,
    slot_gauge,
    send_sem,
    slot_sem,
    near_sem,
    local_sem,
    plane_ready,
    leave_ready,
    equal_ready,
):
    bx, by, nz, ex, ey, ez, parts, count = sizes
    blocks = count // LANES
    place = Place(across, down, sizes)
    half = RATIO // 2
    gx, gy = place.gx, place.gy
    first_y, last_y, leave = place.first_y, place.last_y, place.leave
    for b in range(blocks):
        columns = pl.ds(b * LANES, LANES)
        pltpu.make_async_copy(
            deform.at[pl.ds(0, 8), columns], held.at[1, gy, pl.ds(8 * b, 8)], local_sem.at[0]
        ).start()
        pltpu.make_async_copy(
            deform.at[pl.ds(8, 1), columns], held.at[1, gy, pl.ds(8 * blocks + b, 1)], local_sem.at[0]
        ).start()
    inside = pl.ds(TOP, by)
    pltpu.make_async_copy(slots, near_slots.at[1, 1], local_sem.at[2]).start()
    pltpu.make_async_copy(potential, cells.at[0, pl.ds(1, bx), inside], local_sem.at[1]).start()
    pltpu.make_async_copy(angles, cells.at[pl.ds(1, 2), pl.ds(1, bx), inside], local_sem.at[1]).start()
    pltpu.make_async_copy(recovery, rest_in, local_sem.at[1]).start()

    sides = ((leave, place.leaves), (-leave, None))

    def when(check, act):
        if check is None:
            act()
        else:
            pl.when(check)(act)

    bits = max(down - 1, 1).bit_length()
    odd = place.odd

    def hops_of(column):
        if isinstance(column, int):
            return column.bit_count()
        hops = 0
        for _ in range(bits):
            halved = column // 2
            hops = hops + column - 2 * halved
            column = halved
        return hops

    own_hops = hops_of(gy)

    def above_of(dx, hops):
        chips = leave if dx is leave else 0
        return 4 * (chips + hops - own_hops) + chips

    columns_by_hops = sorted(range(down), key=lambda column: (column.bit_count(), column))

    def peers(act, groups):
        for group in groups:
            rows = ((leave,),) if group else ((-leave, 0),)

            def visit(rows=rows[0]):
                for column in columns_by_hops:
                    for dx in rows:
                        act(dx, column, above_of(dx, hops_of(column)))

            when(place.leaves if group else None, visit)

    relayed = down == 4

    def apart(dx, column):
        if not relayed or dx is not leave or column not in (0, down - 1):
            return True
        here = jnp.logical_and(odd == 1, gy == down - 1) if column == 0 else jnp.logical_and(odd == 0, gy == 0)
        return jnp.logical_not(here)

    relays_table = jnp.logical_and(place.leaves, jnp.logical_and(odd == 1, gy == down - 1)) if relayed else False
    sends_less = jnp.logical_and(place.leaves, jnp.logical_and(odd == 1, gy == down - 1))
    forwards = jnp.logical_and(place.leaves, jnp.logical_and(odd == 1, gy == 0))
    announces = jnp.logical_and(gx >= 3, jnp.logical_and(odd == 1, gy == 0))

    def other(dx, column):
        return column != gy if isinstance(dx, int) else True

    def guarded(test, act):
        def visit(dx, column, above):
            here = jnp.logical_and(test(above), other(dx, column))
            pl.when(here)(functools.partial(act, dx, column))

        return visit

    upper_core = odd == 1

    def meets(dx, above, column):
        even_row = odd == 0 if isinstance(dx, int) else odd == 1
        return jnp.logical_or(above < 0, jnp.logical_and(above == 0, jnp.logical_or(jnp.logical_not(even_row), column == gy)))

    def lower(act):
        def visit(dx, column, above):
            here = jnp.logical_and(meets(0, above, column), jnp.logical_and(other(dx, column), apart(dx, column)))
            pl.when(here)(functools.partial(act, dx, column))

        return visit

    def level(act):
        def visit(dx, column, above):
            there = jnp.logical_and(meets(dx, -above, column), jnp.logical_and(other(dx, column), apart(dx, column)))
            pl.when(there)(functools.partial(act, dx, column))

        return visit

    def equal(act):
        def visit(dx, column, above):
            pl.when(jnp.logical_and(above == 0, column != gy))(functools.partial(act, dx, column))

        return visit

    def beneath(act):
        def visit(dx, column, above):
            pl.when(jnp.logical_and(above < 0, apart(dx, column)))(functools.partial(act, dx, column))

        return visit

    def higher(act):
        return guarded(lambda above: above > 0, act)

    near_hops = {dy: hops_of(gy + dy) for dy in (-1, 0, 1)}
    barrier = pltpu.get_barrier_semaphore()

    def tell(sem, dx, column):
        pl.semaphore_signal(sem, inc=1, device_id=(gx + dx, column), device_id_type=MESH)

    peers(level(functools.partial(tell, barrier)), (0, 1))
    below = 0
    equals = 0
    plane_above, leave_above = [], []
    for column in range(down):
        higher_here = 0
        for dx in (-leave, 0):
            above = above_of(dx, hops_of(column))
            below = below + jnp.where(jnp.logical_and(meets(0, above, column), other(dx, column)), 1, 0)
            higher_here = higher_here + jnp.where(above > 0, 1, 0)
            equals = equals + jnp.where(jnp.logical_and(above == 0, column != gy), 1, 0)
        plane_above.append(higher_here)
        above = above_of(leave, hops_of(column))
        met = jnp.logical_and(meets(0, above, column), apart(leave, column))
        below = below + jnp.where(jnp.logical_and(place.leaves, met), 1, 0)
        leave_above.append(jnp.where(jnp.logical_and(place.leaves, above > 0), 1, 0))

    if relayed:
        below = below + jnp.where(announces, 1, 0)
        pl.when(sends_less)(lambda: tell(barrier, 2, 0))
    pl.semaphore_wait(barrier, below)
    if relayed:
        pl.when(announces)(lambda: tell(leave_ready.at[down - 1], -1, 0))
    pl.when(upper_core)(lambda: tell(equal_ready, -1, gy))
    peers(beneath(functools.partial(tell, leave_ready.at[gy])), (1,))
    peers(beneath(functools.partial(tell, plane_ready.at[gy])), (0,))

    def drain(ref, sem):
        pltpu.make_async_copy(ref, ref, sem).wait()

    rows = pl.ds(0, 9 * blocks)
    line = 4 * nz

    def drain_bytes(amount, sem):
        assert amount % line == 0
        drain(gauge.at[pl.ds(0, amount // line)], sem)

    def drain_slots(amount, sem):
        drain(slot_gauge.at[pl.ds(0, amount)], sem)

    drain(held.at[1, gy, rows], local_sem.at[0])
    drain_slots(1, local_sem.at[2])

    def put(source, target, sem, dx, where):
        pltpu.make_async_remote_copy(
            src_ref=source,
            dst_ref=target,
            send_sem=send_sem.at[0],
            recv_sem=sem,
            device_id=(gx + dx, where),
            device_id_type=MESH,
        ).start()

    def near_of(dx):
        return 0 if isinstance(dx, int) else jnp.where(dx == leave, 1, 0)

    def table_of(dx, column):
        if isinstance(dx, int):
            return jnp.where(relays_table, 3, 2) if column == 0 else 2
        return jnp.where(dx == leave, 1, 2)

    def send_deform(dx, column):
        q = 1 - dx
        put(held.at[1, gy, rows], held.at[q, gy, rows], near_sem.at[table_of(dx, column)], dx, column)

    def send_slots(dx, dy):
        put(near_slots.at[1, 1], near_slots.at[1 - dx, 1 - dy], slot_sem.at[near_of(dx)], dx, gy + dy)

    def send_cells(dx, dy):
        y_source = inside if dy == 0 else pl.ds(TOP if dy < 0 else TOP + by - 1, 1)
        y_target = inside if dy == 0 else pl.ds(TOP + by if dy < 0 else TOP - 1, 1)
        if isinstance(dx, int):
            x_source = x_target = pl.ds(1, bx)
        else:
            x_source = pl.ds(jnp.where(dx < 0, 1, bx), 1)
            x_target = pl.ds(jnp.where(dx < 0, bx + 1, 0), 1)
        corner = dy != 0 and not isinstance(dx, int)
        fields = pl.ds(0, 1 if corner else 3)
        source, target = cells.at[fields, x_source, y_source], cells.at[fields, x_target, y_target]
        put(source, target, near_sem.at[near_of(dx)], dx, gy + dy)

    def neighbours(act, group, sign, column=None):
        for dx in (leave,) if group else (-leave, 0):
            for dy in (-1, 0, 1):
                if isinstance(dx, int) and dy == 0:
                    continue
                above = above_of(dx, near_hops[dy])
                if sign > 0:
                    check = above > 0
                elif sign < 0:
                    check = meets(0, above, gy + dy)
                    if dy:
                        check = jnp.logical_and(check, above < 0)
                else:
                    check = jnp.logical_and(above == 0, dy != 0)
                if column is not None:
                    check = jnp.logical_and(check, gy + dy == column)
                if dy:
                    check = jnp.logical_and(check, jnp.logical_not(first_y if dy < 0 else last_y))
                if group:
                    check = jnp.logical_and(check, place.leaves)
                pl.when(check)(functools.partial(act, dx, dy))

    def local_work():
        width = WINDOW * ez
        row = lax.broadcasted_iota(jnp.int32, (by + 8, width), 0)
        lane = lax.broadcasted_iota(jnp.int32, (by + 8, width), 1)
        low = row < by + bx
        cell = jnp.where(row < by, row, jnp.where(low, -1, by))
        start = jnp.where(row < by, 2 * (row // 8), jnp.where(low, 0, ey - 2))
        spot = (cell.astype(jnp.float32) + 0.5) * (1.0 / RATIO) - 0.5
        coarse = (lane // ez + start - 1).astype(jnp.float32)
        spread_y[...] = jnp.maximum(1.0 - jnp.abs(spot - coarse), 0.0)
        row = lax.broadcasted_iota(jnp.int32, (width, nz), 0)
        lane = lax.broadcasted_iota(jnp.int32, (width, nz), 1)
        spot = jnp.clip((lane.astype(jnp.float32) + 0.5) * (1.0 / RATIO) - 0.5, 0.0, ez - 1.0)
        weight = jnp.maximum(1.0 - jnp.abs(spot - lax.rem(row, ez).astype(jnp.float32)), 0.0)
        spread_z[...] = weight.astype(jnp.bfloat16)
        for s in range(bx):
            own = [cells[number, s + 1, TOP : TOP + by] for number in (1, 2)]
            for number, part in enumerate(fiber_of(*own)):
                fibers[number, s] = part
            voltage = cells[0, s + 1, TOP : TOP + by]
            resting = rest_in[s]
            next_recovery[s] = resting + 0.05 * (-resting - 8.0 * voltage * (voltage - 1.15))
            current = 8.0 * voltage * (voltage - 0.15) * (voltage - 1.0) + voltage * resting
            base[s] = voltage - 0.1 * current

    def send_near(dx, dy):
        send_slots(dx, dy)
        send_cells(dx, dy)

    def wait_cells():
        drain_bytes(4 * bx * by * line, local_sem.at[1])

    meets_equals = jnp.logical_and(upper_core, equals > 0)

    def split_equals(strict):
        def visit(dx, column, above):
            test = above < 0 if strict else above == 0
            lower(lambda *peer: pl.when(test)(functools.partial(send_deform, *peer)))(dx, column, above)

        return visit

    @pl.when(meets_equals)
    def _():
        wait_cells()
        for group in (0, 1):
            neighbours(send_near, group, -1)

    pl.when(meets_equals)(lambda: neighbours(send_near, 0, 0))
    peers(split_equals(False), (0,))
    peers(split_equals(True), (1, 0))

    @pl.when(jnp.logical_not(meets_equals))
    def _():
        for group in (0, 1):
            neighbours(send_slots, group, -1)
        wait_cells()
        for group in (1, 0):
            neighbours(send_cells, group, -1)

    local_work()

    @pl.when(jnp.logical_not(upper_core))
    def _():
        pl.semaphore_wait(equal_ready, 1)

        @pl.when(equals > 0)
        def _():
            neighbours(send_near, 0, 0)
            peers(equal(send_deform), (0,))

    for group, ready, counts in ((0, plane_ready, plane_above), (1, leave_ready, leave_above)):
        for column in columns_by_hops:

            @pl.when(counts[column] > 0)
            def _(group=group, ready=ready, counts=counts, column=column):
                pl.semaphore_wait(ready.at[column], counts[column])
                for dx in (leave,) if group else (-leave, 0):
                    higher(send_deform)(dx, column, above_of(dx, hops_of(column)))
                neighbours(send_near, group, 1, column)

    middle_y = jnp.logical_not(jnp.logical_or(first_y, last_y))
    some_y = jnp.logical_xor(first_y, last_y)
    no_y = jnp.logical_and(first_y, last_y)

    def over_y(act):
        pl.when(middle_y)(functools.partial(act, 2))
        pl.when(some_y)(functools.partial(act, 1))
        pl.when(no_y)(functools.partial(act, 0))

    table = 4 * parts * count

    def wait_leave_near(slot, near, tables=down):
        over_y(lambda n: drain_slots(n + 1, slot))
        over_y(lambda n: drain_bytes(tables * table + (3 * by + n) * line, near))

    def wait_plane_slots(sem):
        over_y(lambda n: drain_slots(2 * n + 1, sem))

    def wait_plane(sem):
        over_y(lambda n: drain_bytes((3 * by + n * (3 * bx + 1)) * line, sem))

    if relayed:

        @pl.when(forwards)
        def _():
            drain_bytes(table, near_sem.at[3])
            source = held.at[1, down - 1, rows]
            put(source, held.at[0, down - 1, rows], near_sem.at[1], leave, 0)

    wait_plane(near_sem.at[0])
    for j in range(bx + 1):
        spot = place.slab(j) if j else jnp.where(place.leaves, place.slab(0), place.slab(1))
        put_volts(place, cells, volts, slopes, spot, j)
    slope = Slopes(place, volts, slopes, parts_x, parts_y, parts_z)

    def rim_of(number):
        pieces = [cells[number, place.slab(j), row : row + 1] for row in (TOP - 1, TOP + by) for j in range(1, bx + 1)]
        return jnp.concatenate(pieces, axis=0)

    rim_fiber = fiber_of(rim_of(1), rim_of(2))
    for number, value in enumerate(rim_fiber):
        rim_fibers[number] = value

    for j in range(bx):
        slope.along_x(j)
        slope.within(j + 1)
    for j in range(1, bx):
        slope.with_x(j)

    wait_plane_slots(slot_sem.at[0])
    index_middle = gather_index(place, near_slots, 1, 0)
    index_side = gather_index(place, near_slots, 1 - leave, -leave)
    if relayed:
        pl.when(jnp.logical_not(forwards))(lambda: drain_bytes((2 * down - 1) * table, near_sem.at[2]))
        pl.when(forwards)(lambda: drain_bytes((2 * down - 2) * table, near_sem.at[2]))
    else:
        drain_bytes((2 * down - 1) * table, near_sem.at[2])
    weight_y, weight_z = spread_y[...], spread_z[...]
    middle_row = pick_row(place, held, 1, index_middle)
    refined[...] = refine_row(place, middle_row, weight_y, weight_z, True)
    middle[0:8] = middle_row[0]
    middle[8:9] = middle_row[1]
    side_row = pick_row(place, held, 1 - leave, index_side)
    side_row = [a - b for a, b in zip(side_row, middle_row)]
    diffs[0] = refine_row(place, side_row, weight_y, weight_z, False)

    def mid(at):
        return refined[at : at + 8]

    def side(at):
        return diffs[0, at : at + 8]

    share = jnp.where(place.leaves, 1.0, 0.0)
    def early_slab(j):
        spot = place.slab(j)

        def fiber_at(rows):
            if j:
                return [fibers[number, spot - 1, rows] for number in range(3)]
            start = TOP + rows.start
            return fiber_of(*(cells[number, spot, start : start + 8] for number in (1, 2)))

        def note(rows, excess):
            voltage = load_rows(volts, (j,), TOP + rows.start, 8)
            partial[j - 1, rows] = base[spot - 1, rows] - excess * (voltage - 0.6)

        weight = share * abs((j - 0.5) / RATIO - 0.5)
        put_tensors(place, conducts, j, mid, side, weight, fiber_at, j == 0, note)

    for j in range(1, half + 1):
        early_slab(j)
    put_rims(place, conducts, {j: j for j in range(1, half + 1)}, mid, side, rim_fiber, share)
    out = send_sem.at[0]
    wait_plane_slots(out)
    wait_plane(out)
    drain_bytes((2 * down - 1) * table, out)

    @pl.when(place.leaves)
    def _():
        wait_leave_near(out, out, down - 1)
        if relayed:
            pl.when(jnp.logical_not(sends_less))(lambda: drain_bytes(table, out))
            pl.when(forwards)(lambda: drain_bytes(table, out))
        else:
            drain_bytes(table, out)

    @pl.when(place.leaves)
    def _():
        wait_leave_near(slot_sem.at[1], near_sem.at[1])
        index = gather_index(place, near_slots, 1 + leave, leave)
        row = pick_row(place, held, 1 + leave, index)
        row = [a - b for a, b in zip(row, (middle[0:8], middle[8:9]))]
        diffs[1] = refine_row(place, row, spread_y[...], spread_z[...], False)
        early_slab(0)


def compute(
    across,
    down,
    sizes,
    fibers,
    rim_fibers,
    refined,
    diffs,
    volts,
    slopes,
    parts_x,
    parts_y,
    parts_z,
    partial,
    base,
    recovered,
    early_conducts,
    cells,
    next_potential,
    next_recovery,
    conducts,
    result,
    out_sem,
):
    bx, by, nz = sizes[:3]
    place = Place(across, down, sizes)
    half = RATIO // 2

    pltpu.make_async_copy(recovered, next_recovery, out_sem.at[0]).start()

    which = jnp.where(place.leaves, 1, 0)
    put_volts(place, cells, volts, slopes, place.slab(bx + 1), bx + 1)
    slope = Slopes(place, volts, slopes, parts_x, parts_y, parts_z)
    slope.along_x(bx)
    slope.with_x(bx)

    def finish(j):
        target = next_potential.at[place.slab(j) - 1]
        pltpu.make_async_copy(result.at[j - 1], target, out_sem.at[0]).start()

    def mid(at):
        return refined[at : at + 8]

    def side(at):
        return diffs[which, at : at + 8]

    for j in range(half + 1, bx + 2):
        spot = place.slab(j)

        def fiber_at(rows, j=j, spot=spot):
            if j <= bx:
                return [fibers[number, spot - 1, rows] for number in range(3)]
            start = TOP + rows.start
            return fiber_of(*(cells[number, spot, start : start + 8] for number in (1, 2)))

        def note(rows, excess, j=j, spot=spot):
            voltage = load_rows(volts, (j,), TOP + rows.start, 8)
            result[j - 1, rows] = base[spot - 1, rows] - excess * (voltage - 0.6)

        weight = abs((j - 0.5) / RATIO - 0.5)
        put_tensors(place, conducts, j - half - 1, mid, side, weight, fiber_at, j == bx + 1, note)
    rim_fiber = [rim_fibers[number] for number in range(3)]
    put_rims(place, conducts, {j - half - 1: j for j in range(half + 1, bx + 1)}, mid, side, rim_fiber, 1.0)
    face_x, across_yz = make_flux(place, parts_x, parts_y, parts_z, early_conducts, conducts, half + 1)
    faces = [face_x(j) for j in range(bx + 1)]
    faces[0] = jnp.where(place.leaves, faces[0], 0.0)
    for j in range(1, bx + 1):
        local = partial[j - 1] if j <= half else result[j - 1]
        result[j - 1] = local + 0.1 * (across_yz(j) + (faces[j] - faces[j - 1]))
        finish(j)
    both = fibers.at[pl.ds(0, 2)]
    pltpu.make_async_copy(both, both, out_sem.at[0]).wait()


def solution(mesh):
    across, down = mesh.shape["gx"], mesh.shape["gy"]

    def local(potential, recovery, angles, deform, slots):
        bx, by, nz = potential.shape
        ex, ey, ez = slots.shape
        parts, count = deform.shape
        assert ex == 1 and bx == RATIO and by == RATIO * ey and by % 8 == 0
        assert count % LANES == 0 and parts == 9 and across % 2 == 0 and (2 * ez) % LANES == 0
        sizes = (bx, by, nz, ex, ey, ez, parts, count)
        blocks = count // LANES
        f32 = jnp.float32
        half = RATIO // 2
        shape = jax.ShapeDtypeStruct(potential.shape, f32)
        anywhere = pl.BlockSpec(memory_space=pl.ANY)
        in_vmem = pl.BlockSpec(memory_space=pltpu.VMEM)
        planes = nz // LANES
        fine = 9 * (by + 8)
        planes = nz // LANES
        fine = 9 * (by + 8)
        rows = pltpu.VMEM((bx + 2, planes, by + 16, LANES), f32)
        passed = (
            pltpu.VMEM((3, bx, by, nz), f32),
            pltpu.VMEM((3, 2 * bx, nz), f32),
            pltpu.VMEM((fine, nz), f32),
            pltpu.VMEM((2, fine, nz), f32),
            rows,
            rows,
            pltpu.VMEM((bx + 1, 3, by, nz), f32),
            pltpu.VMEM((bx, 2, 3, by, nz), f32),
            pltpu.VMEM((bx, 3, by, nz), f32),
            pltpu.VMEM((half, by, nz), f32),
            pltpu.VMEM((bx, by, nz), f32),
            pltpu.VMEM((bx, by, nz), f32),
            pltpu.VMEM((6, half + 1, planes, by + 16, LANES), f32),
            pltpu.VMEM((3, bx + 2, by + 16, nz), f32),
        )
        arrived = pl.pallas_call(
            functools.partial(exchange, across, down, sizes),
            out_shape=passed,
            in_specs=[pl.BlockSpec(memory_space=pltpu.MemorySpace.HBM)] * 5,
            out_specs=(in_vmem,) * len(passed),
            scratch_shapes=[
                pltpu.VMEM((3, down, 8 * blocks + 8, LANES), f32),
                pltpu.VMEM((3, 3, ex, ey, ez), jnp.int32),
                pltpu.VMEM(recovery.shape, f32),
                pltpu.VMEM((by + 8, WINDOW * ez), f32),
                pltpu.VMEM((WINDOW * ez, nz), jnp.bfloat16),
                pltpu.VMEM((16, (ey + 2) * ez), f32),
                pltpu.VMEM((4 * bx * by + 2 * down * parts * count // nz, 1, nz), f32),
                pltpu.VMEM((5, ex, ey, ez), jnp.int32),
                pltpu.SemaphoreType.DMA((1,)),
                pltpu.SemaphoreType.DMA((2,)),
                pltpu.SemaphoreType.DMA((4,)),
                pltpu.SemaphoreType.DMA((3,)),
                pltpu.SemaphoreType.REGULAR((down,)),
                pltpu.SemaphoreType.REGULAR((down,)),
                pltpu.SemaphoreType.REGULAR,
            ],
            compiler_params=pltpu.CompilerParams(
                collective_id=0, has_side_effects=True, vmem_limit_bytes=VMEM_LIMIT
            ),
        )(*(pltpu.with_memory_space_constraint(x, pltpu.MemorySpace.HBM) for x in (potential, recovery, angles, deform, slots)))
        return pl.pallas_call(
            functools.partial(compute, across, down, sizes),
            out_shape=(shape, shape),
            in_specs=[in_vmem] * len(passed),
            out_specs=(anywhere,) * 2,
            scratch_shapes=[
                pltpu.VMEM((6, half + 1, planes, by + 16, LANES), f32),
                pltpu.VMEM((bx, by, nz), f32),
                pltpu.SemaphoreType.DMA((1,)),
            ],
            compiler_params=pltpu.CompilerParams(vmem_limit_bytes=VMEM_LIMIT),
        )(*arrived)

    return jax.shard_map(
        local,
        mesh=mesh,
        in_specs=(
            P("gx", "gy", None),
            P("gx", "gy", None),
            P(None, "gx", "gy", None),
            P(None, ("gx", "gy")),
            P("gx", "gy", None),
        ),
        out_specs=(P("gx", "gy", None), P("gx", "gy", None)),
        check_vma=False,
    )
```

```python
import functools

import jax
import jax.numpy as jnp
from jax import lax
from jax.experimental import pallas as pl
from jax.experimental.pallas import tpu as pltpu
from jax.sharding import PartitionSpec as P

MESH = pl.DeviceIdType.MESH
RATIO = 4
LANES = 128
VMEM_LIMIT = 16 * 1024 * 1024
TOP = 8
WINDOW = 4
FIBER_SCALE = (7.0 / 3.0) ** 0.5
STRETCH_SCALE = (3.0 / 7.0) ** 0.5
XX, YY, ZZ, XY, XZ, YZ = range(6)
PAIRS = ((0, 0), (1, 1), (2, 2), (0, 1), (0, 2), (1, 2))


def split_two(values):
    high = values.astype(jnp.bfloat16)
    low = (values - high.astype(jnp.float32)).astype(jnp.bfloat16)
    return high, low


def dot_two(values, weights):
    high, low = split_two(values)
    return jnp.dot(high, weights, preferred_element_type=jnp.float32) + jnp.dot(
        low, weights, preferred_element_type=jnp.float32
    )


def polynomial(terms, value):
    total = terms[-1]
    for term in terms[-2::-1]:
        total = total * value + term
    return total


HALF_SINE = (0.707106764632592, -0.02946274890445726, 3.682656229209654e-4, -2.187710743548062e-6, 7.155278665108425e-9)
HALF_COSINE = (1.414213496564441, -0.17677636064176425, 3.6825754039592376e-3, -3.0612650004537585e-5, 1.2790856262670407e-7)


def sine_cosine(angle):
    square = angle * angle
    sine = angle * polynomial(HALF_SINE, square)
    cosine = polynomial(HALF_COSINE, square)
    return sine * cosine, 1.0 - sine * sine


def fiber_of(azimuth, elevation):
    sin_u, cos_u = sine_cosine(azimuth)
    sin_e, cos_e = sine_cosine(elevation)
    flat = FIBER_SCALE * cos_e
    return cos_u * flat, sin_u * flat, FIBER_SCALE * sin_e


def tensor_of(entries, fiber, sign, wanted):
    def element(i, j):
        return entries[3 * (i % 3) + j % 3]

    adjugate = [
        [
            element(j + 1, i + 1) * element(j + 2, i + 2)
            - element(j + 1, i + 2) * element(j + 2, i + 1)
            for j in range(3)
        ]
        for i in range(3)
    ]
    determinant = (
        element(0, 0) * adjugate[0][0]
        + element(0, 1) * adjugate[1][0]
        + element(0, 2) * adjugate[2][0]
    )
    inverse = 1.0 / determinant
    square = inverse * inverse
    diagonal = (0.3 * 0.5) * square
    mixed = (0.3 * 0.125) * square
    mirrored = (0.3 * 0.125 * sign) * square
    rows = sorted({i for number in wanted for i in PAIRS[number]})
    pulled = {
        i: adjugate[i][0] * fiber[0] + adjugate[i][1] * fiber[1] + adjugate[i][2] * fiber[2]
        for i in rows
    }
    scale = {XX: diagonal, YY: diagonal, ZZ: diagonal, XY: mirrored, XZ: mirrored, YZ: mixed}
    conduct = {}
    for number in wanted:
        i, j = PAIRS[number]
        metric = (
            adjugate[i][0] * adjugate[j][0]
            + adjugate[i][1] * adjugate[j][1]
            + adjugate[i][2] * adjugate[j][2]
        )
        conduct[number] = scale[number] * (metric + pulled[i] * pulled[j])
    return conduct


def excess_of(entries, fiber):
    parts = [
        entries[3 * i] * fiber[0] + entries[3 * i + 1] * fiber[1] + entries[3 * i + 2] * fiber[2]
        for i in range(3)
    ]
    square = parts[0] * parts[0] + parts[1] * parts[1] + parts[2] * parts[2]
    return jnp.maximum(STRETCH_SCALE * (square * lax.rsqrt(square)) - 1.0, 0.0)


class Place:
    def __init__(self, across, down, sizes):
        self.across, self.down, self.sizes = across, down, sizes
        self.gx, self.gy = lax.axis_index("gx"), lax.axis_index("gy")
        self.first_x, self.last_x = self.gx == 0, self.gx == across - 1
        self.first_y, self.last_y = self.gy == 0, self.gy == down - 1
        odd = lax.rem(self.gx, 2)
        self.odd = odd
        self.leave = 2 * odd - 1
        self.leaves = jnp.logical_not(jnp.logical_or(self.first_x, self.last_x))
        self.late = jnp.where(self.leaves, self.leave, -self.leave)
        self.sign = jnp.where(self.late > 0, 1.0, -1.0)

    def slab(self, j):
        last = self.sizes[0] + 1
        return jnp.where(self.late > 0, j, last - j)


def load_rows(ref, at, start, size):
    planes = [ref[(*at, part, slice(start, start + size))] for part in range(ref.shape[-3])]
    return jnp.concatenate(planes, axis=1)


def store_rows(ref, at, start, value):
    for part in range(ref.shape[-3]):
        rows = slice(start, start + value.shape[0])
        ref[(*at, part, rows)] = value[:, part * LANES : (part + 1) * LANES]


def gather_index(place, near_slots, q, offset):
    ey = place.sizes[4]
    low = jnp.where(place.first_y, near_slots[q, 1, 0, 0:1], near_slots[q, 0, 0, ey - 1 : ey])
    high = jnp.where(place.last_y, near_slots[q, 1, 0, ey - 1 : ey], near_slots[q, 2, 0, 0:1])
    pieces = [low] + [near_slots[q, 1, 0, c : c + 1] for c in range(ey)] + [high]
    count = place.sizes[7]
    return jnp.concatenate(pieces, axis=1) - (place.gx + offset) * (place.down * count)


def page_of(index):
    return index >> (LANES.bit_length() - 1)


def keep_page(rows, page):
    kept = lax.broadcasted_iota(jnp.int32, rows.shape, 0) == page
    return jnp.sum(jnp.where(kept, rows, 0.0), axis=0, keepdims=True)


def pick_row(place, held, q, index):
    blocks = place.sizes[7] // LANES
    totals, lasts = [], []
    for t in range(index.shape[1] // LANES):
        lanes = index[:, t * LANES : (t + 1) * LANES]
        page = page_of(lanes)
        spot = jnp.broadcast_to(lanes & (LANES - 1), (8, LANES))

        def take(rows):
            return jnp.take_along_axis(rows, spot, axis=1, mode="promise_in_bounds")

        total = None
        tails = []
        for h in range(place.down):
            tails.append(held[q, h, 8 * blocks : 9 * blocks])
            for b in range(blocks):
                found = take(held[q, h, 8 * b : 8 * b + 8])
                total = found if total is None else jnp.where(page == h * blocks + b, found, total)
        totals.append(total)
        tails = jnp.concatenate(tails, axis=0)
        last = None
        for g in range(0, place.down * blocks, 8):
            part = keep_page(take(tails[g : g + 8]), page - g)
            last = part if last is None else last + part
        lasts.append(last)
    return jnp.concatenate(totals, axis=1), jnp.concatenate(lasts, axis=1)


def refine_row(place, row, weight_y, weight_z, whole):
    by, ez = place.sizes[1], place.sizes[5]
    total, last = row
    span = WINDOW * ez
    spread = []
    for k in range(9):
        values = total[k : k + 1] if k < 8 else last
        for half in range(by // 8):
            at = 2 * half * ez
            spread.append(weight_y[8 * half : 8 * half + 8] * values[:, at : at + span])
        at = (by // 4 - 2) * ez
        rim = lax.broadcasted_iota(jnp.int32, (8, span), 0) < 4
        spread.append(weight_y[by : by + 8] * jnp.where(rim, values[:, 0:span], values[:, at : at + span]))
    spread = jnp.concatenate(spread, axis=0)
    if whole:
        return dot_two(spread, weight_z)
    return jnp.dot(spread.astype(jnp.bfloat16), weight_z, preferred_element_type=jnp.float32)


def rolls(nz, by):
    lane = lax.broadcasted_iota(jnp.int32, (by, nz), 1)

    def ahead(values):
        return pltpu.roll(values, nz - 1, 1)

    def behind(values):
        return pltpu.roll(values, 1, 1)

    return lane, ahead, behind


def grad_z(values):
    nz = values.shape[1]
    lane, ahead, behind = rolls(nz, values.shape[0])
    upper = jnp.where(lane == nz - 1, values, ahead(values))
    lower = jnp.where(lane == 0, values, behind(values))
    return upper - lower


class Slopes:
    def __init__(self, place, volts, slopes, parts_x, parts_y, parts_z):
        self.place, self.volts, self.slopes = place, volts, slopes
        self.parts_x, self.parts_y, self.parts_z = parts_x, parts_y, parts_z

    def volt(self, j, shift=0):
        return load_rows(self.volts, (j,), TOP + shift, self.place.sizes[1])

    def slope_z(self, j, shift=0):
        return load_rows(self.slopes, (j,), TOP + shift, self.place.sizes[1])

    def slope_y(self, j):
        return self.volt(j, 1) - self.volt(j, -1)

    def slope_x(self, j, shift=0):
        return self.volt(j + 1, shift) - self.volt(j - 1, shift)

    def pair(self, values):
        return values + pltpu.roll(values, values.shape[1] - 1, 1)

    def along_x(self, j):
        self.parts_x[j, 0] = self.volt(j + 1) - self.volt(j)
        self.parts_x[j, 1] = self.slope_y(j) + self.slope_y(j + 1)
        self.parts_x[j, 2] = self.slope_z(j) + self.slope_z(j + 1)

    def with_x(self, j):
        for side, shift in enumerate((1, -1)):
            self.parts_y[j - 1, side, 0] = self.slope_x(j) + self.slope_x(j, shift)
        self.parts_z[j - 1, 0] = self.pair(self.slope_x(j))

    def within(self, j):
        here = self.volt(j)
        for side, shift in enumerate((1, -1)):
            self.parts_y[j - 1, side, 1] = shift * (self.volt(j, shift) - here)
            self.parts_y[j - 1, side, 2] = self.slope_z(j) + self.slope_z(j, shift)
        self.parts_z[j - 1, 1] = self.pair(self.slope_y(j))
        self.parts_z[j - 1, 2] = pltpu.roll(here, here.shape[1] - 1, 1) - here


def make_flux(place, parts_x, parts_y, parts_z, early, late, first):
    by, nz = place.sizes[1:3]
    lane, ahead, behind = rolls(nz, by)
    y_row = lax.broadcasted_iota(jnp.int32, (by, nz), 0)

    def tensor(number, j, shift=0):
        at = (number, j) if j < first else (number, j - first)
        return load_rows(early if j < first else late, at, TOP + shift, by)

    def face_x(j):
        terms = [
            (tensor(number, j) + tensor(number, j + 1)) * parts_x[j, part]
            for part, number in enumerate((XX, XY, XZ))
        ]
        return terms[0] + terms[1] + terms[2]

    def face_y(j, side, shift):
        terms = [
            (tensor(number, j) + tensor(number, j, shift)) * parts_y[j - 1, side, part]
            for part, number in enumerate((XY, YY, YZ))
        ]
        return terms[0] + terms[1] + terms[2]

    def across_yz(j):
        upper = jnp.where(jnp.logical_and(y_row == by - 1, place.last_y), 0.0, face_y(j, 0, 1))
        lower = jnp.where(jnp.logical_and(y_row == 0, place.first_y), 0.0, face_y(j, 1, -1))
        terms = []
        for part, number in enumerate((XZ, YZ, ZZ)):
            mine = tensor(number, j)
            terms.append((mine + ahead(mine)) * parts_z[j - 1, part])
        face_z = jnp.where(lane == nz - 1, 0.0, terms[0] + terms[1] + terms[2])
        return (upper - lower) + (face_z - behind(face_z))

    return face_x, across_yz


def put_tensors(place, conducts, slot, mid, side, weight, fiber_at, halo, note):
    by = place.sizes[1]
    tall = by + 8
    for half in range(by // 8):
        rows = slice(8 * half, 8 * half + 8)
        entries = []
        for k in range(9):
            at = tall * k + 8 * half
            entries.append(mid(at) + weight * side(at))
        fiber = fiber_at(rows)
        wanted = (XX, XY, XZ) if halo else tuple(range(6))
        for number, value in tensor_of(entries, fiber, place.sign, wanted).items():
            store_rows(conducts, (number, slot), TOP + 8 * half, value)
        if not halo:
            note(rows, excess_of(entries, fiber))


def put_rims(place, conducts, slabs, mid, side, rim_fiber, share):
    bx, by, nz = place.sizes[:3]
    tall = by + 8
    row = lax.rem(lax.broadcasted_iota(jnp.int32, (8, nz), 0), bx)
    weight = jnp.zeros((8, nz), jnp.float32)
    for j in slabs.values():
        weight = jnp.where(row == j - 1, share * abs((j - 0.5) / RATIO - 0.5), weight)
    entries = []
    for k in range(9):
        entries.append(mid(tall * k + by) + weight * side(tall * k + by))
    for number, value in tensor_of(entries, rim_fiber, place.sign, (YY, XY, YZ)).items():
        for slot, j in slabs.items():
            store_rows(conducts, (number, slot), TOP - 1, value[j - 1 : j])
            store_rows(conducts, (number, slot), TOP + by, value[bx + j - 1 : bx + j])


def put_volts(place, cells, volts, slopes, spot, slot):
    by = place.sizes[1]
    own = cells[0, spot, TOP : TOP + by]
    low, high = cells[0, spot, TOP - 1 : TOP], cells[0, spot, TOP + by : TOP + by + 1]
    low = jnp.where(place.first_y, own[0:1], low)
    high = jnp.where(place.last_y, own[by - 1 : by], high)
    for start, value in ((TOP, own), (TOP - 1, low), (TOP + by, high)):
        store_rows(volts, (slot,), start, value)
        store_rows(slopes, (slot,), start, grad_z(value))


def exchange(
    across,
    down,
    sizes,
    potential,
    recovery,
    angles,
    deform,
    slots,
    fibers,
    rim_fibers,
    refined,
    diffs,
    volts,
    parts_x,
    parts_y,
    parts_z,
    partial,
    base,
    next_recovery,
    conducts,
    late_fibers,
    cells,
    slopes,
    held,
    near_slots,
    rest_in,
    spread_y,
    spread_z,
    middle,
    gauge,
    slot_gauge,
    send_sem,
    slot_sem,
    near_sem,
    local_sem,
    plane_ready,
    leave_ready,
    equal_ready,
):
    bx, by, nz, ex, ey, ez, parts, count = sizes
    blocks = count // LANES
    place = Place(across, down, sizes)
    half = RATIO // 2
    gx, gy = place.gx, place.gy
    first_y, last_y, leave = place.first_y, place.last_y, place.leave
    for b in range(blocks):
        columns = pl.ds(b * LANES, LANES)
        pltpu.make_async_copy(
            deform.at[pl.ds(0, 8), columns], held.at[1, gy, pl.ds(8 * b, 8)], local_sem.at[0]
        ).start()
        pltpu.make_async_copy(
            deform.at[pl.ds(8, 1), columns], held.at[1, gy, pl.ds(8 * blocks + b, 1)], local_sem.at[0]
        ).start()
    inside = pl.ds(TOP, by)
    pltpu.make_async_copy(slots, near_slots.at[1, 1], local_sem.at[2]).start()
    pltpu.make_async_copy(potential, cells.at[0, pl.ds(1, bx), inside], local_sem.at[1]).start()
    pltpu.make_async_copy(angles, cells.at[pl.ds(1, 2), pl.ds(1, bx), inside], local_sem.at[1]).start()
    pltpu.make_async_copy(recovery, rest_in, local_sem.at[1]).start()

    sides = ((leave, place.leaves), (-leave, None))

    def when(check, act):
        if check is None:
            act()
        else:
            pl.when(check)(act)

    bits = max(down - 1, 1).bit_length()
    odd = place.odd

    def hops_of(column):
        if isinstance(column, int):
            return column.bit_count()
        hops = 0
        for _ in range(bits):
            halved = column // 2
            hops = hops + column - 2 * halved
            column = halved
        return hops

    own_hops = hops_of(gy)

    def above_of(dx, hops):
        chips = leave if dx is leave else 0
        return 4 * (chips + hops - own_hops) + chips

    columns_by_hops = sorted(range(down), key=lambda column: (column.bit_count(), column))

    def peers(act, groups):
        for group in groups:
            rows = ((leave,),) if group else ((-leave, 0),)

            def visit(rows=rows[0]):
                for column in columns_by_hops:
                    for dx in rows:
                        act(dx, column, above_of(dx, hops_of(column)))

            when(place.leaves if group else None, visit)

    relayed = down == 4

    def apart(dx, column):
        if not relayed or dx is not leave or column not in (0, down - 1):
            return True
        here = jnp.logical_and(odd == 1, gy == down - 1) if column == 0 else jnp.logical_and(odd == 0, gy == 0)
        return jnp.logical_not(here)

    relays_table = jnp.logical_and(place.leaves, jnp.logical_and(odd == 1, gy == down - 1)) if relayed else False
    sends_less = jnp.logical_and(place.leaves, jnp.logical_and(odd == 1, gy == down - 1))
    forwards = jnp.logical_and(place.leaves, jnp.logical_and(odd == 1, gy == 0))
    announces = jnp.logical_and(gx >= 3, jnp.logical_and(odd == 1, gy == 0))

    def other(dx, column):
        return column != gy if isinstance(dx, int) else True

    def guarded(test, act):
        def visit(dx, column, above):
            here = jnp.logical_and(test(above), other(dx, column))
            pl.when(here)(functools.partial(act, dx, column))

        return visit

    upper_core = odd == 1

    def meets(dx, above, column):
        even_row = odd == 0 if isinstance(dx, int) else odd == 1
        return jnp.logical_or(above < 0, jnp.logical_and(above == 0, jnp.logical_or(jnp.logical_not(even_row), column == gy)))

    def lower(act):
        def visit(dx, column, above):
            here = jnp.logical_and(meets(0, above, column), jnp.logical_and(other(dx, column), apart(dx, column)))
            pl.when(here)(functools.partial(act, dx, column))

        return visit

    def level(act):
        def visit(dx, column, above):
            there = jnp.logical_and(meets(dx, -above, column), jnp.logical_and(other(dx, column), apart(dx, column)))
            pl.when(there)(functools.partial(act, dx, column))

        return visit

    def equal(act):
        def visit(dx, column, above):
            pl.when(jnp.logical_and(above == 0, column != gy))(functools.partial(act, dx, column))

        return visit

    def beneath(act):
        def visit(dx, column, above):
            pl.when(jnp.logical_and(above < 0, apart(dx, column)))(functools.partial(act, dx, column))

        return visit

    def higher(act):
        return guarded(lambda above: above > 0, act)

    near_hops = {dy: hops_of(gy + dy) for dy in (-1, 0, 1)}
    barrier = pltpu.get_barrier_semaphore()

    def tell(sem, dx, column):
        pl.semaphore_signal(sem, inc=1, device_id=(gx + dx, column), device_id_type=MESH)

    peers(level(functools.partial(tell, barrier)), (0, 1))
    below = 0
    equals = 0
    plane_above, leave_above = [], []
    for column in range(down):
        higher_here = 0
        for dx in (-leave, 0):
            above = above_of(dx, hops_of(column))
            below = below + jnp.where(jnp.logical_and(meets(0, above, column), other(dx, column)), 1, 0)
            higher_here = higher_here + jnp.where(above > 0, 1, 0)
            equals = equals + jnp.where(jnp.logical_and(above == 0, column != gy), 1, 0)
        plane_above.append(higher_here)
        above = above_of(leave, hops_of(column))
        met = jnp.logical_and(meets(0, above, column), apart(leave, column))
        below = below + jnp.where(jnp.logical_and(place.leaves, met), 1, 0)
        leave_above.append(jnp.where(jnp.logical_and(place.leaves, above > 0), 1, 0))

    if relayed:
        below = below + jnp.where(announces, 1, 0)
        pl.when(sends_less)(lambda: tell(barrier, 2, 0))
    pl.semaphore_wait(barrier, below)
    if relayed:
        pl.when(announces)(lambda: tell(leave_ready.at[down - 1], -1, 0))
    pl.when(upper_core)(lambda: tell(equal_ready, -1, gy))
    peers(beneath(functools.partial(tell, leave_ready.at[gy])), (1,))
    peers(beneath(functools.partial(tell, plane_ready.at[gy])), (0,))

    def drain(ref, sem):
        pltpu.make_async_copy(ref, ref, sem).wait()

    rows = pl.ds(0, 9 * blocks)
    line = 4 * nz

    def drain_bytes(amount, sem):
        assert amount % line == 0
        drain(gauge.at[pl.ds(0, amount // line)], sem)

    def drain_slots(amount, sem):
        drain(slot_gauge.at[pl.ds(0, amount)], sem)

    drain(held.at[1, gy, rows], local_sem.at[0])
    drain_slots(1, local_sem.at[2])

    def put(source, target, sem, dx, where):
        pltpu.make_async_remote_copy(
            src_ref=source,
            dst_ref=target,
            send_sem=send_sem.at[0],
            recv_sem=sem,
            device_id=(gx + dx, where),
            device_id_type=MESH,
        ).start()

    def near_of(dx):
        return 0 if isinstance(dx, int) else jnp.where(dx == leave, 1, 0)

    def table_of(dx, column):
        if isinstance(dx, int):
            return jnp.where(relays_table, 3, 2) if column == 0 else 2
        return jnp.where(dx == leave, 1, 2)

    def send_deform(dx, column):
        q = 1 - dx
        put(held.at[1, gy, rows], held.at[q, gy, rows], near_sem.at[table_of(dx, column)], dx, column)

    def send_slots(dx, dy):
        put(near_slots.at[1, 1], near_slots.at[1 - dx, 1 - dy], slot_sem.at[near_of(dx)], dx, gy + dy)

    def send_cells(dx, dy):
        y_source = inside if dy == 0 else pl.ds(TOP if dy < 0 else TOP + by - 1, 1)
        y_target = inside if dy == 0 else pl.ds(TOP + by if dy < 0 else TOP - 1, 1)
        if isinstance(dx, int):
            x_source = x_target = pl.ds(1, bx)
        else:
            x_source = pl.ds(jnp.where(dx < 0, 1, bx), 1)
            x_target = pl.ds(jnp.where(dx < 0, bx + 1, 0), 1)
        corner = dy != 0 and not isinstance(dx, int)
        fields = pl.ds(0, 1 if corner else 3)
        source, target = cells.at[fields, x_source, y_source], cells.at[fields, x_target, y_target]
        put(source, target, near_sem.at[near_of(dx)], dx, gy + dy)

    def neighbours(act, group, sign, column=None):
        for dx in (leave,) if group else (-leave, 0):
            for dy in (-1, 0, 1):
                if isinstance(dx, int) and dy == 0:
                    continue
                above = above_of(dx, near_hops[dy])
                if sign > 0:
                    check = above > 0
                elif sign < 0:
                    check = meets(0, above, gy + dy)
                    if dy:
                        check = jnp.logical_and(check, above < 0)
                else:
                    check = jnp.logical_and(above == 0, dy != 0)
                if column is not None:
                    check = jnp.logical_and(check, gy + dy == column)
                if dy:
                    check = jnp.logical_and(check, jnp.logical_not(first_y if dy < 0 else last_y))
                if group:
                    check = jnp.logical_and(check, place.leaves)
                pl.when(check)(functools.partial(act, dx, dy))

    def local_work():
        width = WINDOW * ez
        row = lax.broadcasted_iota(jnp.int32, (by + 8, width), 0)
        lane = lax.broadcasted_iota(jnp.int32, (by + 8, width), 1)
        low = row < by + bx
        cell = jnp.where(row < by, row, jnp.where(low, -1, by))
        start = jnp.where(row < by, 2 * (row // 8), jnp.where(low, 0, ey - 2))
        spot = (cell.astype(jnp.float32) + 0.5) * (1.0 / RATIO) - 0.5
        coarse = (lane // ez + start - 1).astype(jnp.float32)
        spread_y[...] = jnp.maximum(1.0 - jnp.abs(spot - coarse), 0.0)
        row = lax.broadcasted_iota(jnp.int32, (width, nz), 0)
        lane = lax.broadcasted_iota(jnp.int32, (width, nz), 1)
        spot = jnp.clip((lane.astype(jnp.float32) + 0.5) * (1.0 / RATIO) - 0.5, 0.0, ez - 1.0)
        weight = jnp.maximum(1.0 - jnp.abs(spot - lax.rem(row, ez).astype(jnp.float32)), 0.0)
        spread_z[...] = weight.astype(jnp.bfloat16)
        for s in range(bx):
            own = [cells[number, s + 1, TOP : TOP + by] for number in (1, 2)]
            for number, part in enumerate(fiber_of(*own)):
                fibers[number, s] = part
            voltage = cells[0, s + 1, TOP : TOP + by]
            resting = rest_in[s]
            next_recovery[s] = resting + 0.05 * (-resting - 8.0 * voltage * (voltage - 1.15))
            current = 8.0 * voltage * (voltage - 0.15) * (voltage - 1.0) + voltage * resting
            base[s] = voltage - 0.1 * current

    def send_near(dx, dy):
        send_slots(dx, dy)
        send_cells(dx, dy)

    def wait_cells():
        drain_bytes(4 * bx * by * line, local_sem.at[1])

    meets_equals = jnp.logical_and(upper_core, equals > 0)

    def split_equals(strict):
        def visit(dx, column, above):
            test = above < 0 if strict else above == 0
            lower(lambda *peer: pl.when(test)(functools.partial(send_deform, *peer)))(dx, column, above)

        return visit

    @pl.when(meets_equals)
    def _():
        wait_cells()
        for group in (0, 1):
            neighbours(send_near, group, -1)

    pl.when(meets_equals)(lambda: neighbours(send_near, 0, 0))
    peers(split_equals(False), (0,))
    peers(split_equals(True), (1, 0))

    @pl.when(jnp.logical_not(meets_equals))
    def _():
        for group in (0, 1):
            neighbours(send_slots, group, -1)
        wait_cells()
        for group in (1, 0):
            neighbours(send_cells, group, -1)

    local_work()

    @pl.when(jnp.logical_not(upper_core))
    def _():
        pl.semaphore_wait(equal_ready, 1)

        @pl.when(equals > 0)
        def _():
            neighbours(send_near, 0, 0)
            peers(equal(send_deform), (0,))

    for group, ready, counts in ((0, plane_ready, plane_above), (1, leave_ready, leave_above)):
        for column in columns_by_hops:

            @pl.when(counts[column] > 0)
            def _(group=group, ready=ready, counts=counts, column=column):
                pl.semaphore_wait(ready.at[column], counts[column])
                for dx in (leave,) if group else (-leave, 0):
                    higher(send_deform)(dx, column, above_of(dx, hops_of(column)))
                neighbours(send_near, group, 1, column)

    middle_y = jnp.logical_not(jnp.logical_or(first_y, last_y))
    some_y = jnp.logical_xor(first_y, last_y)
    no_y = jnp.logical_and(first_y, last_y)

    def over_y(act):
        pl.when(middle_y)(functools.partial(act, 2))
        pl.when(some_y)(functools.partial(act, 1))
        pl.when(no_y)(functools.partial(act, 0))

    table = 4 * parts * count

    def wait_leave_near(slot, near, tables=down):
        over_y(lambda n: drain_slots(n + 1, slot))
        over_y(lambda n: drain_bytes(tables * table + (3 * by + n) * line, near))

    def wait_plane_slots(sem):
        over_y(lambda n: drain_slots(2 * n + 1, sem))

    def wait_plane(sem):
        over_y(lambda n: drain_bytes((3 * by + n * (3 * bx + 1)) * line, sem))

    if relayed:

        @pl.when(forwards)
        def _():
            drain_bytes(table, near_sem.at[3])
            source = held.at[1, down - 1, rows]
            put(source, held.at[0, down - 1, rows], near_sem.at[1], leave, 0)

    wait_plane(near_sem.at[0])
    for j in range(bx + 1):
        spot = place.slab(j) if j else jnp.where(place.leaves, place.slab(0), place.slab(1))
        put_volts(place, cells, volts, slopes, spot, j)
    slope = Slopes(place, volts, slopes, parts_x, parts_y, parts_z)

    def rim_of(number):
        pieces = [cells[number, place.slab(j), row : row + 1] for row in (TOP - 1, TOP + by) for j in range(1, bx + 1)]
        return jnp.concatenate(pieces, axis=0)

    rim_fiber = fiber_of(rim_of(1), rim_of(2))
    for number, value in enumerate(rim_fiber):
        rim_fibers[number] = value

    for j in range(bx):
        slope.along_x(j)
        slope.within(j + 1)
    for j in range(1, bx):
        slope.with_x(j)

    wait_plane_slots(slot_sem.at[0])
    index_middle = gather_index(place, near_slots, 1, 0)
    index_side = gather_index(place, near_slots, 1 - leave, -leave)
    edge = bx + 1

    def late_local():
        spot = place.slab(edge)
        put_volts(place, cells, volts, slopes, spot, edge)
        slope.along_x(bx)
        slope.with_x(bx)
        angles_there = [cells[number, spot, TOP : TOP + by] for number in (1, 2)]
        for number, value in enumerate(fiber_of(*angles_there)):
            late_fibers[number] = value

    pl.when(jnp.logical_not(place.leaves))(late_local)
    if relayed:
        pl.when(jnp.logical_not(forwards))(lambda: drain_bytes((2 * down - 1) * table, near_sem.at[2]))
        pl.when(forwards)(lambda: drain_bytes((2 * down - 2) * table, near_sem.at[2]))
    else:
        drain_bytes((2 * down - 1) * table, near_sem.at[2])
    weight_y, weight_z = spread_y[...], spread_z[...]
    middle_row = pick_row(place, held, 1, index_middle)
    refined[...] = refine_row(place, middle_row, weight_y, weight_z, True)
    middle[0:8] = middle_row[0]
    middle[8:9] = middle_row[1]
    side_row = pick_row(place, held, 1 - leave, index_side)
    side_row = [a - b for a, b in zip(side_row, middle_row)]
    diffs[0] = refine_row(place, side_row, weight_y, weight_z, False)

    def mid(at):
        return refined[at : at + 8]

    def side(at):
        return diffs[0, at : at + 8]

    share = jnp.where(place.leaves, 1.0, 0.0)
    def early_slab(j):
        spot = place.slab(j)

        def fiber_at(rows):
            if j:
                return [fibers[number, spot - 1, rows] for number in range(3)]
            start = TOP + rows.start
            return fiber_of(*(cells[number, spot, start : start + 8] for number in (1, 2)))

        def note(rows, excess):
            voltage = load_rows(volts, (j,), TOP + rows.start, 8)
            partial[j - 1, rows] = base[spot - 1, rows] - excess * (voltage - 0.6)

        weight = share * abs((j - 0.5) / RATIO - 0.5)
        put_tensors(place, conducts, j, mid, side, weight, fiber_at, j == 0, note)

    for j in range(1, half + 1):
        early_slab(j)
    put_rims(place, conducts, {j: j for j in range(1, half + 1)}, mid, side, rim_fiber, share)
    out = send_sem.at[0]
    wait_plane_slots(out)
    wait_plane(out)
    drain_bytes((2 * down - 1) * table, out)

    @pl.when(place.leaves)
    def _():
        wait_leave_near(out, out, down - 1)
        if relayed:
            pl.when(jnp.logical_not(sends_less))(lambda: drain_bytes(table, out))
            pl.when(forwards)(lambda: drain_bytes(table, out))
        else:
            drain_bytes(table, out)

    @pl.when(place.leaves)
    def _():
        wait_leave_near(slot_sem.at[1], near_sem.at[1])
        index = gather_index(place, near_slots, 1 + leave, leave)
        row = pick_row(place, held, 1 + leave, index)
        row = [a - b for a, b in zip(row, (middle[0:8], middle[8:9]))]
        diffs[1] = refine_row(place, row, spread_y[...], spread_z[...], False)
        early_slab(0)
        late_local()


def compute(
    across,
    down,
    sizes,
    fibers,
    rim_fibers,
    refined,
    diffs,
    volts,
    parts_x,
    parts_y,
    parts_z,
    partial,
    base,
    recovered,
    early_conducts,
    late_fibers,
    next_potential,
    next_recovery,
    conducts,
    result,
    out_sem,
):
    bx, by, nz = sizes[:3]
    place = Place(across, down, sizes)
    half = RATIO // 2

    pltpu.make_async_copy(recovered, next_recovery, out_sem.at[0]).start()

    which = jnp.where(place.leaves, 1, 0)

    def finish(j):
        target = next_potential.at[place.slab(j) - 1]
        pltpu.make_async_copy(result.at[j - 1], target, out_sem.at[0]).start()

    def mid(at):
        return refined[at : at + 8]

    def side(at):
        return diffs[which, at : at + 8]

    for j in range(half + 1, bx + 2):
        spot = place.slab(j)

        def fiber_at(rows, j=j, spot=spot):
            if j <= bx:
                return [fibers[number, spot - 1, rows] for number in range(3)]
            return [late_fibers[number, rows] for number in range(3)]

        def note(rows, excess, j=j, spot=spot):
            voltage = load_rows(volts, (j,), TOP + rows.start, 8)
            result[j - 1, rows] = base[spot - 1, rows] - excess * (voltage - 0.6)

        weight = abs((j - 0.5) / RATIO - 0.5)
        put_tensors(place, conducts, j - half - 1, mid, side, weight, fiber_at, j == bx + 1, note)
    rim_fiber = [rim_fibers[number] for number in range(3)]
    put_rims(place, conducts, {j - half - 1: j for j in range(half + 1, bx + 1)}, mid, side, rim_fiber, 1.0)
    face_x, across_yz = make_flux(place, parts_x, parts_y, parts_z, early_conducts, conducts, half + 1)
    faces = [face_x(j) for j in range(bx + 1)]
    faces[0] = jnp.where(place.leaves, faces[0], 0.0)
    for j in range(1, bx + 1):
        local = partial[j - 1] if j <= half else result[j - 1]
        result[j - 1] = local + 0.1 * (across_yz(j) + (faces[j] - faces[j - 1]))
        finish(j)
    both = fibers.at[pl.ds(0, 2)]
    pltpu.make_async_copy(both, both, out_sem.at[0]).wait()


def solution(mesh):
    across, down = mesh.shape["gx"], mesh.shape["gy"]

    def local(potential, recovery, angles, deform, slots):
        bx, by, nz = potential.shape
        ex, ey, ez = slots.shape
        parts, count = deform.shape
        assert ex == 1 and bx == RATIO and by == RATIO * ey and by % 8 == 0
        assert count % LANES == 0 and parts == 9 and across % 2 == 0 and (2 * ez) % LANES == 0
        sizes = (bx, by, nz, ex, ey, ez, parts, count)
        blocks = count // LANES
        f32 = jnp.float32
        half = RATIO // 2
        shape = jax.ShapeDtypeStruct(potential.shape, f32)
        anywhere = pl.BlockSpec(memory_space=pl.ANY)
        in_vmem = pl.BlockSpec(memory_space=pltpu.VMEM)
        planes = nz // LANES
        fine = 9 * (by + 8)
        planes = nz // LANES
        fine = 9 * (by + 8)
        rows = pltpu.VMEM((bx + 2, planes, by + 16, LANES), f32)
        passed = (
            pltpu.VMEM((3, bx, by, nz), f32),
            pltpu.VMEM((3, 2 * bx, nz), f32),
            pltpu.VMEM((fine, nz), f32),
            pltpu.VMEM((2, fine, nz), f32),
            rows,
            pltpu.VMEM((bx + 1, 3, by, nz), f32),
            pltpu.VMEM((bx, 2, 3, by, nz), f32),
            pltpu.VMEM((bx, 3, by, nz), f32),
            pltpu.VMEM((half, by, nz), f32),
            pltpu.VMEM((bx, by, nz), f32),
            pltpu.VMEM((bx, by, nz), f32),
            pltpu.VMEM((6, half + 1, planes, by + 16, LANES), f32),
            pltpu.VMEM((3, by, nz), f32),
        )
        arrived = pl.pallas_call(
            functools.partial(exchange, across, down, sizes),
            out_shape=passed,
            in_specs=[pl.BlockSpec(memory_space=pltpu.MemorySpace.HBM)] * 5,
            out_specs=(in_vmem,) * len(passed),
            scratch_shapes=[
                pltpu.VMEM((3, bx + 2, by + 16, nz), f32),
                rows,
                pltpu.VMEM((3, down, 8 * blocks + 8, LANES), f32),
                pltpu.VMEM((3, 3, ex, ey, ez), jnp.int32),
                pltpu.VMEM(recovery.shape, f32),
                pltpu.VMEM((by + 8, WINDOW * ez), f32),
                pltpu.VMEM((WINDOW * ez, nz), jnp.bfloat16),
                pltpu.VMEM((16, (ey + 2) * ez), f32),
                pltpu.VMEM((4 * bx * by + 2 * down * parts * count // nz, 1, nz), f32),
                pltpu.VMEM((5, ex, ey, ez), jnp.int32),
                pltpu.SemaphoreType.DMA((1,)),
                pltpu.SemaphoreType.DMA((2,)),
                pltpu.SemaphoreType.DMA((4,)),
                pltpu.SemaphoreType.DMA((3,)),
                pltpu.SemaphoreType.REGULAR((down,)),
                pltpu.SemaphoreType.REGULAR((down,)),
                pltpu.SemaphoreType.REGULAR,
            ],
            compiler_params=pltpu.CompilerParams(
                collective_id=0, has_side_effects=True, vmem_limit_bytes=VMEM_LIMIT
            ),
        )(*(pltpu.with_memory_space_constraint(x, pltpu.MemorySpace.HBM) for x in (potential, recovery, angles, deform, slots)))
        return pl.pallas_call(
            functools.partial(compute, across, down, sizes),
            out_shape=(shape, shape),
            in_specs=[in_vmem] * len(passed),
            out_specs=(anywhere,) * 2,
            scratch_shapes=[
                pltpu.VMEM((6, half + 1, planes, by + 16, LANES), f32),
                pltpu.VMEM((bx, by, nz), f32),
                pltpu.SemaphoreType.DMA((1,)),
            ],
            compiler_params=pltpu.CompilerParams(vmem_limit_bytes=VMEM_LIMIT),
        )(*arrived)

    return jax.shard_map(
        local,
        mesh=mesh,
        in_specs=(
            P("gx", "gy", None),
            P("gx", "gy", None),
            P(None, "gx", "gy", None),
            P(None, ("gx", "gy")),
            P("gx", "gy", None),
        ),
        out_specs=(P("gx", "gy", None), P("gx", "gy", None)),
        check_vma=False,
    )
```
